32 devices in a mesh: rows: 8 (over y, x, core), mem: 4 (over z).
Axes of the slice: x: 2, y: 2, z: 4, core: 2. Of those that a mesh axis runs over, the one named last changes fastest.
Arguments:
- dec_input: bfloat16 [64, 176, 768], P('rows'), may hold values from -6 to 6
- enc_output: bfloat16 [64, 512, 768], P('rows', 'mem'), may hold values from -6 to 6
- dec_segments: int32 [64, 176], P('rows'), may hold values from 0 to 3, as said below
- enc_segments: int32 [64, 512], P('rows'), may hold values from 0 to 3, as said below
- buckets: int32 [176], replicated, may hold values from 0 to 31
- gains: bfloat16 [3, 768], replicated, may hold values from 0.5 to 1.5
- self_query: bfloat16 [768, 768], P(None, 'mem'), may hold values from -0.0546875 to 0.0546875
- self_kv: bfloat16 [2, 768, 768], P(None, None, 'mem'), may hold values from -0.21875 to 0.21875
- self_out: bfloat16 [768, 768], P('mem'), may hold values from -0.625 to 0.625
- rel_table: bfloat16 [32, 12], P(None, 'mem'), may hold values from -4 to 4
- cross_query: bfloat16 [768, 768], P(None, 'mem'), may hold values from -0.0546875 to 0.0546875
- cross_kv: bfloat16 [2, 768, 768], P(None, None, 'mem'), may hold values from -0.21875 to 0.21875
- cross_out: bfloat16 [768, 768], P('mem'), may hold values from -0.875 to 0.875
- ffn_in: bfloat16 [2, 768, 2048], P(None, None, 'mem'), may hold values from -0.21875 to 0.21875
- ffn_out: bfloat16 [2048, 768], P('mem'), may hold values from -0.25 to 0.25
- cotangent: bfloat16 [64, 176, 768], P('rows'), may hold values from -6 to 6
Outputs:
- dec_output: float32 [64, 176, 768], P('rows', 'mem')
- grad_dec_input: float32 [64, 176, 768], P('rows', 'mem')
- grad_enc_output: float32 [64, 512, 768], P('rows', 'mem')
- grad_gains: float32 [3, 768], P(None, 'mem')
- grad_self_query: float32 [768, 768], P(None, 'mem')
- grad_self_kv: float32 [2, 768, 768], P(None, None, 'mem')
- grad_self_out: float32 [768, 768], P('mem')
- grad_rel_table: float32 [32, 12], P(None, 'mem')
- grad_cross_query: float32 [768, 768], P(None, 'mem')
- grad_cross_kv: float32 [2, 768, 768], P(None, None, 'mem')
- grad_cross_out: float32 [768, 768], P('mem')
- grad_ffn_in: float32 [2, 768, 2048], P(None, None, 'mem')
- grad_ffn_out: float32 [2048, 768], P('mem')
The draws below stay inside these ranges and needn't reach their ends.
Inputs may be any that keep to these rules, and one draw needn't show every extreme that they name: `dec_segments`: each row holds 3 examples with ids 1 to 3 in this order, each one token or longer, followed by one or more padding tokens with id 0. `enc_segments`: each row holds the same 3 example ids as the decoder part of that row, 1 to 3 in this order, each one token or longer, followed by one or more padding tokens with id 0.
All inputs are finite; a program needn't handle non-finite values.
Results may differ from the reference program's by a relative error of at most 0.024.
Values may be sent and summed in bfloat16 or wider, within the bound.
A program may use at most 192 MiB of HBM per device.

```python
from functools import partial
import jax
import jax.numpy as jnp
from jax import lax

D = 768
HEADS = 12
DK = 64
FF = 2048
BUCKETS = 32
LD = 176
LE = 512
EXAMPLES = 3
ROWS_DEV = 8
ROWS = 64


def packed_ids(key, seq_width):
    row_keys = jax.random.split(key, ROWS)
    orders = jax.vmap(lambda one_key: jax.random.permutation(one_key, seq_width - 1))(row_keys)
    cut_points = jnp.sort(orders[:, :EXAMPLES] + 1, axis=1)
    positions = jnp.arange(seq_width)
    crossed = jnp.sum((positions[None, :, None] >= cut_points[:, None, :]).astype(jnp.int32), axis=2)
    return jnp.where(crossed == EXAMPLES, 0, crossed + 1).astype(jnp.int32)


def draw_dec_segments(key, part):
    return packed_ids(jax.random.fold_in(key, 11), LD)


def draw_enc_segments(key, part):
    return packed_ids(jax.random.fold_in(key, 23), LE)


def with_ends(array, rng, smallest, largest):
    longest = array.shape.index(max(array.shape))
    spots = []
    for shift in (0, 1):
        where = [jax.random.randint(jax.random.fold_in(rng, axis), (), 0, length) for axis, length in enumerate(array.shape)]
        where[longest] = (where[longest] + shift) % array.shape[longest]
        spots.append(tuple(where))
    return array.at[spots[0]].set(smallest).at[spots[1]].set(largest)


def level_of(rng, extent, shards, low, largest):
    def one(axis_at, parts):
        heights = jax.random.uniform(jax.random.fold_in(jax.random.fold_in(rng, 6), axis_at), (parts,), jnp.float32, low / len(shards), largest / len(shards))
        return jnp.repeat(jnp.exp(heights), extent[axis_at] // parts).reshape((-1,) + (1,) * (len(extent) - axis_at - 1))

    factor_of = one(*shards[0])
    for cut in shards[1:]:
        factor_of = factor_of * one(*cut)
    return factor_of


def bell_draw(key, dims, spread, bound, cuts=(), held_as=jnp.bfloat16):
    values = jax.random.normal(key, dims, jnp.float32) * spread
    if len(cuts) > 0:
        values = level_of(key, dims, cuts, -0.22, 0.18) * values
    return jnp.clip(values, min=-bound, max=bound).astype(held_as)


def setup_inputs(seed: int = 0) -> dict:
    arg_keys = jax.random.split(jax.random.key(seed), 17)
    dec_input = bell_draw(arg_keys[0], (ROWS, LD, D), 1.0, 6.0, ((0, 8),))
    enc_output = bell_draw(arg_keys[1], (ROWS, LE, D), 1.0, 6.0, ((0, 8), (1, 4)))
    dec_segments = draw_dec_segments(jax.random.fold_in(arg_keys[16], 71), 0)
    enc_segments = draw_enc_segments(jax.random.fold_in(arg_keys[16], 71), 0)
    buckets = with_ends(jax.random.randint(arg_keys[4], (LD,), 0, BUCKETS), jax.random.fold_in(arg_keys[4], 1), 0, BUCKETS - 1).astype(jnp.int32)
    gains = jnp.clip(1.0 + 0.1 * jax.random.normal(arg_keys[5], (3, D), jnp.float32), 0.5, 1.5).astype(jnp.bfloat16)
    self_query = bell_draw(arg_keys[6], (D, HEADS * DK), (16 * D) ** -0.5, 0.0546875, ((1, 4),))
    self_kv = bell_draw(arg_keys[7], (2, D, HEADS * DK), D ** -0.5, 0.21875, ((2, 4),))
    self_out = bell_draw(arg_keys[8], (HEADS * DK, D), (HEADS * DK // 8) ** -0.5, 0.625, ((0, 4),))
    rel_table = bell_draw(arg_keys[9], (BUCKETS, HEADS), 1.0, 4.0, ((1, 4),))
    cross_query = bell_draw(arg_keys[10], (D, HEADS * DK), (16 * D) ** -0.5, 0.0546875, ((1, 4),))
    cross_kv = bell_draw(arg_keys[11], (2, D, HEADS * DK), D ** -0.5, 0.21875, ((2, 4),))
    cross_out = bell_draw(arg_keys[12], (HEADS * DK, D), (HEADS * DK // 16) ** -0.5, 0.875, ((0, 4),))
    ffn_in = bell_draw(arg_keys[13], (2, D, FF), D ** -0.5, 0.21875, ((2, 4),))
    ffn_out = bell_draw(arg_keys[14], (FF, D), (FF // 4) ** -0.5, 0.25, ((0, 4),))
    cotangent = bell_draw(arg_keys[15], (ROWS, LD, D), 1.0, 6.0, ((0, 8),))
    return {"dec_input": dec_input, "enc_output": enc_output, "dec_segments": dec_segments, "enc_segments": enc_segments, "buckets": buckets, "gains": gains, "self_query": self_query, "self_kv": self_kv, "self_out": self_out, "rel_table": rel_table, "cross_query": cross_query, "cross_kv": cross_kv, "cross_out": cross_out, "ffn_in": ffn_in, "ffn_out": ffn_out, "cotangent": cotangent}


@jax.custom_vjp
def low(v):
    return lax.optimization_barrier(v.astype(jnp.bfloat16)).astype(jnp.float32)

@jax.custom_vjp
def low_back(v):
    return v

def low_keep(v):
    return (low(v), None)

def low_pass(kept, grad):
    return (grad,)

def back_keep(v):
    return (v, None)

def back_low(kept, grad):
    return (low(grad),)
low.defvjp(low_keep, low_pass)
low_back.defvjp(back_keep, back_low)
epsilon = 1e-06
negative = -1e+30
highest = lax.Precision.HIGHEST

def matmul(left, right):
    return jnp.dot(left, right, precision=highest)

def rms_scale(values, gain):
    scale = lax.rsqrt(lax.optimization_barrier(jnp.mean(values * values, axis=-1, keepdims=True)) + epsilon)
    return values * scale * gain

def soft_mix(scores, allowed, values_in):
    masked = jnp.where(allowed, scores, negative)
    row_max = lax.optimization_barrier(jnp.max(masked, axis=-1, keepdims=True))
    raised = jnp.exp(masked - row_max)
    weights = raised / lax.optimization_barrier(jnp.sum(raised, axis=-1, keepdims=True))
    return jnp.einsum('rhqs,rshk->rqhk', low(weights), values_in, precision=highest)

def self_block(queries, keys_in, values_in, segments, bias):
    positions = jnp.arange(segments.shape[1])
    allowed = (segments[:, :, None] == segments[:, None, :]) & (positions[:, None] >= positions[None, :])
    scores = low_back(jnp.einsum('rqhk,rshk->rhqs', queries, keys_in, precision=highest) + bias)
    return soft_mix(scores, allowed[:, None], values_in)

def cross_block(queries, keys_in, values_in, dec_ids, enc_ids):
    allowed = dec_ids[:, :, None] == enc_ids[:, None, :]
    scores = low_back(jnp.einsum('rqhk,rshk->rhqs', queries, keys_in, precision=highest))
    return soft_mix(scores, allowed[:, None], values_in)

def grouped(function, arrays, shared):
    groups = ROWS // ROWS_DEV
    stacked = tuple((member.reshape((groups, ROWS_DEV) + member.shape[1:]) for member in arrays))
    checked = jax.checkpoint(function)
    result = lax.map(lambda items: checked(*items, *shared), stacked)
    return result.reshape((ROWS,) + result.shape[2:])

def layer(dec_float, enc_float, gains, self_query, self_kv, self_out, rel_table, cross_query, cross_kv, cross_out, ffn_in, ffn_out, dec_segments, enc_segments, buckets):

    def split_heads(values):
        return values.reshape(values.shape[:-1] + (HEADS, DK))

    def join_heads(values):
        return values.reshape(values.shape[:-2] + (HEADS * DK,))

    def project(values, weight):
        return low_back(low(matmul(values, weight)))
    positions = jnp.arange(LD)
    distance = jnp.maximum(positions[:, None] - positions[None, :], 0)
    bias = jnp.transpose(rel_table[buckets[distance]], (2, 0, 1))
    normed_one = low(rms_scale(dec_float, gains[0]))
    self_mixed = grouped(self_block, (split_heads(project(normed_one, self_query)), split_heads(project(normed_one, self_kv[0])), split_heads(project(normed_one, self_kv[1])), dec_segments), (bias,))
    first = dec_float + low_back(matmul(low_back(low(join_heads(self_mixed))), self_out))
    normed_two = low(rms_scale(first, gains[1]))
    cross_mixed = grouped(cross_block, (split_heads(project(normed_two, cross_query)), split_heads(project(enc_float, cross_kv[0])), split_heads(project(enc_float, cross_kv[1])), dec_segments, enc_segments), ())
    second = first + low_back(matmul(low_back(low(join_heads(cross_mixed))), cross_out))
    normed_three = low(rms_scale(second, gains[2]))
    gate = low_back(matmul(normed_three, ffn_in[0]))
    upward = low_back(matmul(normed_three, ffn_in[1]))
    hidden = low(jax.nn.gelu(gate, approximate=True) * upward)
    return second + low_back(matmul(hidden, ffn_out))

def reference(dec_input, enc_output, dec_segments, enc_segments, buckets, gains, self_query, self_kv, self_out, rel_table, cross_query, cross_kv, cross_out, ffn_in, ffn_out, cotangent):
    floats = tuple((member.astype(jnp.float32) for member in (dec_input, enc_output, gains, self_query, self_kv, self_out, rel_table, cross_query, cross_kv, cross_out, ffn_in, ffn_out)))
    forward = partial(layer, dec_segments=dec_segments, enc_segments=enc_segments, buckets=buckets)
    output, pullback = jax.vjp(forward, *floats)
    gradients = pullback(cotangent.astype(jnp.float32))
    return (output, gradients[0], gradients[1], gradients[2], gradients[3], gradients[4], gradients[5], gradients[6], gradients[7], gradients[8], gradients[9], gradients[10], gradients[11])
```

```python
from functools import partial

import jax
import jax.numpy as jnp
from jax import lax
from jax.experimental import pallas as pl
from jax.experimental.pallas import tpu as pltpu
from jax.sharding import PartitionSpec as P


epsilon = 1e-06
negative = -1e30
highest = lax.Precision.HIGHEST
low = jnp.bfloat16
wide = jnp.float32
pair = 128
head_size = 64


def flip(values, bit):
    size = lax.axis_size("rows")
    return lax.ppermute(values, "rows", [(i, i ^ bit) for i in range(size)])


def fetch(values, step):
    size = lax.axis_size("mem")
    return lax.ppermute(values, "mem", [((i + step) % size, i) for i in range(size)])


def give(values, step):
    size = lax.axis_size("mem")
    return lax.ppermute(values, "mem", [(i, (i + step) % size) for i in range(size)])


def is_up(bit):
    return (lax.axis_index("rows") // bit) % 2


def join(mine, bit, axis):
    other = flip(mine, bit)
    up = is_up(bit) == 1
    return lax.concatenate(
        [jnp.where(up, other, mine), jnp.where(up, mine, other)], axis
    )


def halve(values, bit, axis):
    half = values.shape[axis] // 2
    up = is_up(bit)
    keep = lax.dynamic_slice_in_dim(values, up * half, half, axis)
    send = lax.dynamic_slice_in_dim(values, (1 - up) * half, half, axis)
    return keep, send


def halve_add(values, bit, axis):
    keep, send = halve(values, bit, axis)
    return (keep.astype(wide) + flip(send, bit).astype(wide)).astype(low)


def row_bits(forward):
    bits = []
    bit = 2
    while bit < lax.axis_size("rows"):
        bits.append(bit)
        bit *= 2
    return bits if forward else bits[::-1]


def gather_shard(shard, forward):
    mem = lax.axis_size("mem")
    bits = row_bits(forward)
    piece = halve(shard, 1, 2)[0]
    for bit in bits[::-1]:
        piece = halve(piece, bit, 1)[0]
    far = jnp.stack([fetch(piece, step) for step in range(1, mem)], axis=1)
    for bit in bits:
        far = join(far, bit, 2)
    far = join(far, 1, 3)
    return lax.concatenate([shard[:, None], far], 1)


def reduce_shard(parts, forward):
    mem = lax.axis_size("mem")
    bits = row_bits(forward)
    halves = [halve(part, 1, 3) for part in parts]
    keep = lax.concatenate([half[0] for half in halves], 0)
    send = lax.concatenate([half[1] for half in halves], 0)
    total = (keep.astype(wide) + flip(send, 1).astype(wide)).astype(low)
    for bit in bits[::-1]:
        total = halve_add(total, bit, 2)
    mine = total[:, 0].astype(wide)
    for step in range(1, mem):
        mine = mine + give(total[:, step], step).astype(wide)
    mine = mine.astype(low)
    for bit in bits:
        mine = join(mine, bit, 1)
    return join(mine, 1, 2)


def swap_blocks(blocks):
    mem = lax.axis_size("mem")
    return [blocks[0]] + [give(blocks[mem - step], mem - step) for step in range(1, mem)]


def relative(values, axis, count):
    me = lax.axis_index("mem")
    size = values.shape[axis] // count
    return [
        lax.dynamic_slice_in_dim(values, ((me + step) % count) * size, size, axis)
        for step in range(count)
    ]


def place(blocks, axis, dtype):
    me = lax.axis_index("mem")
    count = len(blocks)
    size = blocks[0].shape[axis]
    shape = list(blocks[0].shape)
    shape[axis] = size * count
    result = jnp.zeros(shape, dtype)
    for step, block in enumerate(blocks):
        result = lax.dynamic_update_slice_in_dim(
            result, block.astype(dtype), ((me + step) % count) * size, axis
        )
    return result


def dot(left, right, left_dim, right_dim):
    return lax.dot_general(
        left, right, (((left_dim,), (right_dim,)), ((), ())), preferred_element_type=wide
    )


def lanes_of(half):
    lane = lax.broadcasted_iota(jnp.int32, (1, pair), 1)
    return ((lane // head_size) == half).astype(wide)


def skewed(row, height):
    spread = jnp.broadcast_to(row, (height, row.shape[1]))
    return pltpu.roll(spread, 0, 1, stride=1, stride_axis=0)


def attend_body(causal, q_ref, k_ref, v_ref, dec_ref, key_ref, *rest):
    if causal:
        bias_ref, out_ref, weight_ref = rest
    else:
        out_ref, weight_ref = rest
    queries, keys_in, values_in = q_ref[0], k_ref[0], v_ref[0]
    rows, keys = queries.shape[0], keys_in.shape[0]
    allowed = dec_ref[0] == key_ref[0]
    if causal:
        i = lax.broadcasted_iota(jnp.int32, (rows, keys), 0)
        j = lax.broadcasted_iota(jnp.int32, (rows, keys), 1)
        allowed = allowed & (i >= j)
    mixed = jnp.zeros((rows, pair), wide)
    for half in range(2):
        lanes = lanes_of(half)
        scores = dot(queries * lanes.astype(low), keys_in, 1, 1)
        if causal:
            scores = scores + skewed(bias_ref[0, half : half + 1, :], rows)[:, :keys]
        scores = jnp.where(allowed, scores, negative)
        raised = jnp.exp(scores - jnp.max(scores, axis=-1, keepdims=True))
        scale = 1.0 / jnp.sum(raised, axis=-1, keepdims=True)
        weights = (raised * scale).astype(low)
        weight_ref[0, half] = weights
        mixed = mixed + dot(weights, values_in, 1, 0) * lanes
    out_ref[0] = mixed.astype(low)


def attend_back_body(causal, w_ref, q_ref, k_ref, v_ref, g_ref, *rest):
    if causal:
        out_ref, dist_ref = rest
    else:
        dq_ref, dkv_ref = rest
    queries, keys_in, values_in, grad = q_ref[0], k_ref[0], v_ref[0], g_ref[0]
    rows, keys = queries.shape[0], keys_in.shape[0]
    dq = jnp.zeros((rows, pair), wide)
    dk = jnp.zeros((keys, pair), wide)
    dv = jnp.zeros((keys, pair), wide)
    for half in range(2):
        lanes = lanes_of(half)
        weights = w_ref[0, half]
        weights_wide = weights.astype(wide)
        grad_weights = dot(grad * lanes.astype(low), values_in, 1, 1)
        inner = jnp.sum(grad_weights * weights_wide, axis=-1, keepdims=True)
        grad_scores = (weights_wide * (grad_weights - inner)).astype(low)
        dv = dv + dot(weights, grad, 0, 0) * lanes
        dq = dq + dot(grad_scores, keys_in, 1, 0) * lanes
        dk = dk + dot(grad_scores, queries, 0, 0) * lanes
        if causal:
            width = dist_ref.shape[-1]
            i = lax.broadcasted_iota(jnp.int32, (rows, rows), 0)
            j = lax.broadcasted_iota(jnp.int32, (rows, rows), 1)
            upside_down = dot((i + j == rows - 1).astype(wide).astype(low), grad_scores, 1, 0)
            padded = jnp.concatenate(
                [upside_down, jnp.zeros((rows, width - keys), wide)], axis=1
            )
            turned = pltpu.roll(padded, 0, 1, stride=1, stride_axis=0)
            dist_ref[0, 0, half : half + 1, :] = jnp.sum(turned, axis=0, keepdims=True)
    if causal:
        out_ref[0, 0] = dq.astype(low)
        out_ref[0, 1] = dk.astype(low)
        out_ref[0, 2] = dv.astype(low)
    else:
        dq_ref[0] = dq.astype(low)
        dkv_ref[0, 0] = dk.astype(low)
        dkv_ref[0, 1] = dv.astype(low)


def column(length, offset):
    return pl.BlockSpec((1, length, pair), lambda r, p: (r, 0, p + offset))


def cost_of(count, rows, keys, pairs, dots):
    return pl.CostEstimate(
        flops=count * pairs * 2 * dots * 2 * rows * keys * pair,
        bytes_accessed=count * pairs * (2 * rows * keys * 2 + 4 * keys * pair * 2),
        transcendentals=count * pairs * 2 * rows * keys,
    )


def whole_row(*shape):
    return pl.BlockSpec((1,) + shape, lambda r, p: (r,) + (0,) * len(shape))


def attend(queries, sides, offsets, dec_ids, key_ids, bias):
    count, rows, _ = queries.shape
    keys = sides.shape[1]
    pairs = queries.shape[2] // pair if bias is None else bias.shape[0]
    width = pairs * pair
    in_specs = [
        column(rows, 0),
        column(keys, offsets[0]),
        column(keys, offsets[1]),
        whole_row(rows, 1),
        whole_row(1, keys),
    ]
    operands = [queries, sides, sides, dec_ids[:, :, None], key_ids[:, None, :]]
    if bias is not None:
        in_specs.append(pl.BlockSpec((1, 2, bias.shape[2]), lambda r, p: (p, 0, 0)))
        operands.append(bias)
    return pl.pallas_call(
        partial(attend_body, bias is not None),
        grid=(count, pairs),
        in_specs=in_specs,
        out_specs=[
            column(rows, 0),
            pl.BlockSpec((1, 2, rows, keys), lambda r, p: (r, p, 0, 0)),
        ],
        out_shape=[
            jax.ShapeDtypeStruct((count, rows, width), low),
            jax.ShapeDtypeStruct((count, pairs * 2, rows, keys), low),
        ],
        cost_estimate=cost_of(count, rows, keys, pairs, 2),
    )(*operands)


def attend_back(weights, queries, sides, offsets, grad, dist_width):
    count, heads, rows, keys = weights.shape
    pairs = heads // 2
    width = pairs * pair
    causal = dist_width is not None
    if causal:
        out_specs = [
            pl.BlockSpec((1, 3, rows, pair), lambda r, p: (r, 0, 0, p)),
            pl.BlockSpec((1, 1, 2, dist_width), lambda r, p: (r, p, 0, 0)),
        ]
        out_shape = [
            jax.ShapeDtypeStruct((count, 3, rows, width), low),
            jax.ShapeDtypeStruct((count, pairs, 2, dist_width), wide),
        ]
    else:
        out_specs = [
            column(rows, 0),
            pl.BlockSpec((1, 2, keys, pair), lambda r, p: (r, 0, 0, p)),
        ]
        out_shape = [
            jax.ShapeDtypeStruct((count, rows, width), low),
            jax.ShapeDtypeStruct((count, 2, keys, width), low),
        ]
    return pl.pallas_call(
        partial(attend_back_body, causal),
        grid=(count, pairs),
        in_specs=[
            pl.BlockSpec((1, 2, rows, keys), lambda r, p: (r, p, 0, 0)),
            column(rows, 0),
            column(keys, offsets[0]),
            column(keys, offsets[1]),
            column(rows, 0),
        ],
        out_specs=out_specs,
        out_shape=out_shape,
        cost_estimate=cost_of(count, rows, keys, pairs, 4),
    )(weights, queries, sides, sides, grad)


def rms(values, gain):
    scale = lax.rsqrt(jnp.mean(values * values, axis=-1, keepdims=True) + epsilon)
    return (values * scale * gain).astype(low), scale


def rms_back(values, scale, gain, grad):
    grad_gain = jnp.sum(grad * values * scale, axis=(0, 1))
    scaled = grad * gain
    inner = jnp.mean(scaled * values, axis=-1, keepdims=True)
    return scaled * scale - values * (scale * scale * scale * inner), grad_gain


def times_t(values, weight):
    return jnp.einsum("rtd,cd->rtc", values, weight, preferred_element_type=wide)


def times(values, weight):
    return jnp.einsum("rtc,cd->rtd", values, weight, preferred_element_type=wide)


def weight_grad(grads, values):
    return jnp.einsum("rtc,rtd->cd", grads, values, preferred_element_type=wide).astype(low)


def gated(gate, upward):
    return jax.nn.gelu(gate, approximate=True) * upward


def shards(
    dec_input,
    enc_output,
    dec_segments,
    enc_segments,
    buckets,
    gains,
    self_query,
    self_kv,
    self_out,
    rel_table,
    cross_query,
    cross_kv,
    cross_out,
    ffn_in,
    ffn_out,
    cotangent,
):
    mem = lax.axis_size("mem")
    me = lax.axis_index("mem")
    group, dec_len, model = dec_input.shape
    count = group // mem
    own_heads = rel_table.shape[1]
    own_width = self_query.shape[1]
    width = own_width * mem
    pairs = width // pair
    own_hidden = ffn_out.shape[0]
    hidden_half = own_hidden // 2
    gain_values = gains.astype(wide)
    bucket_count = rel_table.shape[0]

    self_shards = (
        jnp.stack([self_query.T, self_kv[0].T]),
        jnp.stack([self_kv[1].T, self_out]),
    )
    cross_shards = (
        jnp.stack([cross_query.T, cross_kv[0].T]),
        jnp.stack([cross_kv[1].T, cross_out]),
    )
    ffn_in_t = jnp.transpose(ffn_in, (0, 2, 1))
    ffn_shards = tuple(
        jnp.stack(
            [
                ffn_in_t[0, start : start + hidden_half],
                ffn_in_t[1, start : start + hidden_half],
                ffn_out[start : start + hidden_half],
            ]
        )
        for start in (0, hidden_half)
    )
    self_a = gather_shard(self_shards[0], True)
    self_b = gather_shard(self_shards[1], False)
    tables = [rel_table] + [fetch(rel_table, step) for step in range(1, mem)]
    enc_blocks = swap_blocks(relative(enc_output, 0, mem))
    cross_a = gather_shard(cross_shards[0], True)
    cross_b = gather_shard(cross_shards[1], False)
    ffn_a = gather_shard(ffn_shards[0], True)
    ffn_b = gather_shard(ffn_shards[1], False)

    def mine(values):
        return lax.dynamic_slice_in_dim(values, me * count, count, 0)

    inputs = mine(dec_input).astype(wide)
    grad_out = mine(cotangent)
    dec_ids = mine(dec_segments)
    enc_ids = jnp.concatenate(relative(mine(enc_segments), 1, mem), axis=1)
    memory = jnp.concatenate(enc_blocks, axis=1)
    enc_len = memory.shape[1]

    lane_count = -(-dec_len // pair) * pair
    turned = jnp.concatenate(
        [
            buckets[:1],
            jnp.full((lane_count - dec_len,), -1, buckets.dtype),
            jnp.flip(buckets[1:]),
        ]
    )
    def one_hot_of(ids):
        return (ids[:, None] == jnp.arange(bucket_count)[None, :]).astype(wide)

    one_hot = one_hot_of(turned)
    table = jnp.concatenate(tables, axis=1).astype(wide)
    bias = jnp.einsum("bh,lb->hl", table, one_hot, precision=highest)
    bias = bias.reshape(pairs, 2, lane_count)

    qkv_weight = jnp.concatenate(
        [self_a.reshape(2 * width, model), self_b[0].reshape(width, model)]
    )
    self_out_weight = self_b[1].reshape(width, model)
    normed_one, scale_one = rms(inputs, gain_values[0])
    qkv = times_t(normed_one, qkv_weight).astype(low)
    self_mixed, self_weights = attend(
        qkv, qkv, (pairs, 2 * pairs), dec_ids, dec_ids, bias
    )
    first = inputs + times(self_mixed, self_out_weight)
    normed_two, scale_two = rms(first, gain_values[1])
    cross_query_weight = cross_a[0].reshape(width, model)
    cross_kv_weight = jnp.concatenate(
        [cross_a[1].reshape(width, model), cross_b[0].reshape(width, model)]
    )
    cross_out_weight = cross_b[1].reshape(width, model)
    cross_kv_values = times_t(memory, cross_kv_weight).astype(low)
    cross_queries = times_t(normed_two, cross_query_weight).astype(low)
    cross_mixed, cross_weights = attend(
        cross_queries, cross_kv_values, (0, pairs), dec_ids, enc_ids, None
    )
    second = first + times(cross_mixed, cross_out_weight)
    normed_three, scale_three = rms(second, gain_values[2])

    half_width = mem * hidden_half
    output = second
    grad_three = jnp.zeros_like(second)
    ffn_grads = []
    for held in (ffn_a, ffn_b):
        in_weight = held[:2].reshape(2 * half_width, model)
        out_weight = held[2].reshape(half_width, model)
        gate_up = times_t(normed_three, in_weight)
        hidden_float, pull = jax.vjp(gated, gate_up[..., :half_width], gate_up[..., half_width:])
        hidden = hidden_float.astype(low)
        output = output + times(hidden, out_weight)
        grad_gate, grad_up = pull(times_t(grad_out, out_weight))
        grad_gate_up = jnp.concatenate([grad_gate.astype(low), grad_up.astype(low)], axis=-1)
        grad_three = grad_three + times(grad_gate_up, in_weight)
        ffn_grads.append(
            (
                weight_grad(grad_gate_up, normed_three).reshape(2, mem, hidden_half, model),
                weight_grad(hidden, grad_out).reshape(1, mem, hidden_half, model),
            )
        )
    sum_ffn_a = reduce_shard(ffn_grads[0], True)
    sum_ffn_b = reduce_shard(ffn_grads[1], False)
    out_blocks = swap_blocks(relative(output.astype(low), 1, mem))

    grad_wide = grad_out.astype(wide)
    back, gain_three = rms_back(second, scale_three, gain_values[2], grad_three)
    grad_second = grad_wide + back
    grad_second_low = grad_second.astype(low)
    grad_cross_mixed = times_t(grad_second_low, cross_out_weight).astype(low)
    grad_cross_out = weight_grad(cross_mixed, grad_second_low)
    cross_dq, cross_dkv = attend_back(
        cross_weights, cross_queries, cross_kv_values, (0, pairs), grad_cross_mixed, None
    )
    grad_cross_query = weight_grad(cross_dq, normed_two)
    grad_cross_kv = jnp.einsum(
        "rmsc,rsd->mcd", cross_dkv, memory, preferred_element_type=wide
    ).astype(low)
    grad_memory = jnp.einsum(
        "rmsc,mcd->rsd",
        cross_dkv,
        cross_kv_weight.reshape(2, width, model),
        preferred_element_type=wide,
    ).astype(low)
    memory_blocks = swap_blocks(
        [
            grad_memory[:, step * (enc_len // mem) : (step + 1) * (enc_len // mem)]
            for step in range(mem)
        ]
    )

    def by_owner(values):
        return values.reshape(-1, mem, own_width, model)

    sum_cross_a = reduce_shard((by_owner(grad_cross_query), by_owner(grad_cross_kv[0])), True)
    sum_cross_b = reduce_shard((by_owner(grad_cross_kv[1]), by_owner(grad_cross_out)), False)
    back, gain_two = rms_back(
        first, scale_two, gain_values[1], times(cross_dq, cross_query_weight)
    )
    grad_first = grad_second + back
    grad_first_low = grad_first.astype(low)
    grad_self_mixed = times_t(grad_first_low, self_out_weight).astype(low)
    grad_self_out = weight_grad(self_mixed, grad_first_low)
    self_grads, distance_sums = attend_back(
        self_weights, qkv, qkv, (pairs, 2 * pairs), grad_self_mixed, lane_count
    )
    grad_qkv = jnp.einsum(
        "rmtc,rtd->mcd", self_grads, normed_one, preferred_element_type=wide
    ).astype(low)
    sum_self_a = reduce_shard((by_owner(grad_qkv[:2]),), True)
    sum_self_b = reduce_shard((by_owner(grad_qkv[2]), by_owner(grad_self_out)), False)
    grad_one = jnp.einsum(
        "rmtc,mcd->rtd",
        self_grads,
        qkv_weight.reshape(3, width, model),
        preferred_element_type=wide,
    )
    back, gain_one = rms_back(inputs, scale_one, gain_values[0], grad_one)
    grad_input = grad_first + back
    input_blocks = swap_blocks(relative(grad_input.astype(low), 1, mem))

    falling = jnp.concatenate(
        [jnp.flip(buckets), jnp.full((lane_count - dec_len,), -1, buckets.dtype)]
    )
    grad_table = jnp.einsum(
        "lb,hl->hb",
        one_hot_of(falling),
        jnp.sum(distance_sums, axis=0).reshape(2 * pairs, lane_count),
        precision=highest,
    )
    gain_grads = jnp.concatenate(
        relative(jnp.stack([gain_one, gain_two, gain_three]), 1, mem), axis=0
    ).reshape(mem, 3 * own_width)
    small = jnp.concatenate(
        [gain_grads, grad_table.reshape(mem, own_heads * bucket_count)], axis=1
    )
    total = small[0]
    for step in range(1, mem):
        total = total + give(small[step], step)
    for bit in [1] + row_bits(True):
        total = total + flip(total, bit)

    def head_columns(values):
        return values.astype(wide).T

    return (
        place(out_blocks, 0, wide),
        place(input_blocks, 0, wide),
        place(memory_blocks, 0, wide),
        total[: 3 * own_width].reshape(3, own_width),
        head_columns(sum_self_a[0]),
        jnp.stack([head_columns(sum_self_a[1]), head_columns(sum_self_b[0])]),
        sum_self_b[1].astype(wide),
        total[3 * own_width :].reshape(own_heads, bucket_count).T,
        head_columns(sum_cross_a[0]),
        jnp.stack([head_columns(sum_cross_a[1]), head_columns(sum_cross_b[0])]),
        sum_cross_b[1].astype(wide),
        jnp.stack(
            [
                jnp.concatenate([sum_ffn_a[part], sum_ffn_b[part]]).astype(wide).T
                for part in range(2)
            ]
        ),
        jnp.concatenate([sum_ffn_a[2], sum_ffn_b[2]]).astype(wide),
    )


def solution(mesh):
    in_specs = (
        P("rows", None, None),
        P("rows", "mem", None),
        P("rows", None),
        P("rows", None),
        P(),
        P(),
        P(None, "mem"),
        P(None, None, "mem"),
        P("mem", None),
        P(None, "mem"),
        P(None, "mem"),
        P(None, None, "mem"),
        P("mem", None),
        P(None, None, "mem"),
        P("mem", None),
        P("rows", None, None),
    )
    out_specs = (
        P("rows", "mem", None),
        P("rows", "mem", None),
        P("rows", "mem", None),
        P(None, "mem"),
        P(None, "mem"),
        P(None, None, "mem"),
        P("mem", None),
        P(None, "mem"),
        P(None, "mem"),
        P(None, None, "mem"),
        P("mem", None),
        P(None, None, "mem"),
        P("mem", None),
    )
    return jax.shard_map(shards, mesh=mesh, in_specs=in_specs, out_specs=out_specs, check_vma=False)
```

```python
from functools import partial

import jax
import jax.numpy as jnp
from jax import lax
from jax.experimental import pallas as pl
from jax.experimental.pallas import tpu as pltpu
from jax.sharding import PartitionSpec as P

epsilon = 1e-06
negative = -1e30
highest = lax.Precision.HIGHEST
low = jnp.bfloat16
wide = jnp.float32
pair = 128
head_size = 64


def flip(values, bit):
    size = lax.axis_size("rows")
    return lax.ppermute(values, "rows", [(i, i ^ bit) for i in range(size)])


def relative(values, axis, count):
    me = lax.axis_index("mem")
    size = values.shape[axis] // count
    return [
        lax.dynamic_slice_in_dim(values, ((me + step) % count) * size, size, axis)
        for step in range(count)
    ]


block = 8
quarters = 4
MESH = pl.DeviceIdType.MESH


class Place:
    def __init__(self):
        rows = lax.axis_index("rows")
        self.base = (rows // block) * block
        inner = rows - self.base
        self.core = inner % 2
        self.quarter = inner // 2
        self.near = self.quarter % 2
        self.far = self.quarter // 2
        self.me = lax.axis_index("mem")
        self.mem = lax.axis_size("mem")

    def at(self, quarter, core):
        return (self.base + quarter * 2 + core, self.me)

    def other_core(self):
        return self.at(self.quarter, 1 - self.core)

    def other_quarter(self, step):
        return self.at(self.turn(step), self.core)

    def turn(self, step):
        near = (self.near + step % 2) % 2
        far = (self.far + step // 2) % 2
        return far * 2 + near

    def along(self, step):
        rows = self.base + self.quarter * 2 + self.core
        return (rows, (self.me + step) % self.mem)

    def greet(self):
        barrier = pltpu.get_barrier_semaphore()
        count = 0
        for step in range(1, self.mem):
            pl.semaphore_signal(barrier, inc=1, device_id=self.along(step), device_id_type=MESH)
            count += 1
        for quarter in range(quarters):
            for core in range(2):
                if quarter or core:
                    there = self.at(self.turn(quarter), (self.core + core) % 2)
                    pl.semaphore_signal(barrier, inc=1, device_id=there, device_id_type=MESH)
                    count += 1
        pl.semaphore_wait(barrier, count)


def send(source, target, sems, index, there, arrival=None):
    copy = pltpu.make_async_remote_copy(
        src_ref=source,
        dst_ref=target,
        send_sem=sems[0].at[index],
        recv_sem=sems[1].at[index if arrival is None else arrival],
        device_id=there,
        device_id_type=MESH,
    )
    copy.start()
    return copy


def expect(buffer, sems, index, place):
    pltpu.make_async_remote_copy(
        src_ref=buffer,
        dst_ref=buffer,
        send_sem=sems[0].at[index],
        recv_sem=sems[1].at[index],
        device_id=place.other_core(),
        device_id_type=MESH,
    ).wait_recv()


class Chunk:
    def __init__(self, index, own_width, own_hidden):
        self.index = index
        self.is_ffn = index >= 2
        self.part = index % 2
        if self.is_ffn:
            self.k = 3
            self.rows = own_hidden // 16
        else:
            self.k = 1
            self.rows = own_width // 2

    def spot(self, quarter, core):
        if self.is_ffn:
            start = ((quarter * 2 + self.part) * 2 + core) * self.rows
            return pl.ds(0, 3), pl.ds(pl.multiple_of(start, self.rows), self.rows)
        start = core * self.rows
        return (
            pl.ds(self.part * quarters + quarter, 1),
            pl.ds(pl.multiple_of(start, self.rows), self.rows),
        )

    def shard(self, refs, quarter, core):
        k, rows = self.spot(quarter, core)
        return refs[self.is_ffn].at[k, rows]

    def whole(self, refs, steps, quarter, core):
        k, rows = self.spot(quarter, core)
        return refs[self.is_ffn].at[k, steps, rows]


def gather_body(
    attn_ref, ffn_ref, enc_ref, table_ref,
    attn_out, ffn_out, memory_out, tables_out,
    own_enc, local_sems, far_send, far_recv, enc_send, enc_recv, table_send, table_recv,
    flat_send, flat_recv, core_send, core_recv,
):
    place = Place()
    mem = place.mem
    shards = (attn_ref, ffn_ref)
    wholes = (attn_out, ffn_out)
    count = own_enc.shape[0]
    chunks = [Chunk(i, attn_ref.shape[1], ffn_ref.shape[1]) for i in range(4)]
    locals_in = pltpu.make_async_copy(
        enc_ref.at[pl.ds(place.me * count, count)], own_enc, local_sems.at[0]
    )
    locals_in.start()
    locals_out = [
        pltpu.make_async_copy(attn_ref, attn_out.at[:, 0], local_sems.at[1]),
        pltpu.make_async_copy(ffn_ref, ffn_out.at[:, 0], local_sems.at[2]),
    ]
    for copy in locals_out:
        copy.start()
    tables_out[0] = table_ref[...]
    place.greet()
    sent = []

    def start_far(i):
        for step in range(1, mem):
            back = mem - step
            sent.append(
                send(
                    chunks[i].shard(shards, place.quarter, place.core),
                    chunks[i].whole(wholes, back, place.quarter, place.core),
                    (far_send.at[i], far_recv.at[i]), step, place.along(step), back,
                )
            )

    def start_enc():
        for step in range(1, mem):
            back = mem - step
            target = ((place.me + step) % mem) * count
            sent.append(
                send(
                    enc_ref.at[pl.ds(target, count)], memory_out.at[:, back],
                    (enc_send, enc_recv), step, place.along(step), back,
                )
            )

    def pass_on(i, turn):
        piece = chunks[i].whole(wholes, pl.ds(1, mem - 1), place.turn(turn), place.core)
        sent.append(send(piece, piece, (core_send.at[i], core_recv.at[i]), turn, place.other_core()))

    def finish_flat(i):
        for turn in range(1, quarters):
            piece = chunks[i].whole(wholes, pl.ds(1, mem - 1), place.turn(turn), place.core)
            expect(piece, (flat_send.at[i], flat_recv.at[i]), turn, place)
            pass_on(i, turn)

    for step in range(1, mem):
        back = mem - step
        sent.append(
            send(table_ref, tables_out.at[back], (table_send, table_recv), step, place.along(step), back)
        )
    start_far(0)
    start_far(1)
    for i in range(4):
        for step in range(1, mem):
            piece = chunks[i].whole(wholes, step, place.quarter, place.core)
            expect(piece, (far_send.at[i], far_recv.at[i]), step, place)
        if i + 2 < 4:
            start_far(i + 2)
        if i == 2:
            start_enc()
        piece = chunks[i].whole(wholes, pl.ds(1, mem - 1), place.quarter, place.core)
        for turn in range(1, quarters):
            sent.append(
                send(piece, piece, (flat_send.at[i], flat_recv.at[i]), turn, place.other_quarter(turn))
            )
        pass_on(i, 0)
        if i > 0:
            finish_flat(i - 1)
    finish_flat(3)
    locals_in.wait()
    own_out = pltpu.make_async_copy(own_enc, memory_out.at[:, 0], local_sems.at[0])
    own_out.start()
    for i in range(4):
        for turn in range(quarters):
            piece = chunks[i].whole(wholes, pl.ds(1, mem - 1), place.turn(turn), 1 - place.core)
            expect(piece, (core_send.at[i], core_recv.at[i]), turn, place)
    for step in range(1, mem):
        expect(memory_out.at[:, step], (enc_send, enc_recv), step, place)
        expect(tables_out.at[step], (table_send, table_recv), step, place)
    for copy in sent:
        copy.wait_send()
    for copy in locals_out:
        copy.wait()
    own_out.wait()


def gather_all(attn, ffn, enc, table):
    mem = lax.axis_size("mem")
    count = enc.shape[0] // mem
    dma = pltpu.SemaphoreType.DMA
    in_place = pl.BlockSpec(memory_space=pl.ANY)
    held = pl.BlockSpec(memory_space=pltpu.VMEM)
    return pl.pallas_call(
        gather_body,
        in_specs=[held, held, in_place, held],
        out_specs=[in_place, in_place, in_place, held],
        out_shape=[
            jax.ShapeDtypeStruct((attn.shape[0], mem) + attn.shape[1:], low),
            jax.ShapeDtypeStruct((ffn.shape[0], mem) + ffn.shape[1:], low),
            jax.ShapeDtypeStruct((count, mem) + enc.shape[1:], low),
            jax.ShapeDtypeStruct((mem,) + table.shape, low),
        ],
        scratch_shapes=[
            pltpu.VMEM((count,) + enc.shape[1:], low),
            dma((3,)),
            dma((4, mem)), dma((4, mem)),
            dma((mem,)), dma((mem,)),
            dma((mem,)), dma((mem,)),
            dma((4, quarters)), dma((4, quarters)),
            dma((4, quarters)), dma((4, quarters)),
        ],
        compiler_params=pltpu.CompilerParams(collective_id=0, has_side_effects=True),
    )(attn, ffn, enc, table)


def add_planes(total_ref, total_at, more_ref, more_at, k, steps):
    first, size = steps

    def plane(index, carry):
        i, d = index // size, index % size
        added = more_ref[more_at + (i, d)].astype(wide)
        here = total_at + (i, first + d)
        total_ref[here] = (total_ref[here].astype(wide) + added).astype(low)
        return carry

    lax.fori_loop(0, k * size, plane, 0)


def reduce_body(
    attn_ref, ffn_ref, memory_ref, first_ref, second_ref, small_ref,
    attn_out, ffn_out, memory_out, first_out, second_out, small_out,
    held_attn, held_ffn, core_attn, core_ffn, near_attn, near_ffn, last_attn, last_ffn,
    far_attn, far_ffn, small_far, small_flat,
    local_sems, core_send, core_recv, near_send, near_recv, last_send, last_recv,
    far_send, far_recv, flat_send, flat_recv, pass_send, pass_recv,
    move_send, move_recv, small_send, small_recv,
):
    place = Place()
    mem = place.mem
    half = mem // 2
    grads = (attn_ref, ffn_ref)
    outs = (attn_out, ffn_out)
    chunks = [Chunk(i, attn_out.shape[1], ffn_out.shape[1]) for i in range(4)]
    helds = (held_attn, held_ffn)
    cores = (core_attn, core_ffn)
    nears = (near_attn, near_ffn)
    lasts = (last_attn, last_ffn)
    fars = (far_attn, far_ffn)
    near_there = place.other_quarter(1)
    far_there = place.other_quarter(2)
    sent = []
    loads = {}

    def buffers(i):
        kind, part = chunks[i].is_ffn, chunks[i].part
        return tuple(group[kind].at[part] for group in (helds, cores, nears, lasts, fars))

    def load(i):
        held, core = buffers(i)[:2]
        for quarter in range(quarters):
            copy = pltpu.make_async_copy(
                chunks[i].whole(grads, pl.ds(0, mem), quarter, place.core),
                held.at[quarter], local_sems.at[i, quarter],
            )
            copy.start()
            loads[i, quarter] = copy

    def to_core(i):
        core = buffers(i)[1]
        for quarter in range(quarters):
            sent.append(
                send(
                    chunks[i].whole(grads, pl.ds(0, mem), quarter, 1 - place.core),
                    core.at[quarter], (core_send.at[i], core_recv.at[i]), quarter,
                    place.other_core(),
                )
            )

    def from_core(i):
        held, core, near = buffers(i)[:3]
        for quarter in range(quarters):
            loads[i, quarter].wait()
            expect(core.at[quarter], (core_send.at[i], core_recv.at[i]), quarter, place)
            add_planes(held, (quarter,), core, (quarter,), chunks[i].k, (0, mem))
        sems = (near_send.at[i], near_recv.at[i])
        for bit in range(2):
            quarter = bit * 2 + (1 - place.near)
            sent.append(
                send(
                    held.at[quarter, :, pl.ds(0, half)], near.at[0, bit], sems, bit, near_there
                )
            )
            quarter = (1 - place.far) * 2 + bit
            sent.append(
                send(
                    held.at[quarter, :, pl.ds(half, half)], near.at[1, bit], sems, 2 + bit, far_there
                )
            )

    def from_near(i):
        held, core, near, last = buffers(i)[:4]
        sems = (near_send.at[i], near_recv.at[i])
        for bit in range(2):
            expect(near.at[0, bit], sems, bit, place)
            add_planes(
                held, (bit * 2 + place.near,), near, (0, bit), chunks[i].k, (0, half)
            )
            expect(near.at[1, bit], sems, 2 + bit, place)
            add_planes(
                held, (place.far * 2 + bit,), near, (1, bit), chunks[i].k, (half, half)
            )
        sems = (last_send.at[i], last_recv.at[i])
        quarter = (1 - place.far) * 2 + place.near
        sent.append(send(held.at[quarter, :, pl.ds(0, half)], last.at[0], sems, 0, far_there))
        quarter = place.far * 2 + (1 - place.near)
        sent.append(send(held.at[quarter, :, pl.ds(half, half)], last.at[1], sems, 1, near_there))

    def from_last(i):
        held, _, _, last, far = buffers(i)
        sems = (last_send.at[i], last_recv.at[i])
        for part in range(2):
            expect(last.at[part], sems, part, place)
            add_planes(
                held, (place.quarter,), last, (part,), chunks[i].k, (part * half, half)
            )
        for step in range(1, mem):
            back = mem - step
            sent.append(
                send(
                    held.at[place.quarter, :, step], far.at[back],
                    (far_send.at[i], far_recv.at[i]), step, place.along(step), back,
                )
            )

    def from_far(i):
        held, _, _, _, far = buffers(i)
        for step in range(1, mem):
            expect(far.at[step], (far_send.at[i], far_recv.at[i]), step, place)
        kind = chunks[i].is_ffn
        k_at, rows_at = chunks[i].spot(place.quarter, place.core)
        for k in range(chunks[i].k):
            total = held[place.quarter, k, 0].astype(wide)
            for step in range(1, mem):
                total = total + far[step, k].astype(wide)
            outs[kind][k_at.start + k, rows_at, :] = total.astype(low)
        piece = chunks[i].shard(outs, place.quarter, place.core)
        for turn in range(1, quarters):
            sent.append(
                send(piece, piece, (flat_send.at[i], flat_recv.at[i]), turn, place.other_quarter(turn))
            )
        sent.append(send(piece, piece, (pass_send.at[i], pass_recv.at[i]), 0, place.other_core()))

    def from_flat(i):
        for turn in range(1, quarters):
            piece = chunks[i].shard(outs, place.turn(turn), place.core)
            expect(piece, (flat_send.at[i], flat_recv.at[i]), turn, place)
            sent.append(
                send(piece, piece, (pass_send.at[i], pass_recv.at[i]), turn, place.other_core())
            )

    def from_pass(i):
        for turn in range(quarters):
            piece = chunks[i].shard(outs, place.turn(turn), 1 - place.core)
            expect(piece, (pass_send.at[i], pass_recv.at[i]), turn, place)

    moves = (
        (lambda step: memory_ref.at[:, step], memory_out),
        (lambda step: first_ref.at[step], first_out),
        (lambda step: second_ref.at[step], second_out),
    )
    for i in range(4):
        load(i)
    stays = []
    for index, (source, target) in enumerate(moves):
        copy = pltpu.make_async_copy(source(0), target.at[place.me], local_sems.at[4, index])
        copy.start()
        stays.append(copy)
    place.greet()
    order = (2, 3, 1, 0)
    for i in order:
        to_core(i)
    for index, (source, target) in enumerate(moves):
        for step in range(1, mem):
            sent.append(
                send(
                    source(step), target.at[place.me], (move_send.at[index], move_recv.at[index]),
                    step, place.along(step), mem - step,
                )
            )
    for step in range(1, mem):
        back = mem - step
        sent.append(
            send(small_ref.at[step], small_far.at[back], (small_send, small_recv), step, place.along(step), back)
        )
    phases = (from_core, from_near, from_last, from_far, from_flat, from_pass)
    for time in range(len(order) + len(phases) - 1):
        for slot, i in enumerate(order):
            if 0 <= time - slot < len(phases):
                phases[time - slot](i)
        if time == 1:
            small = small_ref[0]
            for step in range(1, mem):
                expect(small_far.at[step], (small_send, small_recv), step, place)
                small = small + small_far[step]
            small_flat[0] = small
            for turn in range(1, block):
                there = place.at(place.turn(turn // 2), (place.core + turn % 2) % 2)
                sent.append(
                    send(small_flat.at[0], small_flat.at[turn], (small_send, small_recv), mem + turn, there)
                )
    small = small_flat[0]
    for turn in range(1, block):
        expect(small_flat.at[turn], (small_send, small_recv), mem + turn, place)
        small = small + small_flat[turn]
    small_out[...] = small
    for index, (source, target) in enumerate(moves):
        for step in range(1, mem):
            expect(
                target.at[(place.me + step) % mem],
                (move_send.at[index], move_recv.at[index]), step, place,
            )
    for copy in sent:
        copy.wait_send()
    for copy in stays:
        copy.wait()


def reduce_all(attn, ffn, memory, first, second, small):
    mem = lax.axis_size("mem")
    model = attn.shape[-1]
    dma = pltpu.SemaphoreType.DMA
    in_place = pl.BlockSpec(memory_space=pl.ANY)
    held = pl.BlockSpec(memory_space=pltpu.VMEM)
    chunks = [Chunk(i, attn.shape[2], ffn.shape[2]) for i in (0, 2)]

    def both(*shape_of):
        return [
            pltpu.VMEM((2,) + tuple(s(c) if callable(s) else s for s in shape_of), low)
            for c in chunks
        ]

    def k(chunk):
        return chunk.k

    def rows(chunk):
        return chunk.rows

    sem_shapes = ((4, quarters), (4, quarters), (4, 2), (4, mem), (4, quarters), (4, quarters), (3, mem), (mem + block,))
    sems = [dma((5, quarters))]
    for shape in sem_shapes:
        sems += [dma(shape), dma(shape)]
    return pl.pallas_call(
        reduce_body,
        in_specs=[in_place, in_place, held, held, held, held],
        out_specs=[held, held, in_place, in_place, in_place, held],
        out_shape=[
            jax.ShapeDtypeStruct((attn.shape[0],) + attn.shape[2:], low),
            jax.ShapeDtypeStruct((ffn.shape[0],) + ffn.shape[2:], low),
            jax.ShapeDtypeStruct((mem, memory.shape[0]) + memory.shape[2:], low),
            jax.ShapeDtypeStruct(first.shape, low),
            jax.ShapeDtypeStruct(second.shape, low),
            jax.ShapeDtypeStruct(small.shape[1:], wide),
        ],
        scratch_shapes=both(quarters, k, mem, rows, model)
        + both(quarters, k, mem, rows, model)
        + both(2, 2, k, mem // 2, rows, model)
        + both(2, k, mem // 2, rows, model)
        + both(mem, k, rows, model)
        + [pltpu.VMEM((mem,) + small.shape[1:], wide), pltpu.VMEM((block,) + small.shape[1:], wide)]
        + sems,
        compiler_params=pltpu.CompilerParams(collective_id=1, has_side_effects=True),
    )(attn, ffn, memory, first, second, small)


def sum_blocks(values):
    bit = block
    while bit < lax.axis_size("rows"):
        values = values + flip(values, bit)
        bit *= 2
    return values


def dot(left, right, left_dim, right_dim):
    return lax.dot_general(
        left, right, (((left_dim,), (right_dim,)), ((), ())), preferred_element_type=wide
    )


def lanes_of(half):
    lane = lax.broadcasted_iota(jnp.int32, (1, pair), 1)
    return ((lane // head_size) == half).astype(wide)


def skewed(row, height):
    spread = jnp.broadcast_to(row, (height, row.shape[1]))
    return pltpu.roll(spread, 0, 1, stride=1, stride_axis=0)


def attend_body(causal, q_ref, k_ref, v_ref, dec_ref, key_ref, *rest):
    if causal:
        bias_ref, out_ref, weight_ref = rest
    else:
        out_ref, weight_ref = rest
    queries, keys_in, values_in = q_ref[0], k_ref[0], v_ref[0]
    rows, keys = queries.shape[0], keys_in.shape[0]
    allowed = dec_ref[0] == key_ref[0]
    if causal:
        i = lax.broadcasted_iota(jnp.int32, (rows, keys), 0)
        j = lax.broadcasted_iota(jnp.int32, (rows, keys), 1)
        allowed = allowed & (i >= j)
    mixed = jnp.zeros((rows, pair), wide)
    for half in range(2):
        lanes = lanes_of(half)
        scores = dot(queries * lanes.astype(low), keys_in, 1, 1)
        if causal:
            scores = scores + skewed(bias_ref[0, half : half + 1, :], rows)[:, :keys]
        scores = jnp.where(allowed, scores, negative)
        raised = jnp.exp(scores - jnp.max(scores, axis=-1, keepdims=True))
        scale = 1.0 / jnp.sum(raised, axis=-1, keepdims=True)
        weights = (raised * scale).astype(low)
        weight_ref[0, half] = weights
        mixed = mixed + dot(weights, values_in, 1, 0) * lanes
    out_ref[0] = mixed.astype(low)


def attend_back_body(causal, w_ref, q_ref, k_ref, v_ref, g_ref, *rest):
    if causal:
        out_ref, dist_ref = rest
    else:
        dq_ref, dkv_ref = rest
    queries, keys_in, values_in, grad = q_ref[0], k_ref[0], v_ref[0], g_ref[0]
    rows, keys = queries.shape[0], keys_in.shape[0]
    dq = jnp.zeros((rows, pair), wide)
    dk = jnp.zeros((keys, pair), wide)
    dv = jnp.zeros((keys, pair), wide)
    for half in range(2):
        lanes = lanes_of(half)
        weights = w_ref[0, half]
        weights_wide = weights.astype(wide)
        grad_weights = dot(grad * lanes.astype(low), values_in, 1, 1)
        inner = jnp.sum(grad_weights * weights_wide, axis=-1, keepdims=True)
        grad_scores = (weights_wide * (grad_weights - inner)).astype(low)
        dv = dv + dot(weights, grad, 0, 0) * lanes
        dq = dq + dot(grad_scores, keys_in, 1, 0) * lanes
        dk = dk + dot(grad_scores, queries, 0, 0) * lanes
        if causal:
            width = dist_ref.shape[-1]
            i = lax.broadcasted_iota(jnp.int32, (rows, rows), 0)
            j = lax.broadcasted_iota(jnp.int32, (rows, rows), 1)
            upside_down = dot((i + j == rows - 1).astype(wide).astype(low), grad_scores, 1, 0)
            padded = jnp.concatenate(
                [upside_down, jnp.zeros((rows, width - keys), wide)], axis=1
            )
            turned = pltpu.roll(padded, 0, 1, stride=1, stride_axis=0)
            dist_ref[0, 0, half : half + 1, :] = jnp.sum(turned, axis=0, keepdims=True)
    if causal:
        out_ref[0, 0] = dq.astype(low)
        out_ref[0, 1] = dk.astype(low)
        out_ref[0, 2] = dv.astype(low)
    else:
        dq_ref[0] = dq.astype(low)
        dkv_ref[0, 0] = dk.astype(low)
        dkv_ref[0, 1] = dv.astype(low)


def column(length, offset):
    return pl.BlockSpec((1, length, pair), lambda r, p: (r, 0, p + offset))


def cost_of(count, rows, keys, pairs, dots):
    return pl.CostEstimate(
        flops=count * pairs * 2 * dots * 2 * rows * keys * pair,
        bytes_accessed=count * pairs * (2 * rows * keys * 2 + 4 * keys * pair * 2),
        transcendentals=count * pairs * 2 * rows * keys,
    )


def whole_row(*shape):
    return pl.BlockSpec((1,) + shape, lambda r, p: (r,) + (0,) * len(shape))


def attend(queries, sides, offsets, dec_ids, key_ids, bias):
    count, rows, _ = queries.shape
    keys = sides.shape[1]
    pairs = queries.shape[2] // pair if bias is None else bias.shape[0]
    width = pairs * pair
    in_specs = [
        column(rows, 0),
        column(keys, offsets[0]),
        column(keys, offsets[1]),
        whole_row(rows, 1),
        whole_row(1, keys),
    ]
    operands = [queries, sides, sides, dec_ids[:, :, None], key_ids[:, None, :]]
    if bias is not None:
        in_specs.append(pl.BlockSpec((1, 2, bias.shape[2]), lambda r, p: (p, 0, 0)))
        operands.append(bias)
    return pl.pallas_call(
        partial(attend_body, bias is not None),
        grid=(count, pairs),
        in_specs=in_specs,
        out_specs=[
            column(rows, 0),
            pl.BlockSpec((1, 2, rows, keys), lambda r, p: (r, p, 0, 0)),
        ],
        out_shape=[
            jax.ShapeDtypeStruct((count, rows, width), low),
            jax.ShapeDtypeStruct((count, pairs * 2, rows, keys), low),
        ],
        cost_estimate=cost_of(count, rows, keys, pairs, 2),
    )(*operands)


def attend_back(weights, queries, sides, offsets, grad, dist_width):
    count, heads, rows, keys = weights.shape
    pairs = heads // 2
    width = pairs * pair
    causal = dist_width is not None
    if causal:
        out_specs = [
            pl.BlockSpec((1, 3, rows, pair), lambda r, p: (r, 0, 0, p)),
            pl.BlockSpec((1, 1, 2, dist_width), lambda r, p: (r, p, 0, 0)),
        ]
        out_shape = [
            jax.ShapeDtypeStruct((count, 3, rows, width), low),
            jax.ShapeDtypeStruct((count, pairs, 2, dist_width), wide),
        ]
    else:
        out_specs = [
            column(rows, 0),
            pl.BlockSpec((1, 2, keys, pair), lambda r, p: (r, 0, 0, p)),
        ]
        out_shape = [
            jax.ShapeDtypeStruct((count, rows, width), low),
            jax.ShapeDtypeStruct((count, 2, keys, width), low),
        ]
    return pl.pallas_call(
        partial(attend_back_body, causal),
        grid=(count, pairs),
        in_specs=[
            pl.BlockSpec((1, 2, rows, keys), lambda r, p: (r, p, 0, 0)),
            column(rows, 0),
            column(keys, offsets[0]),
            column(keys, offsets[1]),
            column(rows, 0),
        ],
        out_specs=out_specs,
        out_shape=out_shape,
        cost_estimate=cost_of(count, rows, keys, pairs, 4),
    )(weights, queries, sides, sides, grad)


def rms(values, gain):
    scale = lax.rsqrt(jnp.mean(values * values, axis=-1, keepdims=True) + epsilon)
    return (values * scale * gain).astype(low), scale


def rms_back(values, scale, gain, grad):
    grad_gain = jnp.sum(grad * values * scale, axis=(0, 1))
    scaled = grad * gain
    inner = jnp.mean(scaled * values, axis=-1, keepdims=True)
    return scaled * scale - values * (scale * scale * scale * inner), grad_gain


def times_t(values, weight):
    return jnp.einsum("rtd,cd->rtc", values, weight, preferred_element_type=wide)


def times(values, weight):
    return jnp.einsum("rtc,cd->rtd", values, weight, preferred_element_type=wide)


def weight_grad(grads, values):
    return jnp.einsum("rtc,rtd->cd", grads, values, preferred_element_type=wide).astype(low)


def gated(gate, upward):
    return jax.nn.gelu(gate, approximate=True) * upward


def shards(
    dec_input,
    enc_output,
    dec_segments,
    enc_segments,
    buckets,
    gains,
    self_query,
    self_kv,
    self_out,
    rel_table,
    cross_query,
    cross_kv,
    cross_out,
    ffn_in,
    ffn_out,
    cotangent,
):
    mem = lax.axis_size("mem")
    me = lax.axis_index("mem")
    group, dec_len, model = dec_input.shape
    count = group // mem
    own_heads = rel_table.shape[1]
    own_width = self_query.shape[1]
    width = own_width * mem
    pairs = width // pair
    own_hidden = ffn_out.shape[0]
    gain_values = gains.astype(wide)
    bucket_count = rel_table.shape[0]

    attn_shard = jnp.stack(
        [self_query.T, self_kv[0].T, self_kv[1].T, self_out]
        + [cross_query.T, cross_kv[0].T, cross_kv[1].T, cross_out]
    )
    ffn_shard = jnp.stack([ffn_in[0].T, ffn_in[1].T, ffn_out])
    padded_table = jnp.pad(rel_table, ((0, 0), (0, pair - own_heads)))
    attn_weights, ffn_weights, memory, tables = gather_all(
        attn_shard, ffn_shard, enc_output, padded_table
    )
    attn_weights = attn_weights.reshape(-1, width, model)
    ffn_weights = ffn_weights.reshape(-1, model)
    memory = memory.reshape(count, -1, model)

    def mine(values):
        return lax.dynamic_slice_in_dim(values, me * count, count, 0)

    inputs = mine(dec_input).astype(wide)
    grad_out = mine(cotangent)
    dec_ids = mine(dec_segments)
    enc_ids = jnp.concatenate(relative(mine(enc_segments), 1, mem), axis=1)
    enc_len = memory.shape[1]

    lane_count = -(-dec_len // pair) * pair
    turned = jnp.concatenate(
        [
            buckets[:1],
            jnp.full((lane_count - dec_len,), -1, buckets.dtype),
            jnp.flip(buckets[1:]),
        ]
    )
    def one_hot_of(ids):
        return (ids[:, None] == jnp.arange(bucket_count)[None, :]).astype(wide)

    one_hot = one_hot_of(turned)
    table = tables[:, :, :own_heads].astype(wide)
    bias = jnp.einsum("mbh,lb->mhl", table, one_hot, precision=highest)
    bias = bias.reshape(pairs, 2, lane_count)

    qkv_weight = attn_weights[:3].reshape(3 * width, model)
    self_out_weight = attn_weights[3]
    cross_query_weight = attn_weights[4]
    cross_kv_weight = attn_weights[5:7].reshape(2 * width, model)
    cross_out_weight = attn_weights[7]
    normed_one, scale_one = rms(inputs, gain_values[0])
    qkv = times_t(normed_one, qkv_weight).astype(low)
    self_mixed, self_weights = attend(
        qkv, qkv, (pairs, 2 * pairs), dec_ids, dec_ids, bias
    )
    first = inputs + times(self_mixed, self_out_weight)
    normed_two, scale_two = rms(first, gain_values[1])
    cross_kv_values = times_t(memory, cross_kv_weight).astype(low)
    cross_queries = times_t(normed_two, cross_query_weight).astype(low)
    cross_mixed, cross_weights = attend(
        cross_queries, cross_kv_values, (0, pairs), dec_ids, enc_ids, None
    )
    second = first + times(cross_mixed, cross_out_weight)
    normed_three, scale_three = rms(second, gain_values[2])

    hidden_width = mem * own_hidden
    in_weight = ffn_weights[: 2 * hidden_width]
    out_weight = ffn_weights[2 * hidden_width :]
    gate_up = times_t(normed_three, in_weight)
    hidden_float, pull = jax.vjp(gated, gate_up[..., :hidden_width], gate_up[..., hidden_width:])
    hidden = hidden_float.astype(low)
    output = second + times(hidden, out_weight)
    grad_gate, grad_up = pull(times_t(grad_out, out_weight))
    grad_gate_up = jnp.concatenate([grad_gate.astype(low), grad_up.astype(low)], axis=-1)
    grad_three = times(grad_gate_up, in_weight)
    ffn_grads = jnp.concatenate(
        [weight_grad(grad_gate_up, normed_three), weight_grad(hidden, grad_out)]
    ).reshape(3, mem, own_hidden, model)

    grad_wide = grad_out.astype(wide)
    back, gain_three = rms_back(second, scale_three, gain_values[2], grad_three)
    grad_second = grad_wide + back
    grad_second_low = grad_second.astype(low)
    grad_cross_mixed = times_t(grad_second_low, cross_out_weight).astype(low)
    grad_cross_out = weight_grad(cross_mixed, grad_second_low)
    cross_dq, cross_dkv = attend_back(
        cross_weights, cross_queries, cross_kv_values, (0, pairs), grad_cross_mixed, None
    )
    grad_cross_query = weight_grad(cross_dq, normed_two)
    grad_cross_kv = jnp.einsum(
        "rmsc,rsd->mcd", cross_dkv, memory, preferred_element_type=wide
    ).astype(low)
    grad_memory = jnp.einsum(
        "rmsc,mcd->rsd",
        cross_dkv,
        cross_kv_weight.reshape(2, width, model),
        preferred_element_type=wide,
    ).astype(low)
    back, gain_two = rms_back(
        first, scale_two, gain_values[1], times(cross_dq, cross_query_weight)
    )
    grad_first = grad_second + back
    grad_first_low = grad_first.astype(low)
    grad_self_mixed = times_t(grad_first_low, self_out_weight).astype(low)
    grad_self_out = weight_grad(self_mixed, grad_first_low)
    self_grads, distance_sums = attend_back(
        self_weights, qkv, qkv, (pairs, 2 * pairs), grad_self_mixed, lane_count
    )
    grad_qkv = jnp.einsum(
        "rmtc,rtd->mcd", self_grads, normed_one, preferred_element_type=wide
    ).astype(low)
    attn_grads = jnp.concatenate(
        [
            grad_qkv.reshape(3 * width, model),
            grad_self_out,
            grad_cross_query,
            grad_cross_kv.reshape(2 * width, model),
            grad_cross_out,
        ]
    ).reshape(8, mem, own_width, model)
    grad_one = jnp.einsum(
        "rmtc,mcd->rtd",
        self_grads,
        qkv_weight.reshape(3, width, model),
        preferred_element_type=wide,
    )
    back, gain_one = rms_back(inputs, scale_one, gain_values[0], grad_one)
    grad_input = grad_first + back

    falling = jnp.concatenate(
        [jnp.flip(buckets), jnp.full((lane_count - dec_len,), -1, buckets.dtype)]
    )
    grad_table = jnp.einsum(
        "lb,hl->hb",
        one_hot_of(falling),
        jnp.sum(distance_sums, axis=0).reshape(2 * pairs, lane_count),
        precision=highest,
    )
    gain_grads = jnp.concatenate(
        relative(jnp.stack([gain_one, gain_two, gain_three]), 1, mem), axis=0
    ).reshape(mem, 3 * own_width)
    small = jnp.concatenate(
        [gain_grads, grad_table.reshape(mem, own_heads * bucket_count)], axis=1
    )
    small_size = small.shape[1]
    small = jnp.pad(small, ((0, 0), (0, 8 * pair - small_size))).reshape(mem, 8, pair)
    attn_sums, ffn_sums, grad_memory, output, grad_input, small = reduce_all(
        attn_grads,
        ffn_grads,
        grad_memory.reshape(count, mem, enc_len // mem, model),
        jnp.stack(relative(output.astype(low), 1, mem)),
        jnp.stack(relative(grad_input.astype(low), 1, mem)),
        small,
    )
    attn_sums = sum_blocks(attn_sums).astype(wide)
    ffn_sums = sum_blocks(ffn_sums).astype(wide)
    small = sum_blocks(small).reshape(-1)
    split = 3 * own_width

    def columns(values):
        return jnp.swapaxes(values, -1, -2)

    return (
        output.reshape(group, -1, model).astype(wide),
        grad_input.reshape(group, -1, model).astype(wide),
        grad_memory.reshape(group, -1, model).astype(wide),
        small[:split].reshape(3, own_width),
        columns(attn_sums[0]),
        columns(attn_sums[1:3]),
        attn_sums[3],
        small[split:small_size].reshape(own_heads, bucket_count).T,
        columns(attn_sums[4]),
        columns(attn_sums[5:7]),
        attn_sums[7],
        columns(ffn_sums[:2]),
        ffn_sums[2],
    )


def solution(mesh):
    in_specs = (
        P("rows", None, None),
        P("rows", "mem", None),
        P("rows", None),
        P("rows", None),
        P(),
        P(),
        P(None, "mem"),
        P(None, None, "mem"),
        P("mem", None),
        P(None, "mem"),
        P(None, "mem"),
        P(None, None, "mem"),
        P("mem", None),
        P(None, None, "mem"),
        P("mem", None),
        P("rows", None, None),
    )
    out_specs = (
        P("rows", "mem", None),
        P("rows", "mem", None),
        P("rows", "mem", None),
        P(None, "mem"),
        P(None, "mem"),
        P(None, None, "mem"),
        P("mem", None),
        P(None, "mem"),
        P(None, "mem"),
        P(None, None, "mem"),
        P("mem", None),
        P(None, None, "mem"),
        P("mem", None),
    )
    return jax.shard_map(shards, mesh=mesh, in_specs=in_specs, out_specs=out_specs, check_vma=False)
```

```python
from functools import partial

import jax
import jax.numpy as jnp
from jax import lax
from jax.experimental import pallas as pl
from jax.experimental.pallas import tpu as pltpu
from jax.sharding import PartitionSpec as P

epsilon = 1e-06
negative = -1e30
highest = lax.Precision.HIGHEST
low = jnp.bfloat16
wide = jnp.float32
pair = 128
head_size = 64


def flip(values, bit):
    size = lax.axis_size("rows")
    return lax.ppermute(values, "rows", [(i, i ^ bit) for i in range(size)])


def relative(values, axis, count):
    me = lax.axis_index("mem")
    size = values.shape[axis] // count
    return [
        lax.dynamic_slice_in_dim(values, ((me + step) % count) * size, size, axis)
        for step in range(count)
    ]


block = 8
quarters = 4
MESH = pl.DeviceIdType.MESH


class Place:
    def __init__(self):
        rows = lax.axis_index("rows")
        self.base = (rows // block) * block
        inner = rows - self.base
        self.core = inner % 2
        self.quarter = inner // 2
        self.near = self.quarter % 2
        self.far = self.quarter // 2
        self.me = lax.axis_index("mem")
        self.mem = lax.axis_size("mem")

    def at(self, quarter, core):
        return (self.base + quarter * 2 + core, self.me)

    def other_core(self):
        return self.at(self.quarter, 1 - self.core)

    def other_quarter(self, step):
        return self.at(self.turn(step), self.core)

    def turn(self, step):
        near = (self.near + step % 2) % 2
        far = (self.far + step // 2) % 2
        return far * 2 + near

    def along(self, step):
        rows = self.base + self.quarter * 2 + self.core
        return (rows, (self.me + step) % self.mem)

    def greet(self):
        barrier = pltpu.get_barrier_semaphore()
        count = 0
        for step in range(1, self.mem):
            pl.semaphore_signal(barrier, inc=1, device_id=self.along(step), device_id_type=MESH)
            count += 1
        for quarter in range(quarters):
            for core in range(2):
                if quarter or core:
                    there = self.at(self.turn(quarter), (self.core + core) % 2)
                    pl.semaphore_signal(barrier, inc=1, device_id=there, device_id_type=MESH)
                    count += 1
        pl.semaphore_wait(barrier, count)


def send(source, target, sems, index, there, arrival=None):
    copy = pltpu.make_async_remote_copy(
        src_ref=source,
        dst_ref=target,
        send_sem=sems[0].at[index],
        recv_sem=sems[1].at[index if arrival is None else arrival],
        device_id=there,
        device_id_type=MESH,
    )
    copy.start()
    return copy


def expect(buffer, sems, index, place):
    pltpu.make_async_remote_copy(
        src_ref=buffer,
        dst_ref=buffer,
        send_sem=sems[0].at[index],
        recv_sem=sems[1].at[index],
        device_id=place.other_core(),
        device_id_type=MESH,
    ).wait_recv()


class Chunk:
    def __init__(self, index, own_width, own_hidden):
        self.index = index
        self.is_ffn = index >= 2
        self.part = index % 2
        if self.is_ffn:
            self.k = 3
            self.rows = own_hidden // 16
        else:
            self.k = 1
            self.rows = own_width // 2

    def spot(self, quarter, core):
        if self.is_ffn:
            start = ((quarter * 2 + self.part) * 2 + core) * self.rows
            return pl.ds(0, 3), pl.ds(pl.multiple_of(start, self.rows), self.rows)
        start = core * self.rows
        return (
            pl.ds(self.part * quarters + quarter, 1),
            pl.ds(pl.multiple_of(start, self.rows), self.rows),
        )

    def shard(self, refs, quarter, core):
        k, rows = self.spot(quarter, core)
        return refs[self.is_ffn].at[k, rows]

    def shards(self, refs, quarter, core):
        k, rows = self.spot(quarter, core)
        if self.is_ffn:
            return [refs[1].at[pl.ds(0, 2), rows], refs[1].at[pl.ds(2, 1), rows]]
        return [refs[0].at[k, rows]]

    def wholes(self, refs, steps, quarter, core):
        k, rows = self.spot(quarter, core)
        if self.is_ffn:
            return [refs[1].at[:, steps, rows], refs[2].at[:, steps, rows]]
        return [refs[0].at[k, steps, rows]]


def between_ends(step, me, mem):
    to = (me + step) % mem
    return jnp.logical_and(me - to < mem - 1, to - me < mem - 1)


def gather_body(
    attn_ref, ffn_ref, enc_ref, table_ref,
    input_ref, normed_ref, gain_ref, dec_row_ref, dec_column_ref, enc_row_ref, spread_ref,
    attn_out, in_out, down_out, memory_out,
    qkv_out, self_mixed_out, self_weights_out, first_out, normed_out,
    queries_out, sides_out, cross_mixed_out, cross_weights_out,
    own_enc, tables_out, bias_ref, weights_ref, memory_ref, local_sems, load_sems, far_send, far_recv, enc_send, enc_recv, table_send, table_recv,
    flat_send, flat_recv, core_send, core_recv,
):
    place = Place()
    mem = place.mem
    shards = (attn_ref, ffn_ref)
    wholes = (attn_out, in_out, down_out)
    count = own_enc.shape[0]
    chunks = [Chunk(i, attn_ref.shape[1], ffn_ref.shape[1]) for i in range(4)]
    locals_in = pltpu.make_async_copy(
        enc_ref.at[pl.ds(place.me * count, count)], own_enc, local_sems.at[0]
    )
    locals_in.start()
    locals_out = [
        pltpu.make_async_copy(attn_ref, attn_out.at[:, 0], local_sems.at[1]),
        pltpu.make_async_copy(ffn_ref.at[pl.ds(0, 2)], in_out.at[:, 0], local_sems.at[2]),
        pltpu.make_async_copy(ffn_ref.at[pl.ds(2, 1)], down_out.at[:, 0], local_sems.at[3]),
    ]
    for copy in locals_out:
        copy.start()
    tables_out[0] = table_ref[...]
    place.greet()
    sent = []
    waits = []

    def start_far(i):
        sources = chunks[i].shards(shards, place.quarter, place.core)
        for step in range(1, mem):
            back = mem - step
            targets = chunks[i].wholes(wholes, back, place.quarter, place.core)
            for j, (source, target) in enumerate(zip(sources, targets)):
                copy = pltpu.make_async_remote_copy(
                    src_ref=source, dst_ref=target,
                    send_sem=far_send.at[i, 2 * step + j], recv_sem=far_recv.at[i, 2 * back + j],
                    device_id=place.along(step), device_id_type=MESH,
                )
                direct = between_ends(step, place.me, mem)
                pl.when(direct)(copy.start)
                waits.append((direct, copy))

    def relay(i):
        for step, ahead in ((mem - 2, 1), (2, mem - 1)):
            there = (step - ahead) % mem
            at_turn = place.me == (mem - 2 if ahead == 1 else 1)
            sources = chunks[i].wholes(wholes, step, place.quarter, place.core)
            targets = chunks[i].wholes(wholes, there, place.quarter, place.core)
            for j, (source, target) in enumerate(zip(sources, targets)):
                copy = pltpu.make_async_remote_copy(
                    src_ref=source, dst_ref=target,
                    send_sem=far_send.at[i, 2 * mem + (ahead > 1) * 2 + j],
                    recv_sem=far_recv.at[i, 2 * there + j],
                    device_id=place.along(ahead), device_id_type=MESH,
                )
                pl.when(at_turn)(copy.start)
                waits.append((at_turn, copy))

    def start_enc():
        for step in range(1, mem):
            back = mem - step
            target = ((place.me + step) % mem) * count
            sent.append(
                send(
                    enc_ref.at[pl.ds(target, count)], memory_out.at[:, back],
                    (enc_send, enc_recv), step, place.along(step), back,
                )
            )

    def pieces(i, turn, core):
        return enumerate(chunks[i].wholes(wholes, pl.ds(1, mem - 1), place.turn(turn), core))

    def pass_on(i, turn):
        for j, piece in pieces(i, turn, place.core):
            sems = (core_send.at[i], core_recv.at[i])
            sent.append(send(piece, piece, sems, 2 * turn + j, place.other_core()))

    def finish_flat(i):
        for turn in range(1, quarters):
            for j, piece in pieces(i, turn, place.core):
                expect(piece, (flat_send.at[i], flat_recv.at[i]), 2 * turn + j, place)
            pass_on(i, turn)

    def pass_far(i):
        for step in (2, mem - 1, 1) if mem == 4 else range(1, mem):
            for j, piece in enumerate(chunks[i].wholes(wholes, step, place.quarter, place.core)):
                expect(piece, far_sems_of(i), 2 * step + j, place)
            if step == 2:
                relay(i)
        for j, piece in pieces(i, 0, place.core):
            sems = (flat_send.at[i], flat_recv.at[i])
            for turn in range(1, quarters):
                sent.append(send(piece, piece, sems, 2 * turn + j, place.other_quarter(turn)))
        pass_on(i, 0)

    def far_sems_of(i):
        return far_send.at[i], far_recv.at[i]

    def finish_core(i):
        for turn in range(quarters):
            for j, piece in pieces(i, turn, 1 - place.core):
                expect(piece, (core_send.at[i], core_recv.at[i]), 2 * turn + j, place)

    def bring(source, target):
        copy = pltpu.make_async_copy(source, target, load_sems.at[0])
        copy.start()
        copy.wait()

    def weight(k):
        return weights_ref[k].reshape(-1, model)

    model = attn_ref.shape[2]
    rows, dec_len, _ = input_ref.shape
    enc_len = mem * memory_ref.shape[2]
    pairs = model // pair
    own_heads = model // head_size // mem

    start_far(0)
    for step in range(1, mem):
        back = mem - step
        sent.append(
            send(table_ref, tables_out.at[back], (table_send, table_recv), step, place.along(step), back)
        )
    for i in range(1, 4):
        start_far(i)
    pass_far(0)
    for step in range(1, mem):
        expect(tables_out.at[step], (table_send, table_recv), step, place)
    for step in range(mem):
        per_lane = dot(tables_out[step], spread_ref[...], 0, 0)
        for head in range(own_heads):
            bias_ref[step * own_heads + head] = per_lane[head : head + 1]
    pass_far(1)
    start_enc()
    finish_flat(0)
    pass_far(2)
    finish_core(0)
    for copy in locals_out:
        copy.wait()
    bring(attn_out.at[pl.ds(0, quarters)], weights_ref)

    def project_self(k, carry):
        values = dot(normed_ref[...].reshape(-1, model), weight(k), 1, 1)
        qkv_out[k] = values.astype(low).reshape(rows, dec_len, model)
        return carry

    lax.fori_loop(0, 3, project_self, 0)
    pass_far(3)

    def lanes_at(p):
        return pl.ds(pl.multiple_of(p * pair, pair), pair)

    def self_row(r):
        allowed = causal_mask(dec_column_ref[r] == dec_row_ref[r])

        def step(p, carry):
            weights, mixed = attend_pair(
                qkv_out[0, r, :, lanes_at(p)],
                qkv_out[1, r, :, lanes_at(p)],
                qkv_out[2, r, :, lanes_at(p)],
                allowed,
                [bias_ref[2 * p], bias_ref[2 * p + 1]],
            )
            for half in range(2):
                self_weights_out[r, 2 * p + half] = weights[half]
            self_mixed_out[r, :, lanes_at(p)] = mixed
            return carry

        lax.fori_loop(0, pairs, step, 0)

    def cross_row(r):
        allowed = dec_column_ref[r] == enc_row_ref[r]

        def step(p, carry):
            weights, mixed = attend_pair(
                queries_out[r, :, lanes_at(p)],
                sides_out[0, r, :, lanes_at(p)],
                sides_out[1, r, :, lanes_at(p)],
                allowed,
                None,
            )
            for half in range(2):
                cross_weights_out[r, 2 * p + half] = weights[half]
            cross_mixed_out[r, :, lanes_at(p)] = mixed
            return carry

        lax.fori_loop(0, pairs, step, 0)

    for r in range(rows):
        self_row(r)
    finish_flat(1)
    added = dot(self_mixed_out[...].reshape(-1, model), weight(3), 1, 0)
    first = input_ref[...].astype(wide) + added.reshape(rows, dec_len, model)
    first_out[...] = first
    normed_out[...] = rms(first, gain_ref[1:2, :])[0]
    finish_core(1)
    bring(attn_out.at[pl.ds(quarters, quarters)], weights_ref)
    values = dot(normed_out[...].reshape(-1, model), weight(0), 1, 1)
    queries_out[...] = values.astype(low).reshape(rows, dec_len, model)
    finish_flat(2)
    locals_in.wait()
    own_out = pltpu.make_async_copy(own_enc, memory_out.at[:, 0], local_sems.at[0])
    own_out.start()
    for step in range(1, mem):
        expect(memory_out.at[:, step], (enc_send, enc_recv), step, place)
    own_out.wait()
    bring(memory_out, memory_ref)
    for k in range(2):

        def project_side(r, carry):
            values = dot(memory_ref[r].reshape(-1, model), weight(1 + k), 1, 1)
            sides_out[k, r] = values.astype(low)
            return carry

        lax.fori_loop(0, rows, project_side, 0)
    cross_row(0)
    finish_flat(3)
    for r in range(1, rows):
        cross_row(r)
    finish_core(2)
    finish_core(3)
    for copy in sent:
        copy.wait_send()
    for started, copy in waits:
        pl.when(started)(copy.wait_send)


def gather_all(attn, ffn, enc, table, inputs, normed, gains, dec_ids, enc_ids, spread):
    mem = lax.axis_size("mem")
    count, dec_len, model = inputs.shape
    enc_len = enc_ids.shape[1]
    heads = model // head_size
    dma = pltpu.SemaphoreType.DMA
    in_place = pl.BlockSpec(memory_space=pl.ANY)
    held = pl.BlockSpec(memory_space=pltpu.VMEM)
    operands = (
        attn, ffn, enc, table, inputs, normed, gains,
        dec_ids[:, None, :], dec_ids[:, :, None], enc_ids[:, None, :], spread,
    )

    def values(*shape, dtype=low):
        return jax.ShapeDtypeStruct(shape, dtype)

    return pl.pallas_call(
        gather_body,
        in_specs=[held, held, in_place] + [held] * (len(operands) - 3),
        out_specs=[in_place] * 4 + [held] * 9,
        out_shape=[
            values(attn.shape[0], mem, *attn.shape[1:]),
            values(2, mem, *ffn.shape[1:]),
            values(1, mem, *ffn.shape[1:]),
            values(count, mem, *enc.shape[1:]),
            values(3, count, dec_len, model),
            values(count, dec_len, model),
            values(count, heads, dec_len, dec_len),
            values(count, dec_len, model, dtype=wide),
            values(count, dec_len, model),
            values(count, dec_len, model),
            values(2, count, enc_len, model),
            values(count, dec_len, model),
            values(count, heads, dec_len, enc_len),
        ],
        scratch_shapes=[
            pltpu.VMEM((count,) + enc.shape[1:], low),
            pltpu.VMEM((mem,) + table.shape, low),
            pltpu.VMEM((heads, 1, spread.shape[1]), wide),
            pltpu.VMEM((quarters, mem) + attn.shape[1:], low),
            pltpu.VMEM((count, mem) + enc.shape[1:], low),
            dma((4,)), dma((1,)),
            dma((4, 2 * mem + 4)), dma((4, 2 * mem)),
            dma((mem,)), dma((mem,)),
            dma((mem,)), dma((mem,)),
            dma((4, 2 * quarters)), dma((4, 2 * quarters)),
            dma((4, 2 * quarters)), dma((4, 2 * quarters)),
        ],
        compiler_params=pltpu.CompilerParams(
            collective_id=0, has_side_effects=True, vmem_limit_bytes=60000000
        ),
    )(*operands)


def add_planes(total_ref, total_at, more_ref, more_at, k, steps):
    first, size = steps

    def plane(index, carry):
        i, d = index // size, index % size
        added = more_ref[more_at + (i, d)].astype(wide)
        here = total_at + (i, first + d)
        total_ref[here] = (total_ref[here].astype(wide) + added).astype(low)
        return carry

    lax.fori_loop(0, k * size, plane, 0)


def reduce_body(
    qkv_ref, self_out_ref, query_ref, kv_ref, cross_out_ref, in_ref, down_ref,
    memory_ref, first_ref, second_ref, small_ref,
    attn_out, ffn_out, memory_out, first_out, second_out, small_out,
    held_attn, held_ffn, core_attn, core_ffn, near_attn, near_ffn, last_attn, last_ffn,
    far_attn, far_ffn, small_far, small_flat,
    local_sems, core_send, core_recv, near_send, near_recv, last_send, last_recv,
    far_send, far_recv, flat_send, flat_recv, pass_send, pass_recv,
    move_send, move_recv, small_send, small_recv,
):
    place = Place()
    mem = place.mem
    half = mem // 2
    attn_grads = [(qkv_ref, 0), (qkv_ref, 1), (qkv_ref, 2), (self_out_ref, 0)]
    attn_grads += [(query_ref, 0), (kv_ref, 0), (kv_ref, 1), (cross_out_ref, 0)]
    outs = (attn_out, ffn_out)
    chunks = [Chunk(i, attn_out.shape[1], ffn_out.shape[1]) for i in range(4)]
    helds = (held_attn, held_ffn)
    cores = (core_attn, core_ffn)
    nears = (near_attn, near_ffn)
    lasts = (last_attn, last_ffn)
    fars = (far_attn, far_ffn)
    near_there = place.other_quarter(1)
    far_there = place.other_quarter(2)
    sent = []
    loads = {}

    def buffers(i):
        kind, part = chunks[i].is_ffn, chunks[i].part
        return tuple(group[kind].at[part] for group in (helds, cores, nears, lasts, fars))

    def parts_of(i, quarter, core):
        k, rows = chunks[i].spot(quarter, core)
        if chunks[i].is_ffn:
            yield in_ref.at[:, :, rows], 0, 2
            yield down_ref.at[:, :, rows], 2, 1
        else:
            ref, at = attn_grads[chunks[i].part * quarters + quarter]
            yield ref.at[pl.ds(at, 1), :, rows], 0, 1

    def load(i):
        held = buffers(i)[0]
        for quarter in range(quarters):
            loads[i, quarter] = []
            for source, first, planes in parts_of(i, quarter, place.core):
                copy = pltpu.make_async_copy(
                    source, held.at[quarter, pl.ds(first, planes)],
                    local_sems.at[i, quarter + first // 2 * quarters],
                )
                copy.start()
                loads[i, quarter].append(copy)

    def to_core(i):
        core = buffers(i)[1]
        for quarter in range(quarters):
            for source, first, planes in parts_of(i, quarter, 1 - place.core):
                sent.append(
                    send(
                        source, core.at[quarter, pl.ds(first, planes)],
                        (core_send.at[i], core_recv.at[i]), quarter + first // 2 * quarters,
                        place.other_core(),
                    )
                )

    def from_core(i):
        held, core, near = buffers(i)[:3]
        for quarter in range(quarters):
            for copy in loads[i, quarter]:
                copy.wait()
            sems = (core_send.at[i], core_recv.at[i])
            if chunks[i].is_ffn:
                expect(core.at[quarter, pl.ds(0, 2)], sems, quarter, place)
                expect(core.at[quarter, pl.ds(2, 1)], sems, quarter + quarters, place)
            else:
                expect(core.at[quarter], sems, quarter, place)
            add_planes(held, (quarter,), core, (quarter,), chunks[i].k, (0, mem))
        sems = (near_send.at[i], near_recv.at[i])
        for bit in range(2):
            quarter = bit * 2 + (1 - place.near)
            sent.append(
                send(
                    held.at[quarter, :, pl.ds(0, half)], near.at[0, bit], sems, bit, near_there
                )
            )
            quarter = (1 - place.far) * 2 + bit
            sent.append(
                send(
                    held.at[quarter, :, pl.ds(half, half)], near.at[1, bit], sems, 2 + bit, far_there
                )
            )

    def from_near(i):
        held, core, near, last = buffers(i)[:4]
        sems = (near_send.at[i], near_recv.at[i])
        for bit in range(2):
            expect(near.at[0, bit], sems, bit, place)
            add_planes(
                held, (bit * 2 + place.near,), near, (0, bit), chunks[i].k, (0, half)
            )
            expect(near.at[1, bit], sems, 2 + bit, place)
            add_planes(
                held, (place.far * 2 + bit,), near, (1, bit), chunks[i].k, (half, half)
            )
        sems = (last_send.at[i], last_recv.at[i])
        quarter = (1 - place.far) * 2 + place.near
        sent.append(send(held.at[quarter, :, pl.ds(0, half)], last.at[0], sems, 0, far_there))
        quarter = place.far * 2 + (1 - place.near)
        sent.append(send(held.at[quarter, :, pl.ds(half, half)], last.at[1], sems, 1, near_there))

    def from_last(i):
        held, _, _, last, far = buffers(i)
        sems = (last_send.at[i], last_recv.at[i])
        for part in range(2):
            expect(last.at[part], sems, part, place)
            add_planes(
                held, (place.quarter,), last, (part,), chunks[i].k, (part * half, half)
            )
        for step in range(1, mem):
            back = mem - step
            sent.append(
                send(
                    held.at[place.quarter, :, step], far.at[back],
                    (far_send.at[i], far_recv.at[i]), step, place.along(step), back,
                )
            )

    def from_far(i):
        held, _, _, _, far = buffers(i)
        for step in range(1, mem):
            expect(far.at[step], (far_send.at[i], far_recv.at[i]), step, place)
        kind = chunks[i].is_ffn
        k_at, rows_at = chunks[i].spot(place.quarter, place.core)
        for k in range(chunks[i].k):
            total = held[place.quarter, k, 0].astype(wide)
            for step in range(1, mem):
                total = total + far[step, k].astype(wide)
            outs[kind][k_at.start + k, rows_at, :] = total.astype(low)
        piece = chunks[i].shard(outs, place.quarter, place.core)
        for turn in range(1, quarters):
            sent.append(
                send(piece, piece, (flat_send.at[i], flat_recv.at[i]), turn, place.other_quarter(turn))
            )
        sent.append(send(piece, piece, (pass_send.at[i], pass_recv.at[i]), 0, place.other_core()))

    def from_flat(i):
        for turn in range(1, quarters):
            piece = chunks[i].shard(outs, place.turn(turn), place.core)
            expect(piece, (flat_send.at[i], flat_recv.at[i]), turn, place)
            sent.append(
                send(piece, piece, (pass_send.at[i], pass_recv.at[i]), turn, place.other_core())
            )

    def from_pass(i):
        for turn in range(quarters):
            piece = chunks[i].shard(outs, place.turn(turn), 1 - place.core)
            expect(piece, (pass_send.at[i], pass_recv.at[i]), turn, place)

    moves = (
        (lambda step: memory_ref.at[:, step], memory_out),
        (lambda step: first_ref.at[step], first_out),
        (lambda step: second_ref.at[step], second_out),
    )
    for i in range(4):
        load(i)
    stays = []
    for index, (source, target) in enumerate(moves):
        copy = pltpu.make_async_copy(source(0), target.at[place.me], local_sems.at[4, index])
        copy.start()
        stays.append(copy)
    place.greet()
    order = (2, 3, 1, 0)
    for i in order:
        to_core(i)
    for index, (source, target) in enumerate(moves):
        for step in range(1, mem):
            sent.append(
                send(
                    source(step), target.at[place.me], (move_send.at[index], move_recv.at[index]),
                    step, place.along(step), mem - step,
                )
            )
    for step in range(1, mem):
        back = mem - step
        sent.append(
            send(small_ref.at[step], small_far.at[back], (small_send, small_recv), step, place.along(step), back)
        )
    phases = (from_core, from_near, from_last, from_far, from_flat, from_pass)
    for time in range(len(order) + len(phases) - 1):
        for slot, i in reversed(list(enumerate(order))):
            if 0 <= time - slot < len(phases):
                phases[time - slot](i)
        if time == 1:
            small = small_ref[0]
            for step in range(1, mem):
                expect(small_far.at[step], (small_send, small_recv), step, place)
                small = small + small_far[step]
            small_flat[0] = small
            for turn in range(1, block):
                there = place.at(place.turn(turn // 2), (place.core + turn % 2) % 2)
                sent.append(
                    send(small_flat.at[0], small_flat.at[turn], (small_send, small_recv), mem + turn, there)
                )
    small = small_flat[0]
    for turn in range(1, block):
        expect(small_flat.at[turn], (small_send, small_recv), mem + turn, place)
        small = small + small_flat[turn]
    small_out[...] = small
    for index, (source, target) in enumerate(moves):
        for step in range(1, mem):
            expect(
                target.at[(place.me + step) % mem],
                (move_send.at[index], move_recv.at[index]), step, place,
            )
    for copy in sent:
        copy.wait_send()
    for copy in stays:
        copy.wait()


def reduce_all(attn, ffn, memory, first, second, small):
    mem = lax.axis_size("mem")
    own_width, model = attn[0].shape[-2:]
    own_hidden = ffn[0].shape[-2]
    attn_count = sum(grad.shape[0] for grad in attn)
    ffn_count = sum(grad.shape[0] for grad in ffn)
    dma = pltpu.SemaphoreType.DMA
    in_place = pl.BlockSpec(memory_space=pl.ANY)
    held = pl.BlockSpec(memory_space=pltpu.VMEM)
    chunks = [Chunk(i, own_width, own_hidden) for i in (0, 2)]

    def both(*shape_of):
        return [
            pltpu.VMEM((2,) + tuple(s(c) if callable(s) else s for s in shape_of), low)
            for c in chunks
        ]

    def k(chunk):
        return chunk.k

    def rows(chunk):
        return chunk.rows

    sem_shapes = ((4, 2 * quarters), (4, quarters), (4, 2), (4, mem), (4, quarters), (4, quarters), (3, mem), (mem + block,))
    sems = [dma((5, 2 * quarters))]
    for shape in sem_shapes:
        sems += [dma(shape), dma(shape)]
    return pl.pallas_call(
        reduce_body,
        in_specs=[in_place] * (len(attn) + len(ffn)) + [held, held, held, held],
        out_specs=[held, held, in_place, in_place, in_place, held],
        out_shape=[
            jax.ShapeDtypeStruct((attn_count, own_width, model), low),
            jax.ShapeDtypeStruct((ffn_count, own_hidden, model), low),
            jax.ShapeDtypeStruct((mem, memory.shape[0]) + memory.shape[2:], low),
            jax.ShapeDtypeStruct(first.shape, low),
            jax.ShapeDtypeStruct(second.shape, low),
            jax.ShapeDtypeStruct(small.shape[1:], wide),
        ],
        scratch_shapes=both(quarters, k, mem, rows, model)
        + both(quarters, k, mem, rows, model)
        + both(2, 2, k, mem // 2, rows, model)
        + both(2, k, mem // 2, rows, model)
        + both(mem, k, rows, model)
        + [pltpu.VMEM((mem,) + small.shape[1:], wide), pltpu.VMEM((block,) + small.shape[1:], wide)]
        + sems,
        compiler_params=pltpu.CompilerParams(collective_id=1, has_side_effects=True),
    )(*attn, *ffn, memory, first, second, small)


def sum_blocks(values):
    bit = block
    while bit < lax.axis_size("rows"):
        values = values + flip(values, bit)
        bit *= 2
    return values


def dot(left, right, left_dim, right_dim):
    return lax.dot_general(
        left, right, (((left_dim,), (right_dim,)), ((), ())), preferred_element_type=wide
    )


def lanes_of(half):
    lane = lax.broadcasted_iota(jnp.int32, (1, pair), 1)
    return ((lane // head_size) == half).astype(wide)


def skewed(row, height):
    spread = jnp.broadcast_to(row, (height, row.shape[1]))
    return pltpu.roll(spread, 0, 1, stride=1, stride_axis=0)


def causal_mask(same):
    rows, keys = same.shape
    i = lax.broadcasted_iota(jnp.int32, (rows, keys), 0)
    j = lax.broadcasted_iota(jnp.int32, (rows, keys), 1)
    return same & (i >= j)


def attend_pair(queries, keys_in, values_in, allowed, bias):
    rows, keys = allowed.shape
    kept = []
    mixed = jnp.zeros((rows, pair), wide)
    for half in range(2):
        lanes = lanes_of(half)
        scores = dot(queries * lanes.astype(low), keys_in, 1, 1)
        if bias is not None:
            scores = scores + skewed(bias[half], rows)[:, :keys]
        scores = jnp.where(allowed, scores, negative)
        raised = jnp.exp(scores - jnp.max(scores, axis=-1, keepdims=True))
        scale = 1.0 / jnp.sum(raised, axis=-1, keepdims=True)
        weights = (raised * scale).astype(low)
        kept.append(weights)
        mixed = mixed + dot(weights, values_in, 1, 0) * lanes
    return kept, mixed.astype(low)


def attend_back_body(causal, w_ref, q_ref, k_ref, v_ref, g_ref, *rest):
    if causal:
        out_ref, dist_ref = rest
    else:
        dq_ref, dkv_ref = rest
    queries, keys_in, values_in, grad = q_ref[0], k_ref[0], v_ref[0], g_ref[0]
    rows, keys = queries.shape[0], keys_in.shape[0]
    dq = jnp.zeros((rows, pair), wide)
    dk = jnp.zeros((keys, pair), wide)
    dv = jnp.zeros((keys, pair), wide)
    for half in range(2):
        lanes = lanes_of(half)
        weights = w_ref[0, half]
        weights_wide = weights.astype(wide)
        grad_weights = dot(grad * lanes.astype(low), values_in, 1, 1)
        inner = jnp.sum(grad_weights * weights_wide, axis=-1, keepdims=True)
        grad_scores = (weights_wide * (grad_weights - inner)).astype(low)
        dv = dv + dot(weights, grad, 0, 0) * lanes
        dq = dq + dot(grad_scores, keys_in, 1, 0) * lanes
        dk = dk + dot(grad_scores, queries, 0, 0) * lanes
        if causal:
            width = dist_ref.shape[-1]
            i = lax.broadcasted_iota(jnp.int32, (rows, rows), 0)
            j = lax.broadcasted_iota(jnp.int32, (rows, rows), 1)
            upside_down = dot((i + j == rows - 1).astype(wide).astype(low), grad_scores, 1, 0)
            padded = jnp.concatenate(
                [upside_down, jnp.zeros((rows, width - keys), wide)], axis=1
            )
            turned = pltpu.roll(padded, 0, 1, stride=1, stride_axis=0)
            dist_ref[0, 0, half : half + 1, :] = jnp.sum(turned, axis=0, keepdims=True)
    if causal:
        out_ref[0, 0] = dq.astype(low)
        out_ref[0, 1] = dk.astype(low)
        out_ref[0, 2] = dv.astype(low)
    else:
        dq_ref[0] = dq.astype(low)
        dkv_ref[0, 0] = dk.astype(low)
        dkv_ref[0, 1] = dv.astype(low)


def column(length, k=None):
    if k is None:
        return pl.BlockSpec((1, length, pair), lambda r, p: (r, 0, p))
    return pl.BlockSpec((None, 1, length, pair), lambda r, p: (k, r, 0, p))


def cost_of(count, rows, keys, pairs, dots):
    return pl.CostEstimate(
        flops=count * pairs * 2 * dots * 2 * rows * keys * pair,
        bytes_accessed=count * pairs * (2 * rows * keys * 2 + 4 * keys * pair * 2),
        transcendentals=count * pairs * 2 * rows * keys,
    )


def attend_back(weights, queries, keys_in, values_in, grad, dist_width):
    count, heads, rows, keys = weights.shape
    pairs = heads // 2
    width = pairs * pair
    causal = dist_width is not None
    if causal:
        out_specs = [
            pl.BlockSpec((1, 3, rows, pair), lambda r, p: (r, 0, 0, p)),
            pl.BlockSpec((1, 1, 2, dist_width), lambda r, p: (r, p, 0, 0)),
        ]
        out_shape = [
            jax.ShapeDtypeStruct((count, 3, rows, width), low),
            jax.ShapeDtypeStruct((count, pairs, 2, dist_width), wide),
        ]
    else:
        out_specs = [
            column(rows),
            pl.BlockSpec((1, 2, keys, pair), lambda r, p: (r, 0, 0, p)),
        ]
        out_shape = [
            jax.ShapeDtypeStruct((count, rows, width), low),
            jax.ShapeDtypeStruct((count, 2, keys, width), low),
        ]
    return pl.pallas_call(
        partial(attend_back_body, causal),
        grid=(count, pairs),
        in_specs=[
            pl.BlockSpec((1, 2, rows, keys), lambda r, p: (r, p, 0, 0)),
            column(rows, queries[1]),
            column(keys, keys_in[1]),
            column(keys, values_in[1]),
            column(rows),
        ],
        out_specs=out_specs,
        out_shape=out_shape,
        cost_estimate=cost_of(count, rows, keys, pairs, 4),
    )(weights, queries[0], keys_in[0], values_in[0], grad)


def rms(values, gain):
    scale = lax.rsqrt(jnp.mean(values * values, axis=-1, keepdims=True) + epsilon)
    return (values * scale * gain).astype(low), scale


def rms_back(values, scale, gain, grad):
    grad_gain = jnp.sum(grad * values * scale, axis=(0, 1))
    scaled = grad * gain
    inner = jnp.mean(scaled * values, axis=-1, keepdims=True)
    return scaled * scale - values * (scale * scale * scale * inner), grad_gain


def times_t(values, weight):
    return jnp.einsum("rtd,cd->rtc", values, weight, preferred_element_type=wide)


def times(values, weight):
    return jnp.einsum("rtc,cd->rtd", values, weight, preferred_element_type=wide)


def weight_grad(grads, values):
    return jnp.einsum("rtc,rtd->cd", grads, values, preferred_element_type=wide).astype(low)


def gated(gate, upward):
    return jax.nn.gelu(gate, approximate=True) * upward


def shards(
    dec_input,
    enc_output,
    dec_segments,
    enc_segments,
    buckets,
    gains,
    self_query,
    self_kv,
    self_out,
    rel_table,
    cross_query,
    cross_kv,
    cross_out,
    ffn_in,
    ffn_out,
    cotangent,
):
    mem = lax.axis_size("mem")
    me = lax.axis_index("mem")
    group, dec_len, model = dec_input.shape
    count = group // mem
    own_heads = rel_table.shape[1]
    own_width = self_query.shape[1]
    width = own_width * mem
    pairs = width // pair
    own_hidden = ffn_out.shape[0]
    gain_values = gains.astype(wide)
    bucket_count = rel_table.shape[0]

    attn_shard = jnp.stack(
        [self_query.T, self_kv[0].T, self_kv[1].T, self_out]
        + [cross_query.T, cross_kv[0].T, cross_kv[1].T, cross_out]
    )
    ffn_shard = jnp.stack([ffn_in[0].T, ffn_in[1].T, ffn_out])
    padded_table = jnp.pad(rel_table, ((0, 0), (0, pair - own_heads)))

    def mine(values):
        return lax.dynamic_slice_in_dim(values, me * count, count, 0)

    own_input = mine(dec_input)
    inputs = own_input.astype(wide)
    grad_out = mine(cotangent)
    dec_ids = mine(dec_segments)
    enc_ids = jnp.concatenate(relative(mine(enc_segments), 1, mem), axis=1)
    enc_len = enc_ids.shape[1]

    lane_count = -(-dec_len // pair) * pair
    turned = jnp.concatenate(
        [
            buckets[:1],
            jnp.full((lane_count - dec_len,), -1, buckets.dtype),
            jnp.flip(buckets[1:]),
        ]
    )
    spread = (jnp.arange(bucket_count)[:, None] == turned[None, :]).astype(low)

    normed_one, scale_one = rms(inputs, gain_values[0])
    (
        attn_weights, in_weight, out_weight, memory,
        qkv, self_mixed, self_weights, first, normed_two,
        cross_queries, cross_sides, cross_mixed, cross_weights,
    ) = gather_all(
        attn_shard, ffn_shard, enc_output, padded_table,
        own_input, normed_one, gain_values, dec_ids, enc_ids, spread,
    )
    attn_weights = attn_weights.reshape(-1, width, model)
    in_weight = in_weight.reshape(-1, model)
    out_weight = out_weight.reshape(-1, model)
    memory = memory.reshape(count, -1, model)
    qkv_weight = attn_weights[:3]
    self_out_weight = attn_weights[3]
    cross_query_weight = attn_weights[4]
    cross_kv_weight = attn_weights[5:7]
    cross_out_weight = attn_weights[7]
    scale_two = rms(first, gain_values[1])[1]
    second = first + times(cross_mixed, cross_out_weight)
    normed_three, scale_three = rms(second, gain_values[2])

    hidden_width = mem * own_hidden
    gate_up = times_t(normed_three, in_weight)
    hidden_float, pull = jax.vjp(gated, gate_up[..., :hidden_width], gate_up[..., hidden_width:])
    hidden = hidden_float.astype(low)
    output = second + times(hidden, out_weight)
    grad_gate, grad_up = pull(times_t(grad_out, out_weight))
    grad_gate_up = jnp.concatenate([grad_gate.astype(low), grad_up.astype(low)], axis=-1)
    grad_three = times(grad_gate_up, in_weight)
    ffn_grads = [
        grad.reshape(-1, mem, own_hidden, model)
        for grad in (weight_grad(grad_gate_up, normed_three), weight_grad(hidden, grad_out))
    ]

    grad_wide = grad_out.astype(wide)
    back, gain_three = rms_back(second, scale_three, gain_values[2], grad_three)
    grad_second = grad_wide + back
    grad_second_low = grad_second.astype(low)
    grad_cross_mixed = times_t(grad_second_low, cross_out_weight).astype(low)
    grad_cross_out = weight_grad(cross_mixed, grad_second_low)
    cross_dq, cross_dkv = attend_back(
        cross_weights,
        (cross_queries, None),
        (cross_sides, 0),
        (cross_sides, 1),
        grad_cross_mixed,
        None,
    )
    grad_cross_query = weight_grad(cross_dq, normed_two)
    grad_cross_kv = jnp.einsum(
        "rmsc,rsd->mcd", cross_dkv, memory, preferred_element_type=wide
    ).astype(low)
    grad_memory = jnp.einsum(
        "rmsc,mcd->rsd",
        cross_dkv,
        cross_kv_weight,
        preferred_element_type=wide,
    ).astype(low)
    back, gain_two = rms_back(
        first, scale_two, gain_values[1], times(cross_dq, cross_query_weight)
    )
    grad_first = grad_second + back
    grad_first_low = grad_first.astype(low)
    grad_self_mixed = times_t(grad_first_low, self_out_weight).astype(low)
    grad_self_out = weight_grad(self_mixed, grad_first_low)
    self_grads, distance_sums = attend_back(
        self_weights, (qkv, 0), (qkv, 1), (qkv, 2), grad_self_mixed, lane_count
    )
    grad_qkv = jnp.einsum(
        "rmtc,rtd->mcd", self_grads, normed_one, preferred_element_type=wide
    ).astype(low)
    attn_grads = [
        grad.reshape(-1, mem, own_width, model)
        for grad in (grad_qkv, grad_self_out, grad_cross_query, grad_cross_kv, grad_cross_out)
    ]
    grad_one = jnp.einsum(
        "rmtc,mcd->rtd",
        self_grads,
        qkv_weight,
        preferred_element_type=wide,
    )
    back, gain_one = rms_back(inputs, scale_one, gain_values[0], grad_one)
    grad_input = grad_first + back

    def one_hot_of(ids):
        return (ids[:, None] == jnp.arange(bucket_count)[None, :]).astype(wide)

    falling = jnp.concatenate(
        [jnp.flip(buckets), jnp.full((lane_count - dec_len,), -1, buckets.dtype)]
    )
    grad_table = jnp.einsum(
        "lb,hl->hb",
        one_hot_of(falling),
        jnp.sum(distance_sums, axis=0).reshape(2 * pairs, lane_count),
        precision=highest,
    )
    gain_grads = jnp.concatenate(
        relative(jnp.stack([gain_one, gain_two, gain_three]), 1, mem), axis=0
    ).reshape(mem, 3 * own_width)
    small = jnp.concatenate(
        [gain_grads, grad_table.reshape(mem, own_heads * bucket_count)], axis=1
    )
    small_size = small.shape[1]
    small = jnp.pad(small, ((0, 0), (0, 8 * pair - small_size))).reshape(mem, 8, pair)
    attn_sums, ffn_sums, grad_memory, output, grad_input, small = reduce_all(
        attn_grads,
        ffn_grads,
        grad_memory.reshape(count, mem, enc_len // mem, model),
        jnp.stack(relative(output.astype(low), 1, mem)),
        jnp.stack(relative(grad_input.astype(low), 1, mem)),
        small,
    )
    attn_sums = sum_blocks(attn_sums).astype(wide)
    ffn_sums = sum_blocks(ffn_sums).astype(wide)
    small = sum_blocks(small).reshape(-1)
    split = 3 * own_width

    def columns(values):
        return jnp.swapaxes(values, -1, -2)

    return (
        output.reshape(group, -1, model).astype(wide),
        grad_input.reshape(group, -1, model).astype(wide),
        grad_memory.reshape(group, -1, model).astype(wide),
        small[:split].reshape(3, own_width),
        columns(attn_sums[0]),
        columns(attn_sums[1:3]),
        attn_sums[3],
        small[split:small_size].reshape(own_heads, bucket_count).T,
        columns(attn_sums[4]),
        columns(attn_sums[5:7]),
        attn_sums[7],
        columns(ffn_sums[:2]),
        ffn_sums[2],
    )


def solution(mesh):
    in_specs = (
        P("rows", None, None),
        P("rows", "mem", None),
        P("rows", None),
        P("rows", None),
        P(),
        P(),
        P(None, "mem"),
        P(None, None, "mem"),
        P("mem", None),
        P(None, "mem"),
        P(None, "mem"),
        P(None, None, "mem"),
        P("mem", None),
        P(None, None, "mem"),
        P("mem", None),
        P("rows", None, None),
    )
    out_specs = (
        P("rows", "mem", None),
        P("rows", "mem", None),
        P("rows", "mem", None),
        P(None, "mem"),
        P(None, "mem"),
        P(None, None, "mem"),
        P("mem", None),
        P(None, "mem"),
        P(None, "mem"),
        P(None, None, "mem"),
        P("mem", None),
        P(None, None, "mem"),
        P("mem", None),
    )
    return jax.shard_map(shards, mesh=mesh, in_specs=in_specs, out_specs=out_specs, check_vma=False)
```

```python
from functools import partial

import jax
import jax.numpy as jnp
from jax import lax
from jax.experimental import pallas as pl
from jax.experimental.pallas import tpu as pltpu
from jax.sharding import PartitionSpec as P

epsilon = 1e-06
negative = -1e30
highest = lax.Precision.HIGHEST
low = jnp.bfloat16
wide = jnp.float32
pair = 128
head_size = 64


def flip(values, bit):
    size = lax.axis_size("rows")
    return lax.ppermute(values, "rows", [(i, i ^ bit) for i in range(size)])


def relative(values, axis, count):
    me = lax.axis_index("mem")
    size = values.shape[axis] // count
    return [
        lax.dynamic_slice_in_dim(values, ((me + step) % count) * size, size, axis)
        for step in range(count)
    ]


block = 8
quarters = 4
MESH = pl.DeviceIdType.MESH


class Place:
    def __init__(self):
        rows = lax.axis_index("rows")
        self.base = (rows // block) * block
        inner = rows - self.base
        self.core = inner % 2
        self.quarter = inner // 2
        self.near = self.quarter % 2
        self.far = self.quarter // 2
        self.me = lax.axis_index("mem")
        self.mem = lax.axis_size("mem")

    def at(self, quarter, core):
        return (self.base + quarter * 2 + core, self.me)

    def other_core(self):
        return self.at(self.quarter, 1 - self.core)

    def other_quarter(self, step):
        return self.at(self.turn(step), self.core)

    def turn(self, step):
        near = (self.near + step % 2) % 2
        far = (self.far + step // 2) % 2
        return far * 2 + near

    def along(self, step):
        rows = self.base + self.quarter * 2 + self.core
        return (rows, (self.me + step) % self.mem)

    def greet(self):
        barrier = pltpu.get_barrier_semaphore()
        count = 0
        for step in range(1, self.mem):
            pl.semaphore_signal(barrier, inc=1, device_id=self.along(step), device_id_type=MESH)
            count += 1
        for quarter in range(quarters):
            for core in range(2):
                if quarter or core:
                    there = self.at(self.turn(quarter), (self.core + core) % 2)
                    pl.semaphore_signal(barrier, inc=1, device_id=there, device_id_type=MESH)
                    count += 1
        pl.semaphore_wait(barrier, count)


def send(source, target, sems, index, there, arrival=None):
    copy = pltpu.make_async_remote_copy(
        src_ref=source,
        dst_ref=target,
        send_sem=sems[0].at[index],
        recv_sem=sems[1].at[index if arrival is None else arrival],
        device_id=there,
        device_id_type=MESH,
    )
    copy.start()
    return copy


def expect(buffer, sems, index, place):
    pltpu.make_async_remote_copy(
        src_ref=buffer,
        dst_ref=buffer,
        send_sem=sems[0].at[index],
        recv_sem=sems[1].at[index],
        device_id=place.other_core(),
        device_id_type=MESH,
    ).wait_recv()


class Chunk:
    def __init__(self, index, own_width, own_hidden):
        self.index = index
        self.is_ffn = index >= 2
        self.part = index % 2
        if self.is_ffn:
            self.k = 3
            self.rows = own_hidden // 16
        else:
            self.k = 1
            self.rows = own_width // 2

    def spot(self, quarter, core):
        if self.is_ffn:
            start = ((quarter * 2 + self.part) * 2 + core) * self.rows
            return pl.ds(0, 3), pl.ds(pl.multiple_of(start, self.rows), self.rows)
        start = core * self.rows
        return (
            pl.ds(self.part * quarters + quarter, 1),
            pl.ds(pl.multiple_of(start, self.rows), self.rows),
        )

    def shard(self, refs, quarter, core):
        k, rows = self.spot(quarter, core)
        return refs[self.is_ffn].at[k, rows]

    def shards(self, refs, quarter, core):
        k, rows = self.spot(quarter, core)
        if self.is_ffn:
            return [refs[1].at[pl.ds(0, 2), rows], refs[1].at[pl.ds(2, 1), rows]]
        return [refs[0].at[k, rows]]

    def wholes(self, refs, steps, quarter, core):
        k, rows = self.spot(quarter, core)
        if self.is_ffn:
            return [refs[1].at[:, steps, rows], refs[2].at[:, steps, rows]]
        return [refs[0].at[k, steps, rows]]


def between_ends(step, me, mem):
    to = (me + step) % mem
    return jnp.logical_and(me - to < mem - 1, to - me < mem - 1)


def gather_body(
    attn_ref, ffn_ref, enc_ref, table_ref,
    input_ref, normed_ref, gain_ref, dec_row_ref, dec_column_ref, enc_row_ref, spread_ref,
    attn_out, in_out, down_out, memory_out,
    qkv_out, self_mixed_out, self_weights_out, first_out, normed_out,
    queries_out, sides_out, cross_mixed_out, cross_weights_out,
    own_enc, tables_out, bias_ref, weights_ref, memory_ref, local_sems, load_sems, far_send, far_recv, enc_send, enc_recv, table_send, table_recv,
    flat_send, flat_recv, core_send, core_recv,
):
    place = Place()
    mem = place.mem
    shards = (attn_ref, ffn_ref)
    wholes = (attn_out, in_out, down_out)
    count = own_enc.shape[0]
    chunks = [Chunk(i, attn_ref.shape[1], ffn_ref.shape[1]) for i in range(4)]
    locals_in = pltpu.make_async_copy(
        enc_ref.at[pl.ds(place.me * count, count)], own_enc, local_sems.at[0]
    )
    locals_in.start()
    locals_out = [
        pltpu.make_async_copy(attn_ref, attn_out.at[:, 0], local_sems.at[1]),
        pltpu.make_async_copy(ffn_ref.at[pl.ds(0, 2)], in_out.at[:, 0], local_sems.at[2]),
        pltpu.make_async_copy(ffn_ref.at[pl.ds(2, 1)], down_out.at[:, 0], local_sems.at[3]),
    ]
    for copy in locals_out:
        copy.start()
    tables_out[0] = table_ref[...]
    place.greet()
    sent = []
    waits = []

    def start_far(i):
        sources = chunks[i].shards(shards, place.quarter, place.core)
        for step in range(1, mem):
            back = mem - step
            targets = chunks[i].wholes(wholes, back, place.quarter, place.core)
            for j, (source, target) in enumerate(zip(sources, targets)):
                copy = pltpu.make_async_remote_copy(
                    src_ref=source, dst_ref=target,
                    send_sem=far_send.at[i, 2 * step + j], recv_sem=far_recv.at[i, 2 * back + j],
                    device_id=place.along(step), device_id_type=MESH,
                )
                direct = between_ends(step, place.me, mem)
                pl.when(direct)(copy.start)
                waits.append((direct, copy))

    def relay(i):
        for step, ahead in ((mem - 2, 1), (2, mem - 1)):
            there = (step - ahead) % mem
            at_turn = place.me == (mem - 2 if ahead == 1 else 1)
            sources = chunks[i].wholes(wholes, step, place.quarter, place.core)
            targets = chunks[i].wholes(wholes, there, place.quarter, place.core)
            for j, (source, target) in enumerate(zip(sources, targets)):
                copy = pltpu.make_async_remote_copy(
                    src_ref=source, dst_ref=target,
                    send_sem=far_send.at[i, 2 * mem + (ahead > 1) * 2 + j],
                    recv_sem=far_recv.at[i, 2 * there + j],
                    device_id=place.along(ahead), device_id_type=MESH,
                )
                pl.when(at_turn)(copy.start)
                waits.append((at_turn, copy))

    def start_enc():
        for step in range(1, mem):
            back = mem - step
            target = ((place.me + step) % mem) * count
            sent.append(
                send(
                    enc_ref.at[pl.ds(target, count)], memory_out.at[:, back],
                    (enc_send, enc_recv), step, place.along(step), back,
                )
            )

    def pieces(i, turn, core):
        return enumerate(chunks[i].wholes(wholes, pl.ds(1, mem - 1), place.turn(turn), core))

    def pass_on(i, turn):
        for j, piece in pieces(i, turn, place.core):
            sems = (core_send.at[i], core_recv.at[i])
            sent.append(send(piece, piece, sems, 2 * turn + j, place.other_core()))

    def finish_flat(i):
        for turn in range(1, quarters):
            for j, piece in pieces(i, turn, place.core):
                expect(piece, (flat_send.at[i], flat_recv.at[i]), 2 * turn + j, place)
            pass_on(i, turn)

    def pass_far(i):
        for step in (2, mem - 1, 1) if mem == 4 else range(1, mem):
            for j, piece in enumerate(chunks[i].wholes(wholes, step, place.quarter, place.core)):
                expect(piece, far_sems_of(i), 2 * step + j, place)
            if step == 2:
                relay(i)
        for j, piece in pieces(i, 0, place.core):
            sems = (flat_send.at[i], flat_recv.at[i])
            for turn in range(1, quarters):
                sent.append(send(piece, piece, sems, 2 * turn + j, place.other_quarter(turn)))
        pass_on(i, 0)

    def far_sems_of(i):
        return far_send.at[i], far_recv.at[i]

    def finish_core(i):
        for turn in range(quarters):
            for j, piece in pieces(i, turn, 1 - place.core):
                expect(piece, (core_send.at[i], core_recv.at[i]), 2 * turn + j, place)

    def bring(source, target):
        copy = pltpu.make_async_copy(source, target, load_sems.at[0])
        copy.start()
        copy.wait()

    def weight(k):
        return weights_ref[k].reshape(-1, model)

    model = attn_ref.shape[2]
    rows, dec_len, _ = input_ref.shape
    enc_len = mem * memory_ref.shape[2]
    pairs = model // pair
    own_heads = model // head_size // mem

    start_far(0)
    for step in range(1, mem):
        back = mem - step
        sent.append(
            send(table_ref, tables_out.at[back], (table_send, table_recv), step, place.along(step), back)
        )
    for i in range(1, 4):
        start_far(i)
    pass_far(0)
    for step in range(1, mem):
        expect(tables_out.at[step], (table_send, table_recv), step, place)
    for step in range(mem):
        per_lane = dot(tables_out[step], spread_ref[...], 0, 0)
        for head in range(own_heads):
            bias_ref[step * own_heads + head] = per_lane[head : head + 1]
    pass_far(1)
    start_enc()
    finish_flat(0)
    pass_far(2)
    finish_core(0)
    for copy in locals_out:
        copy.wait()
    bring(attn_out.at[pl.ds(0, quarters)], weights_ref)

    def project_self(k, carry):
        values = dot(normed_ref[...].reshape(-1, model), weight(k), 1, 1)
        qkv_out[k] = values.astype(low).reshape(rows, dec_len, model)
        return carry

    lax.fori_loop(0, 3, project_self, 0)
    pass_far(3)

    def lanes_at(p):
        return pl.ds(pl.multiple_of(p * pair, pair), pair)

    def self_row(r):
        allowed = causal_mask(dec_column_ref[r] == dec_row_ref[r])

        def step(p, carry):
            weights, mixed = attend_pair(
                qkv_out[0, r, :, lanes_at(p)],
                qkv_out[1, r, :, lanes_at(p)],
                qkv_out[2, r, :, lanes_at(p)],
                allowed,
                [bias_ref[2 * p], bias_ref[2 * p + 1]],
            )
            for half in range(2):
                self_weights_out[r, 2 * p + half] = weights[half]
            self_mixed_out[r, :, lanes_at(p)] = mixed
            return carry

        lax.fori_loop(0, pairs, step, 0)

    def cross_row(r):
        allowed = dec_column_ref[r] == enc_row_ref[r]

        def step(p, carry):
            weights, mixed = attend_pair(
                queries_out[r, :, lanes_at(p)],
                sides_out[0, r, :, lanes_at(p)],
                sides_out[1, r, :, lanes_at(p)],
                allowed,
                None,
            )
            for half in range(2):
                cross_weights_out[r, 2 * p + half] = weights[half]
            cross_mixed_out[r, :, lanes_at(p)] = mixed
            return carry

        lax.fori_loop(0, pairs, step, 0)

    for r in range(rows):
        self_row(r)
    finish_flat(1)
    added = dot(self_mixed_out[...].reshape(-1, model), weight(3), 1, 0)
    first = input_ref[...].astype(wide) + added.reshape(rows, dec_len, model)
    first_out[...] = first
    normed_out[...] = rms(first, gain_ref[1:2, :])[0]
    finish_core(1)
    bring(attn_out.at[pl.ds(quarters, quarters)], weights_ref)
    values = dot(normed_out[...].reshape(-1, model), weight(0), 1, 1)
    queries_out[...] = values.astype(low).reshape(rows, dec_len, model)
    finish_flat(2)
    locals_in.wait()
    own_out = pltpu.make_async_copy(own_enc, memory_out.at[:, 0], local_sems.at[0])
    own_out.start()
    for step in range(1, mem):
        expect(memory_out.at[:, step], (enc_send, enc_recv), step, place)
    own_out.wait()
    bring(memory_out, memory_ref)
    for k in range(2):

        def project_side(r, carry):
            values = dot(memory_ref[r].reshape(-1, model), weight(1 + k), 1, 1)
            sides_out[k, r] = values.astype(low)
            return carry

        lax.fori_loop(0, rows, project_side, 0)
    cross_row(0)
    finish_flat(3)
    for r in range(1, rows):
        cross_row(r)
    finish_core(2)
    finish_core(3)
    for copy in sent:
        copy.wait_send()
    for started, copy in waits:
        pl.when(started)(copy.wait_send)


def gather_all(attn, ffn, enc, table, inputs, normed, gains, dec_ids, enc_ids, spread):
    mem = lax.axis_size("mem")
    count, dec_len, model = inputs.shape
    enc_len = enc_ids.shape[1]
    heads = model // head_size
    dma = pltpu.SemaphoreType.DMA
    in_place = pl.BlockSpec(memory_space=pl.ANY)
    held = pl.BlockSpec(memory_space=pltpu.VMEM)
    operands = (
        attn, ffn, enc, table, inputs, normed, gains,
        dec_ids[:, None, :], dec_ids[:, :, None], enc_ids[:, None, :], spread,
    )

    def values(*shape, dtype=low):
        return jax.ShapeDtypeStruct(shape, dtype)

    return pl.pallas_call(
        gather_body,
        in_specs=[held, held, in_place] + [held] * (len(operands) - 3),
        out_specs=[in_place] * 4 + [held] * 9,
        out_shape=[
            values(attn.shape[0], mem, *attn.shape[1:]),
            values(2, mem, *ffn.shape[1:]),
            values(1, mem, *ffn.shape[1:]),
            values(count, mem, *enc.shape[1:]),
            values(3, count, dec_len, model),
            values(count, dec_len, model),
            values(count, heads, dec_len, dec_len),
            values(count, dec_len, model, dtype=wide),
            values(count, dec_len, model),
            values(count, dec_len, model),
            values(2, count, enc_len, model),
            values(count, dec_len, model),
            values(count, heads, dec_len, enc_len),
        ],
        scratch_shapes=[
            pltpu.VMEM((count,) + enc.shape[1:], low),
            pltpu.VMEM((mem,) + table.shape, low),
            pltpu.VMEM((heads, 1, spread.shape[1]), wide),
            pltpu.VMEM((quarters, mem) + attn.shape[1:], low),
            pltpu.VMEM((count, mem) + enc.shape[1:], low),
            dma((4,)), dma((1,)),
            dma((4, 2 * mem + 4)), dma((4, 2 * mem)),
            dma((mem,)), dma((mem,)),
            dma((mem,)), dma((mem,)),
            dma((4, 2 * quarters)), dma((4, 2 * quarters)),
            dma((4, 2 * quarters)), dma((4, 2 * quarters)),
        ],
        compiler_params=pltpu.CompilerParams(
            collective_id=0, has_side_effects=True, vmem_limit_bytes=60000000
        ),
    )(*operands)


def add_planes(total_ref, total_at, more_ref, more_at, k, steps):
    first, size = steps

    def plane(index, carry):
        i, d = index // size, index % size
        added = more_ref[more_at + (i, d)].astype(wide)
        here = total_at + (i, first + d)
        total_ref[here] = (total_ref[here].astype(wide) + added).astype(low)
        return carry

    lax.fori_loop(0, k * size, plane, 0)


class Reduction:
    def __init__(self, place, chunk, index, buffers, sems, out_ref, sent, parts_of):
        self.place, self.chunk, self.out_ref, self.sent = place, chunk, out_ref, sent
        self.held, self.core, self.near, self.last, self.far = (ref.at[index] for ref in buffers)
        self.local = sems[0].at[index]
        pairs = [(sems[j].at[index], sems[j + 1].at[index]) for j in range(1, len(sems), 2)]
        self.core_sems, self.near_sems, self.last_sems = pairs[:3]
        self.far_sems, self.flat_sems, self.pass_sems = pairs[3:]
        self.parts_of = parts_of
        self.loads = []
        self.half = place.mem // 2

    def begin(self):
        for quarter in range(quarters):
            for j, (source, first, planes) in enumerate(self.parts_of(quarter, self.place.core)):
                copy = pltpu.make_async_copy(
                    source, self.held.at[quarter, pl.ds(first, planes)],
                    self.local.at[2 * quarter + j],
                )
                copy.start()
                self.loads.append(copy)

    def to_core(self):
        for quarter in range(quarters):
            parts = self.parts_of(quarter, 1 - self.place.core)
            for j, (source, first, planes) in enumerate(parts):
                self.sent.append(
                    send(
                        source, self.core.at[quarter, pl.ds(first, planes)],
                        self.core_sems, 2 * quarter + j, self.place.other_core(),
                    )
                )

    def from_core(self):
        place, held, near, half = self.place, self.held, self.near, self.half
        for copy in self.loads:
            copy.wait()
        for quarter in range(quarters):
            parts = self.parts_of(quarter, place.core)
            for j, (_, first, planes) in enumerate(parts):
                landed = self.core.at[quarter, pl.ds(first, planes)]
                expect(landed, self.core_sems, 2 * quarter + j, place)
            add_planes(held, (quarter,), self.core, (quarter,), self.chunk.k, (0, place.mem))
        for bit in range(2):
            quarter = bit * 2 + (1 - place.near)
            source = held.at[quarter, :, pl.ds(0, half)]
            self.sent.append(
                send(source, near.at[0, bit], self.near_sems, bit, place.other_quarter(1))
            )
            quarter = (1 - place.far) * 2 + bit
            source = held.at[quarter, :, pl.ds(half, half)]
            self.sent.append(
                send(source, near.at[1, bit], self.near_sems, 2 + bit, place.other_quarter(2))
            )

    def from_near(self):
        place, held, near, half = self.place, self.held, self.near, self.half
        k = self.chunk.k
        for bit in range(2):
            expect(near.at[0, bit], self.near_sems, bit, place)
            add_planes(held, (bit * 2 + place.near,), near, (0, bit), k, (0, half))
            expect(near.at[1, bit], self.near_sems, 2 + bit, place)
            add_planes(held, (place.far * 2 + bit,), near, (1, bit), k, (half, half))
        quarter = (1 - place.far) * 2 + place.near
        source = held.at[quarter, :, pl.ds(0, half)]
        self.sent.append(send(source, self.last.at[0], self.last_sems, 0, place.other_quarter(2)))
        quarter = place.far * 2 + (1 - place.near)
        source = held.at[quarter, :, pl.ds(half, half)]
        self.sent.append(send(source, self.last.at[1], self.last_sems, 1, place.other_quarter(1)))

    def from_last(self):
        place, half = self.place, self.half
        for part in range(2):
            expect(self.last.at[part], self.last_sems, part, place)
            steps = (part * half, half)
            add_planes(self.held, (place.quarter,), self.last, (part,), self.chunk.k, steps)
        for step in range(1, place.mem):
            back = place.mem - step
            source = self.held.at[place.quarter, :, step]
            self.sent.append(
                send(source, self.far.at[back], self.far_sems, step, place.along(step), back)
            )

    def from_far(self):
        place = self.place
        for step in range(1, place.mem):
            expect(self.far.at[step], self.far_sems, step, place)
        k_at, rows_at = self.chunk.spot(place.quarter, place.core)
        for k in range(self.chunk.k):
            total = self.held[place.quarter, k, 0].astype(wide)
            for step in range(1, place.mem):
                total = total + self.far[step, k].astype(wide)
            self.out_ref[k_at.start + k, rows_at, :] = total.astype(low)
        piece = self.piece(place.quarter, place.core)
        for turn in range(1, quarters):
            self.sent.append(send(piece, piece, self.flat_sems, turn, place.other_quarter(turn)))
        self.sent.append(send(piece, piece, self.pass_sems, 0, place.other_core()))

    def piece(self, quarter, core):
        k, rows = self.chunk.spot(quarter, core)
        return self.out_ref.at[k, rows]

    def from_flat(self):
        place = self.place
        for turn in range(1, quarters):
            piece = self.piece(place.turn(turn), place.core)
            expect(piece, self.flat_sems, turn, place)
            self.sent.append(send(piece, piece, self.pass_sems, turn, place.other_core()))

    def from_pass(self):
        place = self.place
        for turn in range(quarters):
            piece = self.piece(place.turn(turn), 1 - place.core)
            expect(piece, self.pass_sems, turn, place)


def reduction_scratch(chunk, mem, model):
    k, rows = chunk.k, chunk.rows

    def room(*shape):
        return pltpu.VMEM((2,) + shape + (rows, model), low)

    buffers = [
        room(quarters, k, mem),
        room(quarters, k, mem),
        room(2, 2, k, mem // 2),
        room(2, k, mem // 2),
        room(mem, k),
    ]
    sems = [pltpu.SemaphoreType.DMA((2, 2 * quarters))]
    for count in (2 * quarters, quarters, 2, mem, quarters, quarters):
        sems += [pltpu.SemaphoreType.DMA((2, count)) for _ in range(2)]
    return buffers + sems


buffer_count = 5
reduction_refs = 18


def start_moves(place, moves, sems, local_sems):
    sent, stays = [], []
    for index, (source, target) in enumerate(moves):
        copy = pltpu.make_async_copy(source(0), target.at[place.me], local_sems.at[index])
        copy.start()
        stays.append(copy)
        for step in range(1, place.mem):
            sent.append(
                send(
                    source(step), target.at[place.me],
                    (sems[0].at[index], sems[1].at[index]),
                    step, place.along(step), place.mem - step,
                )
            )
    return sent, stays


def finish_moves(place, moves, sems, stays):
    for index, (_, target) in enumerate(moves):
        for step in range(1, place.mem):
            expect(
                target.at[(place.me + step) % place.mem],
                (sems[0].at[index], sems[1].at[index]), step, place,
            )
    for copy in stays:
        copy.wait()


def reduce_body(
    qkv_ref, self_out_ref, query_ref, kv_ref, cross_out_ref,
    memory_ref, second_ref, small_ref,
    attn_out, memory_out, second_out, small_out,
    small_far, small_flat, stay_sems, move_send, move_recv, small_send, small_recv,
    *scratch,
):
    place = Place()
    mem = place.mem
    grads = [(qkv_ref, 0), (qkv_ref, 1), (qkv_ref, 2), (self_out_ref, 0)]
    grads += [(query_ref, 0), (kv_ref, 0), (kv_ref, 1), (cross_out_ref, 0)]
    sent = []

    def reduction(part):
        chunk = Chunk(part, attn_out.shape[1], 0)

        def parts_of(quarter, core):
            ref, at = grads[part * quarters + quarter]
            return [(ref.at[pl.ds(at, 1), :, chunk.spot(quarter, core)[1]], 0, 1)]

        return Reduction(
            place, chunk, part, scratch[:buffer_count], scratch[buffer_count:], attn_out, sent,
            parts_of,
        )

    order = [reduction(1), reduction(0)]
    moves = (
        (lambda step: memory_ref.at[:, step], memory_out),
        (lambda step: second_ref.at[step], second_out),
    )
    for chunk in order:
        chunk.begin()
    place.greet()
    for chunk in order:
        chunk.to_core()
    for step in range(1, mem):
        back = mem - step
        sent.append(
            send(small_ref.at[step], small_far.at[back], (small_send, small_recv), step, place.along(step), back)
        )
    moving, stays = start_moves(place, moves, (move_send, move_recv), stay_sems)
    sent += moving
    phases = ("from_core", "from_near", "from_last", "from_far", "from_flat", "from_pass")
    for time in range(len(order) + len(phases) - 1):
        for slot in reversed(range(len(order))):
            if 0 <= time - slot < len(phases):
                getattr(order[slot], phases[time - slot])()
        if time == 1:
            small = small_ref[0]
            for step in range(1, mem):
                expect(small_far.at[step], (small_send, small_recv), step, place)
                small = small + small_far[step]
            small_flat[0] = small
            for turn in range(1, block):
                there = place.at(place.turn(turn // 2), (place.core + turn % 2) % 2)
                sent.append(
                    send(small_flat.at[0], small_flat.at[turn], (small_send, small_recv), mem + turn, there)
                )
    small = small_flat[0]
    for turn in range(1, block):
        expect(small_flat.at[turn], (small_send, small_recv), mem + turn, place)
        small = small + small_flat[turn]
    small_out[...] = small
    finish_moves(place, moves, (move_send, move_recv), stays)
    for copy in sent:
        copy.wait_send()


def reduce_all(attn, memory, second, small):
    mem = lax.axis_size("mem")
    own_width, model = attn[0].shape[-2:]
    attn_count = sum(grad.shape[0] for grad in attn)
    dma = pltpu.SemaphoreType.DMA
    in_place = pl.BlockSpec(memory_space=pl.ANY)
    held = pl.BlockSpec(memory_space=pltpu.VMEM)
    return pl.pallas_call(
        reduce_body,
        in_specs=[in_place] * len(attn) + [held, held, held],
        out_specs=[held, in_place, in_place, held],
        out_shape=[
            jax.ShapeDtypeStruct((attn_count, own_width, model), low),
            jax.ShapeDtypeStruct((mem, memory.shape[0]) + memory.shape[2:], low),
            jax.ShapeDtypeStruct(second.shape, low),
            jax.ShapeDtypeStruct(small.shape[1:], wide),
        ],
        scratch_shapes=[
            pltpu.VMEM((mem,) + small.shape[1:], wide),
            pltpu.VMEM((block,) + small.shape[1:], wide),
            dma((2,)), dma((2, mem)), dma((2, mem)), dma((mem + block,)), dma((mem + block,)),
        ]
        + reduction_scratch(Chunk(0, own_width, 0), mem, model),
        compiler_params=pltpu.CompilerParams(collective_id=1, has_side_effects=True),
    )(*attn, memory, second, small)


def back_body(
    in_ref, down_ref, attn_weights_ref, cross_weights_ref, self_weights_ref, sides_in, qkv_in,
    output_ref, grad_second_ref, first_ref, input_ref, normed_one_ref, normed_two_ref,
    self_mixed_ref, cross_mixed_ref, queries_ref, memory_ref, gain_ref,
    ffn_out, output_out, qkv_grad_out, self_grad_out, query_grad_out, kv_grad_out,
    cross_grad_out, memory_out, input_out, gain_out, dist_out,
    weights_ref, cross_probs, self_probs, sides_ref, qkv_ref, mixed_grad_ref, query_grad_ref,
    load_sems, stay_sems, move_send, move_recv, *scratch,
):
    place = Place()
    sent = []
    rows, dec_len, model = input_ref.shape
    pairs = model // pair

    def reduction(part):
        chunk = Chunk(2 + part, 0, ffn_out.shape[1])

        def parts_of(quarter, core):
            at = chunk.spot(quarter, core)[1]
            return [(in_ref.at[:, :, at], 0, 2), (down_ref.at[:, :, at], 2, 1)]

        return Reduction(
            place, chunk, part, scratch[:buffer_count], scratch[buffer_count:], ffn_out, sent,
            parts_of,
        )

    one, two = reduction(0), reduction(1)
    loads = []
    for index, (source, target) in enumerate(
        (
            (attn_weights_ref.at[pl.ds(quarters, quarters)], weights_ref),
            (sides_in, sides_ref),
            (cross_weights_ref, cross_probs),
            (qkv_in, qkv_ref),
            (self_weights_ref, self_probs),
        )
    ):
        copy = pltpu.make_async_copy(source, target, load_sems.at[index])
        copy.start()
        loads.append(copy)
    one.begin()
    two.begin()
    place.greet()
    one.to_core()
    two.to_core()
    moves = ((lambda step: output_ref.at[step], output_out),)
    moving, stays = start_moves(place, moves, (move_send, move_recv), stay_sems)
    sent += moving

    def weight(k):
        return weights_ref[k].reshape(-1, model)

    def flat(values):
        return values.reshape(-1, model)

    def lanes_at(p):
        return pl.ds(pl.multiple_of(p * pair, pair), pair)

    grad_second = flat(grad_second_ref[...])
    grad_low = grad_second.astype(low)
    loads[0].wait()
    mixed_grad = dot(grad_low, weight(3), 1, 1).astype(low)
    mixed_grad_ref[...] = mixed_grad.reshape(rows, dec_len, model)
    cross_grad_out[...] = dot(flat(cross_mixed_ref[...]), grad_low, 0, 0).astype(low)
    one.from_core()
    two.from_core()
    loads[1].wait()
    loads[2].wait()

    def cross_row(r):
        def step(p, carry):
            at = lanes_at(p)
            dq, dk, dv, _ = attend_back_pair(
                [cross_probs[r, 2 * p], cross_probs[r, 2 * p + 1]],
                queries_ref[r, :, at], sides_ref[0, r, :, at], sides_ref[1, r, :, at],
                mixed_grad_ref[r, :, at], None,
            )
            query_grad_ref[r, :, at] = dq
            sides_ref[0, r, :, at] = dk
            sides_ref[1, r, :, at] = dv
            return carry

        lax.fori_loop(0, pairs, step, 0)

    cross_row(0)
    one.from_near()
    for r in range(1, rows):
        cross_row(r)
    query_grad = flat(query_grad_ref[...])
    query_grad_out[...] = dot(query_grad, flat(normed_two_ref[...]), 0, 0).astype(low)
    grad_two = dot(query_grad, weight(0), 1, 0)
    two.from_near()
    one.from_last()
    for k in range(2):
        kv_grad_out[k] = dot(flat(sides_ref[k]), flat(memory_ref[...]), 0, 0).astype(low)

    def encoder_row(r, carry):
        both = dot(sides_ref[0, r], weight(1), 1, 0) + dot(sides_ref[1, r], weight(2), 1, 0)
        memory_out[r] = both.astype(low)
        return carry

    lax.fori_loop(0, rows, encoder_row, 0)
    two.from_last()
    reload = pltpu.make_async_copy(
        attn_weights_ref.at[pl.ds(0, quarters)], weights_ref, load_sems.at[5]
    )
    reload.start()

    first = flat(first_ref[...])
    back, gain_two = rms_back_flat(first, gain_ref[1:2, :], grad_two)
    grad_first = grad_second + back
    grad_low = grad_first.astype(low)
    reload.wait()
    mixed_grad = dot(grad_low, weight(3), 1, 1).astype(low)
    mixed_grad_ref[...] = mixed_grad.reshape(rows, dec_len, model)
    self_grad_out[...] = dot(flat(self_mixed_ref[...]), grad_low, 0, 0).astype(low)
    input_out[...] = grad_first.reshape(rows, dec_len, model)
    loads[3].wait()
    loads[4].wait()

    def self_row(r):
        def step(p, carry):
            at = lanes_at(p)
            dq, dk, dv, dist = attend_back_pair(
                [self_probs[r, 2 * p], self_probs[r, 2 * p + 1]],
                qkv_ref[0, r, :, at], qkv_ref[1, r, :, at], qkv_ref[2, r, :, at],
                mixed_grad_ref[r, :, at], dist_out.shape[-1],
            )
            qkv_ref[0, r, :, at] = dq
            qkv_ref[1, r, :, at] = dk
            qkv_ref[2, r, :, at] = dv
            for half in range(2):
                dist_out[r, 2 * p + half] = dist[half]
            return carry

        lax.fori_loop(0, pairs, step, 0)

    self_row(0)
    one.from_far()
    for r in range(1, rows):
        self_row(r)
    two.from_far()
    one.from_flat()

    def project_back(k, carry):
        grads = flat(qkv_ref[k])
        qkv_grad_out[k] = dot(grads, flat(normed_one_ref[...]), 0, 0).astype(low)
        return carry

    lax.fori_loop(0, 3, project_back, 0)
    grad_one = jnp.zeros((rows * dec_len, model), wide)
    for k in range(3):
        grad_one = grad_one + dot(flat(qkv_ref[k]), weight(k), 1, 0)
    back, gain_one = rms_back_flat(flat(input_ref[...]).astype(wide), gain_ref[0:1, :], grad_one)
    input_out[...] = input_out[...] + back.reshape(rows, dec_len, model)
    gain_out[0:1, :] = gain_one
    gain_out[1:2, :] = gain_two
    two.from_flat()
    one.from_pass()
    two.from_pass()
    finish_moves(place, moves, (move_send, move_recv), stays)
    for copy in sent:
        copy.wait_send()


def back_all(
    ffn, attn_weights, cross_weights, self_weights, sides, qkv, output,
    grad_second, first, inputs, normed_one, normed_two, self_mixed, cross_mixed, queries,
    memory, gains, lane_count,
):
    mem = lax.axis_size("mem")
    own_hidden, model = ffn[0].shape[-2:]
    ffn_count = sum(grad.shape[0] for grad in ffn)
    count, heads, dec_len, _ = self_weights.shape
    dma = pltpu.SemaphoreType.DMA
    in_place = pl.BlockSpec(memory_space=pl.ANY)
    held = pl.BlockSpec(memory_space=pltpu.VMEM)

    def values(*shape, dtype=low):
        return jax.ShapeDtypeStruct(shape, dtype)

    return pl.pallas_call(
        back_body,
        in_specs=[in_place] * 7 + [held] * 11,
        out_specs=[held, in_place] + [held] * 9,
        out_shape=[
            values(ffn_count, own_hidden, model),
            values(*output.shape),
            values(3, model, model),
            values(model, model),
            values(model, model),
            values(2, model, model),
            values(model, model),
            values(*memory.shape),
            values(*inputs.shape, dtype=wide),
            values(2, model, dtype=wide),
            values(count, heads, 1, lane_count, dtype=wide),
        ],
        scratch_shapes=[
            pltpu.VMEM((quarters,) + attn_weights.shape[1:], low),
            pltpu.VMEM(cross_weights.shape, low),
            pltpu.VMEM(self_weights.shape, low),
            pltpu.VMEM(sides.shape, low),
            pltpu.VMEM(qkv.shape, low),
            pltpu.VMEM(inputs.shape, low),
            pltpu.VMEM(inputs.shape, low),
            dma((6,)), dma((1,)), dma((1, mem)), dma((1, mem)),
        ]
        + reduction_scratch(Chunk(2, 0, own_hidden), mem, model),
        compiler_params=pltpu.CompilerParams(
            collective_id=2, has_side_effects=True, vmem_limit_bytes=63000000
        ),
    )(
        *ffn, attn_weights, cross_weights, self_weights, sides, qkv, output,
        grad_second, first, inputs, normed_one, normed_two, self_mixed, cross_mixed, queries,
        memory, gains,
    )


def sum_blocks(values):
    bit = block
    while bit < lax.axis_size("rows"):
        values = values + flip(values, bit)
        bit *= 2
    return values


def dot(left, right, left_dim, right_dim):
    return lax.dot_general(
        left, right, (((left_dim,), (right_dim,)), ((), ())), preferred_element_type=wide
    )


def lanes_of(half):
    lane = lax.broadcasted_iota(jnp.int32, (1, pair), 1)
    return ((lane // head_size) == half).astype(wide)


def skewed(row, height):
    spread = jnp.broadcast_to(row, (height, row.shape[1]))
    return pltpu.roll(spread, 0, 1, stride=1, stride_axis=0)


def causal_mask(same):
    rows, keys = same.shape
    i = lax.broadcasted_iota(jnp.int32, (rows, keys), 0)
    j = lax.broadcasted_iota(jnp.int32, (rows, keys), 1)
    return same & (i >= j)


def attend_pair(queries, keys_in, values_in, allowed, bias):
    rows, keys = allowed.shape
    kept = []
    mixed = jnp.zeros((rows, pair), wide)
    for half in range(2):
        lanes = lanes_of(half)
        scores = dot(queries * lanes.astype(low), keys_in, 1, 1)
        if bias is not None:
            scores = scores + skewed(bias[half], rows)[:, :keys]
        scores = jnp.where(allowed, scores, negative)
        raised = jnp.exp(scores - jnp.max(scores, axis=-1, keepdims=True))
        scale = 1.0 / jnp.sum(raised, axis=-1, keepdims=True)
        weights = (raised * scale).astype(low)
        kept.append(weights)
        mixed = mixed + dot(weights, values_in, 1, 0) * lanes
    return kept, mixed.astype(low)


def attend_back_pair(weights_pair, queries, keys_in, values_in, grad, dist_width):
    rows, keys = weights_pair[0].shape
    dq = jnp.zeros((rows, pair), wide)
    dk = jnp.zeros((keys, pair), wide)
    dv = jnp.zeros((keys, pair), wide)
    dist = []
    for half in range(2):
        lanes = lanes_of(half)
        weights = weights_pair[half]
        weights_wide = weights.astype(wide)
        grad_weights = dot(grad * lanes.astype(low), values_in, 1, 1)
        inner = jnp.sum(grad_weights * weights_wide, axis=-1, keepdims=True)
        grad_scores = (weights_wide * (grad_weights - inner)).astype(low)
        dv = dv + dot(weights, grad, 0, 0) * lanes
        dq = dq + dot(grad_scores, keys_in, 1, 0) * lanes
        dk = dk + dot(grad_scores, queries, 0, 0) * lanes
        if dist_width is not None:
            i = lax.broadcasted_iota(jnp.int32, (rows, rows), 0)
            j = lax.broadcasted_iota(jnp.int32, (rows, rows), 1)
            upside_down = dot((i + j == rows - 1).astype(wide).astype(low), grad_scores, 1, 0)
            padded = jnp.concatenate(
                [upside_down, jnp.zeros((rows, dist_width - keys), wide)], axis=1
            )
            turned = pltpu.roll(padded, 0, 1, stride=1, stride_axis=0)
            dist.append(jnp.sum(turned, axis=0, keepdims=True))
    return dq.astype(low), dk.astype(low), dv.astype(low), dist


def rms_back_flat(values, gain, grad):
    scale = lax.rsqrt(jnp.mean(values * values, axis=-1, keepdims=True) + epsilon)
    grad_gain = jnp.sum(grad * values * scale, axis=0, keepdims=True)
    scaled = grad * gain
    inner = jnp.mean(scaled * values, axis=-1, keepdims=True)
    return scaled * scale - values * (scale * scale * scale * inner), grad_gain


def rms(values, gain):
    scale = lax.rsqrt(jnp.mean(values * values, axis=-1, keepdims=True) + epsilon)
    return (values * scale * gain).astype(low), scale


def rms_back(values, scale, gain, grad):
    grad_gain = jnp.sum(grad * values * scale, axis=(0, 1))
    scaled = grad * gain
    inner = jnp.mean(scaled * values, axis=-1, keepdims=True)
    return scaled * scale - values * (scale * scale * scale * inner), grad_gain


def times_t(values, weight):
    return jnp.einsum("rtd,cd->rtc", values, weight, preferred_element_type=wide)


def times(values, weight):
    return jnp.einsum("rtc,cd->rtd", values, weight, preferred_element_type=wide)


def weight_grad(grads, values):
    return jnp.einsum("rtc,rtd->cd", grads, values, preferred_element_type=wide).astype(low)


def gated(gate, upward):
    return jax.nn.gelu(gate, approximate=True) * upward


def shards(
    dec_input,
    enc_output,
    dec_segments,
    enc_segments,
    buckets,
    gains,
    self_query,
    self_kv,
    self_out,
    rel_table,
    cross_query,
    cross_kv,
    cross_out,
    ffn_in,
    ffn_out,
    cotangent,
):
    mem = lax.axis_size("mem")
    me = lax.axis_index("mem")
    group, dec_len, model = dec_input.shape
    count = group // mem
    own_heads = rel_table.shape[1]
    own_width = self_query.shape[1]
    width = own_width * mem
    pairs = width // pair
    own_hidden = ffn_out.shape[0]
    gain_values = gains.astype(wide)
    bucket_count = rel_table.shape[0]

    attn_shard = jnp.stack(
        [self_query.T, self_kv[0].T, self_kv[1].T, self_out]
        + [cross_query.T, cross_kv[0].T, cross_kv[1].T, cross_out]
    )
    ffn_shard = jnp.stack([ffn_in[0].T, ffn_in[1].T, ffn_out])
    padded_table = jnp.pad(rel_table, ((0, 0), (0, pair - own_heads)))

    def mine(values):
        return lax.dynamic_slice_in_dim(values, me * count, count, 0)

    own_input = mine(dec_input)
    inputs = own_input.astype(wide)
    grad_out = mine(cotangent)
    dec_ids = mine(dec_segments)
    enc_ids = jnp.concatenate(relative(mine(enc_segments), 1, mem), axis=1)
    enc_len = enc_ids.shape[1]

    lane_count = -(-dec_len // pair) * pair
    turned = jnp.concatenate(
        [
            buckets[:1],
            jnp.full((lane_count - dec_len,), -1, buckets.dtype),
            jnp.flip(buckets[1:]),
        ]
    )
    spread = (jnp.arange(bucket_count)[:, None] == turned[None, :]).astype(low)

    normed_one, scale_one = rms(inputs, gain_values[0])
    (
        attn_weights_in, in_weight, out_weight, memory,
        qkv, self_mixed, self_weights, first, normed_two,
        cross_queries, cross_sides, cross_mixed, cross_weights,
    ) = gather_all(
        attn_shard, ffn_shard, enc_output, padded_table,
        own_input, normed_one, gain_values, dec_ids, enc_ids, spread,
    )
    cross_out_weight = attn_weights_in[7].reshape(width, model)
    in_weight = in_weight.reshape(-1, model)
    out_weight = out_weight.reshape(-1, model)
    memory = memory.reshape(count, -1, model)
    second = first + times(cross_mixed, cross_out_weight)
    normed_three, scale_three = rms(second, gain_values[2])

    hidden_width = mem * own_hidden
    gate_up = times_t(normed_three, in_weight)
    hidden_float, pull = jax.vjp(gated, gate_up[..., :hidden_width], gate_up[..., hidden_width:])
    hidden = hidden_float.astype(low)
    output = second + times(hidden, out_weight)
    grad_gate, grad_up = pull(times_t(grad_out, out_weight))
    grad_gate_up = jnp.concatenate([grad_gate.astype(low), grad_up.astype(low)], axis=-1)
    grad_three = times(grad_gate_up, in_weight)
    ffn_grads = [
        grad.reshape(-1, mem, own_hidden, model)
        for grad in (weight_grad(grad_gate_up, normed_three), weight_grad(hidden, grad_out))
    ]

    grad_wide = grad_out.astype(wide)
    back, gain_three = rms_back(second, scale_three, gain_values[2], grad_three)
    grad_second = grad_wide + back
    (
        ffn_sums, output, grad_qkv, grad_self_out, grad_cross_query, grad_cross_kv,
        grad_cross_out, grad_memory, grad_input, gain_sums, distance_sums,
    ) = back_all(
        ffn_grads, attn_weights_in, cross_weights, self_weights, cross_sides, qkv,
        jnp.stack(relative(output.astype(low), 1, mem)),
        grad_second, first, own_input, normed_one, normed_two, self_mixed, cross_mixed,
        cross_queries, memory, gain_values, lane_count,
    )
    attn_grads = [
        grad.reshape(-1, mem, own_width, model)
        for grad in (grad_qkv, grad_self_out, grad_cross_query, grad_cross_kv, grad_cross_out)
    ]

    def one_hot_of(ids):
        return (ids[:, None] == jnp.arange(bucket_count)[None, :]).astype(wide)

    falling = jnp.concatenate(
        [jnp.flip(buckets), jnp.full((lane_count - dec_len,), -1, buckets.dtype)]
    )
    grad_table = jnp.einsum(
        "lb,hl->hb",
        one_hot_of(falling),
        jnp.sum(distance_sums, axis=0).reshape(2 * pairs, lane_count),
        precision=highest,
    )
    gain_grads = jnp.concatenate(
        relative(jnp.concatenate([gain_sums, gain_three[None]]), 1, mem), axis=0
    ).reshape(mem, 3 * own_width)
    small = jnp.concatenate(
        [gain_grads, grad_table.reshape(mem, own_heads * bucket_count)], axis=1
    )
    small_size = small.shape[1]
    small = jnp.pad(small, ((0, 0), (0, 8 * pair - small_size))).reshape(mem, 8, pair)
    attn_sums, grad_memory, grad_input, small = reduce_all(
        attn_grads,
        grad_memory.reshape(count, mem, enc_len // mem, model),
        jnp.stack(relative(grad_input.astype(low), 1, mem)),
        small,
    )
    attn_sums = sum_blocks(attn_sums).astype(wide)
    ffn_sums = sum_blocks(ffn_sums).astype(wide)
    small = sum_blocks(small).reshape(-1)
    split = 3 * own_width

    def columns(values):
        return jnp.swapaxes(values, -1, -2)

    return (
        output.reshape(group, -1, model).astype(wide),
        grad_input.reshape(group, -1, model).astype(wide),
        grad_memory.reshape(group, -1, model).astype(wide),
        small[:split].reshape(3, own_width),
        columns(attn_sums[0]),
        columns(attn_sums[1:3]),
        attn_sums[3],
        small[split:small_size].reshape(own_heads, bucket_count).T,
        columns(attn_sums[4]),
        columns(attn_sums[5:7]),
        attn_sums[7],
        columns(ffn_sums[:2]),
        ffn_sums[2],
    )


def solution(mesh):
    in_specs = (
        P("rows", None, None),
        P("rows", "mem", None),
        P("rows", None),
        P("rows", None),
        P(),
        P(),
        P(None, "mem"),
        P(None, None, "mem"),
        P("mem", None),
        P(None, "mem"),
        P(None, "mem"),
        P(None, None, "mem"),
        P("mem", None),
        P(None, None, "mem"),
        P("mem", None),
        P("rows", None, None),
    )
    out_specs = (
        P("rows", "mem", None),
        P("rows", "mem", None),
        P("rows", "mem", None),
        P(None, "mem"),
        P(None, "mem"),
        P(None, None, "mem"),
        P("mem", None),
        P(None, "mem"),
        P(None, "mem"),
        P(None, None, "mem"),
        P("mem", None),
        P(None, None, "mem"),
        P("mem", None),
    )
    return jax.shard_map(shards, mesh=mesh, in_specs=in_specs, out_specs=out_specs, check_vma=False)
```

```python
from functools import partial

import jax
import jax.numpy as jnp
from jax import lax
from jax.experimental import pallas as pl
from jax.experimental.pallas import tpu as pltpu
from jax.sharding import PartitionSpec as P

epsilon = 1e-06
negative = -1e30
highest = lax.Precision.HIGHEST
low = jnp.bfloat16
wide = jnp.float32
pair = 128
head_size = 64


def flip(values, bit):
    size = lax.axis_size("rows")
    return lax.ppermute(values, "rows", [(i, i ^ bit) for i in range(size)])


def relative(values, axis, count):
    me = lax.axis_index("mem")
    size = values.shape[axis] // count
    return [
        lax.dynamic_slice_in_dim(values, ((me + step) % count) * size, size, axis)
        for step in range(count)
    ]


block = 8
quarters = 4
MESH = pl.DeviceIdType.MESH


class Place:
    def __init__(self):
        rows = lax.axis_index("rows")
        self.base = (rows // block) * block
        inner = rows - self.base
        self.core = inner % 2
        self.quarter = inner // 2
        self.near = self.quarter % 2
        self.far = self.quarter // 2
        self.me = lax.axis_index("mem")
        self.mem = lax.axis_size("mem")

    def at(self, quarter, core):
        return (self.base + quarter * 2 + core, self.me)

    def other_core(self):
        return self.at(self.quarter, 1 - self.core)

    def other_quarter(self, step):
        return self.at(self.turn(step), self.core)

    def turn(self, step):
        near = (self.near + step % 2) % 2
        far = (self.far + step // 2) % 2
        return far * 2 + near

    def along(self, step):
        rows = self.base + self.quarter * 2 + self.core
        return (rows, (self.me + step) % self.mem)

    def greet(self):
        barrier = pltpu.get_barrier_semaphore()
        count = 0
        for step in range(1, self.mem):
            pl.semaphore_signal(barrier, inc=1, device_id=self.along(step), device_id_type=MESH)
            count += 1
        for quarter in range(quarters):
            for core in range(2):
                if quarter or core:
                    there = self.at(self.turn(quarter), (self.core + core) % 2)
                    pl.semaphore_signal(barrier, inc=1, device_id=there, device_id_type=MESH)
                    count += 1
        pl.semaphore_wait(barrier, count)


def send(source, target, sems, index, there, arrival=None):
    copy = pltpu.make_async_remote_copy(
        src_ref=source,
        dst_ref=target,
        send_sem=sems[0].at[index],
        recv_sem=sems[1].at[index if arrival is None else arrival],
        device_id=there,
        device_id_type=MESH,
    )
    copy.start()
    return copy


def expect(buffer, sems, index, place):
    pltpu.make_async_remote_copy(
        src_ref=buffer,
        dst_ref=buffer,
        send_sem=sems[0].at[index],
        recv_sem=sems[1].at[index],
        device_id=place.other_core(),
        device_id_type=MESH,
    ).wait_recv()


class Chunk:
    def __init__(self, index, own_width, own_hidden):
        self.index = index
        self.is_ffn = index >= 2
        self.part = index % 2
        if self.is_ffn:
            self.k = 3
            self.rows = own_hidden // 16
        else:
            self.k = 1
            self.rows = own_width // 2

    def spot(self, quarter, core):
        if self.is_ffn:
            start = ((quarter * 2 + self.part) * 2 + core) * self.rows
            return pl.ds(0, 3), pl.ds(pl.multiple_of(start, self.rows), self.rows)
        start = core * self.rows
        return (
            pl.ds(self.part * quarters + quarter, 1),
            pl.ds(pl.multiple_of(start, self.rows), self.rows),
        )

    def shard(self, refs, quarter, core):
        k, rows = self.spot(quarter, core)
        return refs[self.is_ffn].at[k, rows]

    def shards(self, refs, quarter, core):
        k, rows = self.spot(quarter, core)
        if self.is_ffn:
            return [refs[1].at[pl.ds(0, 2), rows], refs[1].at[pl.ds(2, 1), rows]]
        return [refs[0].at[k, rows]]

    def wholes(self, refs, steps, quarter, core):
        k, rows = self.spot(quarter, core)
        if self.is_ffn:
            return [refs[1].at[:, steps, rows], refs[2].at[:, steps, rows]]
        return [refs[0].at[k, steps, rows]]


def between_ends(step, me, mem):
    to = (me + step) % mem
    return jnp.logical_and(me - to < mem - 1, to - me < mem - 1)


def gather_body(
    attn_ref, ffn_ref, enc_ref, table_ref,
    input_ref, normed_ref, gain_ref, dec_row_ref, dec_column_ref, enc_row_ref, spread_ref,
    attn_out, in_out, down_out, memory_out,
    qkv_out, self_mixed_out, self_weights_out, first_out, normed_out,
    queries_out, sides_out, cross_mixed_out, cross_weights_out,
    own_enc, tables_out, bias_ref, weights_ref, memory_ref, local_sems, load_sems, far_send, far_recv, enc_send, enc_recv, table_send, table_recv,
    flat_send, flat_recv, core_send, core_recv,
):
    place = Place()
    mem = place.mem
    shards = (attn_ref, ffn_ref)
    wholes = (attn_out, in_out, down_out)
    count = own_enc.shape[0]
    chunks = [Chunk(i, attn_ref.shape[1], ffn_ref.shape[1]) for i in range(4)]
    locals_in = pltpu.make_async_copy(
        enc_ref.at[pl.ds(place.me * count, count)], own_enc, local_sems.at[0]
    )
    locals_in.start()
    locals_out = [
        pltpu.make_async_copy(attn_ref, attn_out.at[:, 0], local_sems.at[1]),
        pltpu.make_async_copy(ffn_ref.at[pl.ds(0, 2)], in_out.at[:, 0], local_sems.at[2]),
        pltpu.make_async_copy(ffn_ref.at[pl.ds(2, 1)], down_out.at[:, 0], local_sems.at[3]),
    ]
    for copy in locals_out:
        copy.start()
    tables_out[0] = table_ref[...]
    place.greet()
    sent = []
    waits = []

    def start_far(i):
        sources = chunks[i].shards(shards, place.quarter, place.core)
        for step in range(1, mem):
            back = mem - step
            targets = chunks[i].wholes(wholes, back, place.quarter, place.core)
            for j, (source, target) in enumerate(zip(sources, targets)):
                copy = pltpu.make_async_remote_copy(
                    src_ref=source, dst_ref=target,
                    send_sem=far_send.at[i, 2 * step + j], recv_sem=far_recv.at[i, 2 * back + j],
                    device_id=place.along(step), device_id_type=MESH,
                )
                direct = between_ends(step, place.me, mem)
                pl.when(direct)(copy.start)
                waits.append((direct, copy))

    def relay(i):
        for step, ahead in ((mem - 2, 1), (2, mem - 1)):
            there = (step - ahead) % mem
            at_turn = place.me == (mem - 2 if ahead == 1 else 1)
            sources = chunks[i].wholes(wholes, step, place.quarter, place.core)
            targets = chunks[i].wholes(wholes, there, place.quarter, place.core)
            for j, (source, target) in enumerate(zip(sources, targets)):
                copy = pltpu.make_async_remote_copy(
                    src_ref=source, dst_ref=target,
                    send_sem=far_send.at[i, 2 * mem + (ahead > 1) * 2 + j],
                    recv_sem=far_recv.at[i, 2 * there + j],
                    device_id=place.along(ahead), device_id_type=MESH,
                )
                pl.when(at_turn)(copy.start)
                waits.append((at_turn, copy))

    def start_enc():
        for step in range(1, mem):
            back = mem - step
            target = ((place.me + step) % mem) * count
            sent.append(
                send(
                    enc_ref.at[pl.ds(target, count)], memory_out.at[:, back],
                    (enc_send, enc_recv), step, place.along(step), back,
                )
            )

    def pieces(i, turn, core):
        return enumerate(chunks[i].wholes(wholes, pl.ds(1, mem - 1), place.turn(turn), core))

    def pass_on(i, turn):
        for j, piece in pieces(i, turn, place.core):
            sems = (core_send.at[i], core_recv.at[i])
            sent.append(send(piece, piece, sems, 2 * turn + j, place.other_core()))

    def finish_flat(i):
        for turn in range(1, quarters):
            for j, piece in pieces(i, turn, place.core):
                expect(piece, (flat_send.at[i], flat_recv.at[i]), 2 * turn + j, place)
            pass_on(i, turn)

    def pass_far(i):
        for step in (2, mem - 1, 1) if mem == 4 else range(1, mem):
            for j, piece in enumerate(chunks[i].wholes(wholes, step, place.quarter, place.core)):
                expect(piece, far_sems_of(i), 2 * step + j, place)
            if step == 2:
                relay(i)
        for j, piece in pieces(i, 0, place.core):
            sems = (flat_send.at[i], flat_recv.at[i])
            for turn in range(1, quarters):
                sent.append(send(piece, piece, sems, 2 * turn + j, place.other_quarter(turn)))
        pass_on(i, 0)

    def far_sems_of(i):
        return far_send.at[i], far_recv.at[i]

    def finish_core(i):
        for turn in range(quarters):
            for j, piece in pieces(i, turn, 1 - place.core):
                expect(piece, (core_send.at[i], core_recv.at[i]), 2 * turn + j, place)

    def bring(source, target):
        copy = pltpu.make_async_copy(source, target, load_sems.at[0])
        copy.start()
        copy.wait()

    def weight(k):
        return weights_ref[k].reshape(-1, model)

    model = attn_ref.shape[2]
    rows, dec_len, _ = input_ref.shape
    enc_len = mem * memory_ref.shape[2]
    pairs = model // pair
    own_heads = model // head_size // mem

    start_far(0)
    for step in range(1, mem):
        back = mem - step
        sent.append(
            send(table_ref, tables_out.at[back], (table_send, table_recv), step, place.along(step), back)
        )
    for i in range(1, 4):
        start_far(i)
    pass_far(0)
    for step in range(1, mem):
        expect(tables_out.at[step], (table_send, table_recv), step, place)
    for step in range(mem):
        per_lane = dot(tables_out[step], spread_ref[...], 0, 0)
        for head in range(own_heads):
            bias_ref[step * own_heads + head] = per_lane[head : head + 1]
    pass_far(1)
    start_enc()
    finish_flat(0)
    pass_far(2)
    finish_core(0)
    for copy in locals_out:
        copy.wait()
    bring(attn_out.at[pl.ds(0, quarters)], weights_ref)

    def project_self(k, carry):
        values = dot(normed_ref[...].reshape(-1, model), weight(k), 1, 1)
        qkv_out[k] = values.astype(low).reshape(rows, dec_len, model)
        return carry

    lax.fori_loop(0, 3, project_self, 0)
    pass_far(3)

    def lanes_at(p):
        return pl.ds(pl.multiple_of(p * pair, pair), pair)

    def self_row(r):
        allowed = causal_mask(dec_column_ref[r] == dec_row_ref[r])

        def step(p, carry):
            weights, mixed = attend_pair(
                qkv_out[0, r, :, lanes_at(p)],
                qkv_out[1, r, :, lanes_at(p)],
                qkv_out[2, r, :, lanes_at(p)],
                allowed,
                [bias_ref[2 * p], bias_ref[2 * p + 1]],
            )
            for half in range(2):
                self_weights_out[r, 2 * p + half] = weights[half]
            self_mixed_out[r, :, lanes_at(p)] = mixed
            return carry

        lax.fori_loop(0, pairs, step, 0)

    def cross_row(r):
        allowed = dec_column_ref[r] == enc_row_ref[r]

        def step(p, carry):
            weights, mixed = attend_pair(
                queries_out[r, :, lanes_at(p)],
                sides_out[0, r, :, lanes_at(p)],
                sides_out[1, r, :, lanes_at(p)],
                allowed,
                None,
            )
            for half in range(2):
                cross_weights_out[r, 2 * p + half] = weights[half]
            cross_mixed_out[r, :, lanes_at(p)] = mixed
            return carry

        lax.fori_loop(0, pairs, step, 0)

    for r in range(rows):
        self_row(r)
    finish_flat(1)
    added = dot(self_mixed_out[...].reshape(-1, model), weight(3), 1, 0)
    first = input_ref[...].astype(wide) + added.reshape(rows, dec_len, model)
    first_out[...] = first
    normed_out[...] = rms(first, gain_ref[1:2, :])[0]
    finish_core(1)
    bring(attn_out.at[pl.ds(quarters, quarters)], weights_ref)
    values = dot(normed_out[...].reshape(-1, model), weight(0), 1, 1)
    queries_out[...] = values.astype(low).reshape(rows, dec_len, model)
    finish_flat(2)
    locals_in.wait()
    own_out = pltpu.make_async_copy(own_enc, memory_out.at[:, 0], local_sems.at[0])
    own_out.start()
    for step in range(1, mem):
        expect(memory_out.at[:, step], (enc_send, enc_recv), step, place)
    own_out.wait()
    bring(memory_out, memory_ref)
    for k in range(2):

        def project_side(r, carry):
            values = dot(memory_ref[r].reshape(-1, model), weight(1 + k), 1, 1)
            sides_out[k, r] = values.astype(low)
            return carry

        lax.fori_loop(0, rows, project_side, 0)
    cross_row(0)
    finish_flat(3)
    for r in range(1, rows):
        cross_row(r)
    finish_core(2)
    finish_core(3)
    for copy in sent:
        copy.wait_send()
    for started, copy in waits:
        pl.when(started)(copy.wait_send)


def gather_all(attn, ffn, enc, table, inputs, normed, gains, dec_ids, enc_ids, spread):
    mem = lax.axis_size("mem")
    count, dec_len, model = inputs.shape
    enc_len = enc_ids.shape[1]
    heads = model // head_size
    dma = pltpu.SemaphoreType.DMA
    in_place = pl.BlockSpec(memory_space=pl.ANY)
    held = pl.BlockSpec(memory_space=pltpu.VMEM)
    operands = (
        attn, ffn, enc, table, inputs, normed, gains,
        dec_ids[:, None, :], dec_ids[:, :, None], enc_ids[:, None, :], spread,
    )

    def values(*shape, dtype=low):
        return jax.ShapeDtypeStruct(shape, dtype)

    return pl.pallas_call(
        gather_body,
        in_specs=[held, held, in_place] + [held] * (len(operands) - 3),
        out_specs=[in_place] * 4 + [held] * 9,
        out_shape=[
            values(attn.shape[0], mem, *attn.shape[1:]),
            values(2, mem, *ffn.shape[1:]),
            values(1, mem, *ffn.shape[1:]),
            values(count, mem, *enc.shape[1:]),
            values(3, count, dec_len, model),
            values(count, dec_len, model),
            values(count, heads, dec_len, dec_len),
            values(count, dec_len, model, dtype=wide),
            values(count, dec_len, model),
            values(count, dec_len, model),
            values(2, count, enc_len, model),
            values(count, dec_len, model),
            values(count, heads, dec_len, enc_len),
        ],
        scratch_shapes=[
            pltpu.VMEM((count,) + enc.shape[1:], low),
            pltpu.VMEM((mem,) + table.shape, low),
            pltpu.VMEM((heads, 1, spread.shape[1]), wide),
            pltpu.VMEM((quarters, mem) + attn.shape[1:], low),
            pltpu.VMEM((count, mem) + enc.shape[1:], low),
            dma((4,)), dma((1,)),
            dma((4, 2 * mem + 4)), dma((4, 2 * mem)),
            dma((mem,)), dma((mem,)),
            dma((mem,)), dma((mem,)),
            dma((4, 2 * quarters)), dma((4, 2 * quarters)),
            dma((4, 2 * quarters)), dma((4, 2 * quarters)),
        ],
        compiler_params=pltpu.CompilerParams(
            collective_id=0, has_side_effects=True, vmem_limit_bytes=60000000
        ),
    )(*operands)


def add_planes(total_ref, total_at, more_ref, more_at, k, steps):
    first, size = steps

    def plane(index, carry):
        i, d = index // size, index % size
        added = more_ref[more_at + (i, d)].astype(wide)
        here = total_at + (i, first + d)
        total_ref[here] = (total_ref[here].astype(wide) + added).astype(low)
        return carry

    lax.fori_loop(0, k * size, plane, 0)


class Reduction:
    def __init__(self, place, chunk, held, index, scratch, out_ref, sent, parts_of):
        self.place, self.chunk, self.out_ref, self.sent = place, chunk, out_ref, sent
        self.held = held
        refs = [ref.at[index] for ref in scratch]
        self.core, self.near, self.last, self.far, self.local = refs[:5]
        pairs = [(refs[j], refs[j + 1]) for j in range(5, len(refs), 2)]
        self.core_sems, self.near_sems, self.last_sems = pairs[:3]
        self.far_sems, self.flat_sems, self.pass_sems = pairs[3:]
        self.parts_of = parts_of
        self.loads = []
        self.half = place.mem // 2

    def begin(self):
        for quarter in range(quarters):
            for j, (source, first, planes) in enumerate(self.parts_of(quarter, self.place.core)):
                copy = pltpu.make_async_copy(
                    source, self.held.at[quarter, pl.ds(first, planes)],
                    self.local.at[2 * quarter + j],
                )
                copy.start()
                self.loads.append(copy)

    def to_core(self):
        for quarter in range(quarters):
            parts = self.parts_of(quarter, 1 - self.place.core)
            for j, (source, first, planes) in enumerate(parts):
                self.sent.append(
                    send(
                        source, self.core.at[quarter, pl.ds(first, planes)],
                        self.core_sems, 2 * quarter + j, self.place.other_core(),
                    )
                )

    def from_core(self):
        place, held, near, half = self.place, self.held, self.near, self.half
        for copy in self.loads:
            copy.wait()
        for quarter in range(quarters):
            parts = self.parts_of(quarter, place.core)
            for j, (_, first, planes) in enumerate(parts):
                landed = self.core.at[quarter, pl.ds(first, planes)]
                expect(landed, self.core_sems, 2 * quarter + j, place)
            add_planes(held, (quarter,), self.core, (quarter,), self.chunk.k, (0, place.mem))
        for bit in range(2):
            quarter = bit * 2 + (1 - place.near)
            source = held.at[quarter, :, pl.ds(0, half)]
            self.sent.append(
                send(source, near.at[0, bit], self.near_sems, bit, place.other_quarter(1))
            )
            quarter = (1 - place.far) * 2 + bit
            source = held.at[quarter, :, pl.ds(half, half)]
            self.sent.append(
                send(source, near.at[1, bit], self.near_sems, 2 + bit, place.other_quarter(2))
            )

    def from_near(self):
        place, held, near, half = self.place, self.held, self.near, self.half
        k = self.chunk.k
        for bit in range(2):
            expect(near.at[0, bit], self.near_sems, bit, place)
            add_planes(held, (bit * 2 + place.near,), near, (0, bit), k, (0, half))
            expect(near.at[1, bit], self.near_sems, 2 + bit, place)
            add_planes(held, (place.far * 2 + bit,), near, (1, bit), k, (half, half))
        quarter = (1 - place.far) * 2 + place.near
        source = held.at[quarter, :, pl.ds(0, half)]
        self.sent.append(send(source, self.last.at[0], self.last_sems, 0, place.other_quarter(2)))
        quarter = place.far * 2 + (1 - place.near)
        source = held.at[quarter, :, pl.ds(half, half)]
        self.sent.append(send(source, self.last.at[1], self.last_sems, 1, place.other_quarter(1)))

    def from_last(self):
        place, half = self.place, self.half
        for part in range(2):
            expect(self.last.at[part], self.last_sems, part, place)
            steps = (part * half, half)
            add_planes(self.held, (place.quarter,), self.last, (part,), self.chunk.k, steps)
        for step in range(1, place.mem):
            back = place.mem - step
            source = self.held.at[place.quarter, :, step]
            self.sent.append(
                send(source, self.far.at[back], self.far_sems, step, place.along(step), back)
            )

    def from_far(self):
        place = self.place
        for step in range(1, place.mem):
            expect(self.far.at[step], self.far_sems, step, place)
        k_at, rows_at = self.chunk.spot(place.quarter, place.core)
        for k in range(self.chunk.k):
            total = self.held[place.quarter, k, 0].astype(wide)
            for step in range(1, place.mem):
                total = total + self.far[step, k].astype(wide)
            self.out_ref[k_at.start + k, rows_at, :] = total.astype(low)
        piece = self.piece(place.quarter, place.core)
        for turn in range(1, quarters):
            self.sent.append(send(piece, piece, self.flat_sems, turn, place.other_quarter(turn)))
        self.sent.append(send(piece, piece, self.pass_sems, 0, place.other_core()))

    def piece(self, quarter, core):
        k, rows = self.chunk.spot(quarter, core)
        return self.out_ref.at[k, rows]

    def from_flat(self):
        place = self.place
        for turn in range(1, quarters):
            piece = self.piece(place.turn(turn), place.core)
            expect(piece, self.flat_sems, turn, place)
            self.sent.append(send(piece, piece, self.pass_sems, turn, place.other_core()))

    def from_pass(self):
        place = self.place
        for turn in range(quarters):
            piece = self.piece(place.turn(turn), 1 - place.core)
            expect(piece, self.pass_sems, turn, place)


def reduction_scratch(chunk, mem, model):
    k, rows = chunk.k, chunk.rows

    def room(*shape):
        return pltpu.VMEM((2,) + shape + (rows, model), low)

    buffers = [
        room(quarters, k, mem),
        room(2, 2, k, mem // 2),
        room(2, k, mem // 2),
        room(mem, k),
    ]
    sems = [pltpu.SemaphoreType.DMA((2, 2 * quarters))]
    for count in (2 * quarters, quarters, 2, mem, quarters, quarters):
        sems += [pltpu.SemaphoreType.DMA((2, count)) for _ in range(2)]
    return buffers + sems


reduction_refs = 17


class Move:
    def __init__(self, place, index, source, target, sems):
        self.place, self.target = place, target
        self.sems = (sems[0].at[index], sems[1].at[index])
        self.stay = pltpu.make_async_copy(source(0), target(place.me), sems[2].at[index])
        self.stay.start()
        self.sent = [
            send(
                source(step), target(place.me), self.sems, step, place.along(step),
                place.mem - step,
            )
            for step in range(1, place.mem)
        ]

    def finish(self):
        place = self.place
        for step in range(1, place.mem):
            expect(self.target((place.me + step) % place.mem), self.sems, step, place)
        for copy in self.sent:
            copy.wait_send()
        self.stay.wait()


def back_body(
    in_ref, down_ref, attn_weights_ref, cross_weights_ref, self_weights_ref, sides_in, qkv_in,
    output_ref, grad_second_ref, first_ref, input_ref, normed_one_ref, normed_two_ref,
    self_mixed_ref, cross_mixed_ref, queries_ref, memory_ref, gain_ref, gain_three_ref,
    attn_out, ffn_out, output_out, memory_out, input_out, small_out,
    held_ffn, grads_ref, weights_ref, cross_probs, self_probs, sides_ref, qkv_ref,
    mixed_grad_ref, query_grad_ref, grad_first_ref, memory_blocks, input_blocks,
    small_ref, small_far, small_flat,
    load_sems, move_send, move_recv, stay_sems, small_send, small_recv, *scratch,
):
    place = Place()
    mem = place.mem
    sent = []
    rows, dec_len, model = input_ref.shape
    pairs = model // pair
    heads = 2 * pairs
    own_heads = heads // mem

    def ffn_reduction(part):
        chunk = Chunk(2 + part, 0, ffn_out.shape[1])

        def parts_of(quarter, core):
            at = chunk.spot(quarter, core)[1]
            return [(in_ref.at[:, :, at], 0, 2), (down_ref.at[:, :, at], 2, 1)]

        return Reduction(
            place, chunk, held_ffn.at[part], part, scratch[:reduction_refs], ffn_out, sent,
            parts_of,
        )

    def attn_reduction(part):
        chunk = Chunk(part, attn_out.shape[1], 0)

        def parts_of(quarter, core):
            return [(grads_ref.at[part * quarters + quarter, :, :, core], 0, 1)]

        held = grads_ref.at[pl.ds(part * quarters, quarters), :, :, place.core]
        return Reduction(
            place, chunk, held, part, scratch[reduction_refs:], attn_out, sent, parts_of
        )

    one, two = ffn_reduction(0), ffn_reduction(1)
    third, fourth = attn_reduction(1), attn_reduction(0)

    def load(index, source, target):
        copy = pltpu.make_async_copy(source, target, load_sems.at[index])
        copy.start()
        return copy

    def load_weight(index, k, slot):
        return load(index, attn_weights_ref.at[k], weights_ref.at[slot])

    got_out = load_weight(0, 7, 0)
    got_sides = load(1, sides_in, sides_ref)
    got_probs = load(2, cross_weights_ref.at[0], cross_probs)
    got_kv = [load_weight(3, 5, 1), load_weight(4, 6, 2)]
    one.begin()
    two.begin()
    got_qkv = load(5, qkv_in, qkv_ref)
    got_self_probs = load(6, self_weights_ref.at[0], self_probs)
    place.greet()
    one.to_core()
    two.to_core()
    moves = []

    def move(source, target):
        sems = (move_send, move_recv, stay_sems)
        moves.append(Move(place, len(moves), source, target, sems))

    move(lambda step: output_ref.at[step], lambda d: output_out.at[d])

    def weight(slot):
        return weights_ref[slot].reshape(-1, model)

    def flat(values):
        return values.reshape(-1, model)

    def lanes_at(p):
        return pl.ds(pl.multiple_of(p * pair, pair), pair)

    def keep(k, grad):
        grads_ref[k] = grad.astype(low).reshape(grads_ref.shape[1:])

    grad_low = flat(grad_second_ref[...]).astype(low)
    got_out.wait()
    mixed_grad = dot(grad_low, weight(0), 1, 1).astype(low)
    mixed_grad_ref[...] = mixed_grad.reshape(rows, dec_len, model)
    got_query = load_weight(7, 4, 0)
    one.from_core()
    keep(7, dot(flat(cross_mixed_ref[...]), grad_low, 0, 0))
    two.from_core()
    got_sides.wait()
    got_probs.wait()
    for copy in got_kv:
        copy.wait()

    def cross_row(r):
        def step(p, carry):
            at = lanes_at(p)
            dq, dk, dv, _ = attend_back_pair(
                [cross_probs[2 * p], cross_probs[2 * p + 1]],
                queries_ref[r, :, at], sides_ref[0, r, :, at], sides_ref[1, r, :, at],
                mixed_grad_ref[r, :, at], None,
            )
            query_grad_ref[r, :, at] = dq
            sides_ref[0, r, :, at] = dk
            sides_ref[1, r, :, at] = dv
            return carry

        lax.fori_loop(0, pairs, step, 0)
        if r + 1 < rows:
            following = load(8 + r, cross_weights_ref.at[r + 1], cross_probs)
        both = dot(sides_ref[0, r], weight(1), 1, 0) + dot(sides_ref[1, r], weight(2), 1, 0)
        memory_blocks[r] = both.astype(low).reshape(memory_blocks.shape[1:])
        if r + 1 < rows:
            following.wait()

    def move_memory(r):
        move(lambda step: memory_blocks.at[r, step], lambda d: memory_out.at[d, r])

    cross_row(0)
    move_memory(0)
    one.from_near()
    for r in range(1, rows):
        cross_row(r)
    got_self_out = load_weight(3, 3, 1)
    query_grad = flat(query_grad_ref[...])
    keep(4, dot(query_grad, flat(normed_two_ref[...]), 0, 0))
    two.from_near()
    for k in range(2):
        keep(5 + k, dot(flat(sides_ref[k]), flat(memory_ref[...]), 0, 0))
    third.to_core()
    one.from_last()

    got_query.wait()
    grad_two = dot(query_grad, weight(0), 1, 0)
    back, gain_two = rms_back_flat(flat(first_ref[...]), gain_ref[1:2, :], grad_two)
    grad_first = flat(grad_second_ref[...]) + back
    grad_first_ref[...] = grad_first
    grad_low = grad_first.astype(low)
    got_self_out.wait()
    mixed_grad = dot(grad_low, weight(1), 1, 1).astype(low)
    mixed_grad_ref[...] = mixed_grad.reshape(rows, dec_len, model)
    got_qkv_weights = [load_weight(7, 0, 0), load_weight(3, 1, 1), load_weight(4, 2, 2)]
    third.from_core()
    two.from_last()
    for r in range(1, rows):
        move_memory(r)
    keep(3, dot(flat(self_mixed_ref[...]), grad_low, 0, 0))
    got_qkv.wait()
    got_self_probs.wait()

    def self_row(r):
        def step(p, carry):
            at = lanes_at(p)
            dq, dk, dv, dist = attend_back_pair(
                [self_probs[2 * p], self_probs[2 * p + 1]],
                qkv_ref[0, r, :, at], qkv_ref[1, r, :, at], qkv_ref[2, r, :, at],
                mixed_grad_ref[r, :, at], small_ref.shape[-1],
            )
            qkv_ref[0, r, :, at] = dq
            qkv_ref[1, r, :, at] = dk
            qkv_ref[2, r, :, at] = dv
            for half in range(2):
                spot = 2 * p + half
                owner = (place.me + lax.div(spot, own_heads)) % mem
                head = owner * own_heads + lax.rem(spot, own_heads)
                small_ref[head] = dist[half] if r == 0 else small_ref[head] + dist[half]
            return carry

        lax.fori_loop(0, pairs, step, 0)
        if r + 1 < rows:
            following = load(8 + r, self_weights_ref.at[r + 1], self_probs)
            following.wait()

    self_row(0)
    third.from_near()
    one.from_far()
    for r in range(1, rows):
        self_row(r)
    third.from_last()
    two.from_far()
    one.from_flat()

    def project_back(k, carry):
        keep(k, dot(flat(qkv_ref[k]), flat(normed_one_ref[...]), 0, 0))
        return carry

    lax.fori_loop(0, 3, project_back, 0)
    fourth.to_core()
    for copy in got_qkv_weights:
        copy.wait()
    grad_one = dot(flat(qkv_ref[0]), weight(0), 1, 0)
    fourth.from_core()
    for k in range(1, 3):
        grad_one = grad_one + dot(flat(qkv_ref[k]), weight(k), 1, 0)
    back, gain_one = rms_back_flat(flat(input_ref[...]).astype(wide), gain_ref[0:1, :], grad_one)
    grad_input = (grad_first_ref[...] + back).astype(low).reshape(rows, dec_len, model)
    own_len = dec_len // mem
    for d in range(mem):
        input_blocks[d] = grad_input[:, d * own_len : (d + 1) * own_len, :]
    size = small_ref.shape[-1]
    for index, gain_grad in enumerate((gain_one, gain_two, gain_three_ref[...])):
        for j in range(model // size):
            spot = heads + index * (model // size) + j
            small_ref[spot] = gain_grad[:, j * size : (j + 1) * size]
    for step in range(1, mem):
        back_step = mem - step
        sent.append(
            send(
                small_ref, small_far.at[back_step], (small_send, small_recv), step,
                place.along(step), back_step,
            )
        )
    two.from_flat()
    one.from_pass()
    third.from_far()
    fourth.from_near()
    move(
        lambda step: input_blocks.at[(place.me + step) % mem], lambda d: input_out.at[d]
    )
    total = small_ref[...]
    for step in range(1, mem):
        expect(small_far.at[step], (small_send, small_recv), step, place)
        total = total + small_far[step]
    small_flat[0] = total
    for turn in range(1, block):
        there = place.at(place.turn(turn // 2), (place.core + turn % 2) % 2)
        sems = (small_send, small_recv)
        sent.append(send(small_flat.at[0], small_flat.at[turn], sems, mem + turn, there))
    two.from_pass()
    third.from_flat()
    fourth.from_last()
    third.from_pass()
    total = small_flat[0]
    for turn in range(1, block):
        expect(small_flat.at[turn], (small_send, small_recv), mem + turn, place)
        total = total + small_flat[turn]
    small_out[...] = total
    fourth.from_far()
    fourth.from_flat()
    fourth.from_pass()
    for moving in moves:
        moving.finish()
    for copy in sent:
        copy.wait_send()


def back_all(
    ffn, attn_weights, cross_weights, self_weights, sides, qkv, output,
    grad_second, first, inputs, normed_one, normed_two, self_mixed, cross_mixed, queries,
    memory, gains, gain_three, lane_count,
):
    mem = lax.axis_size("mem")
    own_hidden, model = ffn[0].shape[-2:]
    own_width = attn_weights.shape[2]
    count, heads, dec_len, _ = self_weights.shape
    enc_len = memory.shape[1]
    small_shape = (heads + 3 * (model // lane_count), 1, lane_count)
    dma = pltpu.SemaphoreType.DMA
    in_place = pl.BlockSpec(memory_space=pl.ANY)
    held = pl.BlockSpec(memory_space=pltpu.VMEM)
    attn_chunk, ffn_chunk = Chunk(0, own_width, 0), Chunk(2, 0, own_hidden)
    move_count = count + 2

    def values(*shape, dtype=low):
        return jax.ShapeDtypeStruct(shape, dtype)

    return pl.pallas_call(
        back_body,
        in_specs=[in_place] * 7 + [held] * 12,
        out_specs=[held, held, in_place, in_place, in_place, held],
        out_shape=[
            values(2 * quarters, own_width, model),
            values(3, own_hidden, model),
            values(*output.shape),
            values(mem, count, enc_len // mem, model),
            values(*output.shape),
            values(*small_shape, dtype=wide),
        ],
        scratch_shapes=[
            pltpu.VMEM((2, quarters, 3, mem, ffn_chunk.rows, model), low),
            pltpu.VMEM((2 * quarters, 1, mem, 2, attn_chunk.rows, model), low),
            pltpu.VMEM((3,) + attn_weights.shape[1:], low),
            pltpu.VMEM(cross_weights.shape[1:], low),
            pltpu.VMEM(self_weights.shape[1:], low),
            pltpu.VMEM(sides.shape, low),
            pltpu.VMEM(qkv.shape, low),
            pltpu.VMEM(inputs.shape, low),
            pltpu.VMEM(inputs.shape, low),
            pltpu.VMEM((count * dec_len, model), wide),
            pltpu.VMEM((count, mem, enc_len // mem, model), low),
            pltpu.VMEM(output.shape, low),
            pltpu.VMEM(small_shape, wide),
            pltpu.VMEM((mem,) + small_shape, wide),
            pltpu.VMEM((block,) + small_shape, wide),
            dma((8 + count,)),
            dma((move_count, mem)), dma((move_count, mem)), dma((move_count,)),
            dma((mem + block,)), dma((mem + block,)),
        ]
        + reduction_scratch(ffn_chunk, mem, model)
        + reduction_scratch(attn_chunk, mem, model),
        compiler_params=pltpu.CompilerParams(
            collective_id=1, has_side_effects=True, vmem_limit_bytes=66000000
        ),
    )(
        *ffn, attn_weights, cross_weights, self_weights, sides, qkv, output,
        grad_second, first, inputs, normed_one, normed_two, self_mixed, cross_mixed, queries,
        memory, gains, gain_three,
    )


def sum_blocks(values):
    bit = block
    while bit < lax.axis_size("rows"):
        values = values + flip(values, bit)
        bit *= 2
    return values


def dot(left, right, left_dim, right_dim):
    return lax.dot_general(
        left, right, (((left_dim,), (right_dim,)), ((), ())), preferred_element_type=wide
    )


def lanes_of(half):
    lane = lax.broadcasted_iota(jnp.int32, (1, pair), 1)
    return ((lane // head_size) == half).astype(wide)


def skewed(row, height):
    spread = jnp.broadcast_to(row, (height, row.shape[1]))
    return pltpu.roll(spread, 0, 1, stride=1, stride_axis=0)


def causal_mask(same):
    rows, keys = same.shape
    i = lax.broadcasted_iota(jnp.int32, (rows, keys), 0)
    j = lax.broadcasted_iota(jnp.int32, (rows, keys), 1)
    return same & (i >= j)


def attend_pair(queries, keys_in, values_in, allowed, bias):
    rows, keys = allowed.shape
    kept = []
    mixed = jnp.zeros((rows, pair), wide)
    for half in range(2):
        lanes = lanes_of(half)
        scores = dot(queries * lanes.astype(low), keys_in, 1, 1)
        if bias is not None:
            scores = scores + skewed(bias[half], rows)[:, :keys]
        scores = jnp.where(allowed, scores, negative)
        raised = jnp.exp(scores - jnp.max(scores, axis=-1, keepdims=True))
        scale = 1.0 / jnp.sum(raised, axis=-1, keepdims=True)
        weights = (raised * scale).astype(low)
        kept.append(weights)
        mixed = mixed + dot(weights, values_in, 1, 0) * lanes
    return kept, mixed.astype(low)


def attend_back_pair(weights_pair, queries, keys_in, values_in, grad, dist_width):
    rows, keys = weights_pair[0].shape
    dq = jnp.zeros((rows, pair), wide)
    dk = jnp.zeros((keys, pair), wide)
    dv = jnp.zeros((keys, pair), wide)
    dist = []
    for half in range(2):
        lanes = lanes_of(half)
        weights = weights_pair[half]
        weights_wide = weights.astype(wide)
        grad_weights = dot(grad * lanes.astype(low), values_in, 1, 1)
        inner = jnp.sum(grad_weights * weights_wide, axis=-1, keepdims=True)
        grad_scores = (weights_wide * (grad_weights - inner)).astype(low)
        dv = dv + dot(weights, grad, 0, 0) * lanes
        dq = dq + dot(grad_scores, keys_in, 1, 0) * lanes
        dk = dk + dot(grad_scores, queries, 0, 0) * lanes
        if dist_width is not None:
            i = lax.broadcasted_iota(jnp.int32, (rows, rows), 0)
            j = lax.broadcasted_iota(jnp.int32, (rows, rows), 1)
            upside_down = dot((i + j == rows - 1).astype(wide).astype(low), grad_scores, 1, 0)
            padded = jnp.concatenate(
                [upside_down, jnp.zeros((rows, dist_width - keys), wide)], axis=1
            )
            turned = pltpu.roll(padded, 0, 1, stride=1, stride_axis=0)
            dist.append(jnp.sum(turned, axis=0, keepdims=True))
    return dq.astype(low), dk.astype(low), dv.astype(low), dist


def rms_back_flat(values, gain, grad):
    scale = lax.rsqrt(jnp.mean(values * values, axis=-1, keepdims=True) + epsilon)
    grad_gain = jnp.sum(grad * values * scale, axis=0, keepdims=True)
    scaled = grad * gain
    inner = jnp.mean(scaled * values, axis=-1, keepdims=True)
    return scaled * scale - values * (scale * scale * scale * inner), grad_gain


def rms(values, gain):
    scale = lax.rsqrt(jnp.mean(values * values, axis=-1, keepdims=True) + epsilon)
    return (values * scale * gain).astype(low), scale


def rms_back(values, scale, gain, grad):
    grad_gain = jnp.sum(grad * values * scale, axis=(0, 1))
    scaled = grad * gain
    inner = jnp.mean(scaled * values, axis=-1, keepdims=True)
    return scaled * scale - values * (scale * scale * scale * inner), grad_gain


def times_t(values, weight):
    return jnp.einsum("rtd,cd->rtc", values, weight, preferred_element_type=wide)


def times(values, weight):
    return jnp.einsum("rtc,cd->rtd", values, weight, preferred_element_type=wide)


def weight_grad(grads, values):
    return jnp.einsum("rtc,rtd->cd", grads, values, preferred_element_type=wide).astype(low)


def gated(gate, upward):
    return jax.nn.gelu(gate, approximate=True) * upward


def shards(
    dec_input,
    enc_output,
    dec_segments,
    enc_segments,
    buckets,
    gains,
    self_query,
    self_kv,
    self_out,
    rel_table,
    cross_query,
    cross_kv,
    cross_out,
    ffn_in,
    ffn_out,
    cotangent,
):
    mem = lax.axis_size("mem")
    me = lax.axis_index("mem")
    group, dec_len, model = dec_input.shape
    count = group // mem
    own_heads = rel_table.shape[1]
    own_width = self_query.shape[1]
    width = own_width * mem
    pairs = width // pair
    own_hidden = ffn_out.shape[0]
    gain_values = gains.astype(wide)
    bucket_count = rel_table.shape[0]

    attn_shard = jnp.stack(
        [self_query.T, self_kv[0].T, self_kv[1].T, self_out]
        + [cross_query.T, cross_kv[0].T, cross_kv[1].T, cross_out]
    )
    ffn_shard = jnp.stack([ffn_in[0].T, ffn_in[1].T, ffn_out])
    padded_table = jnp.pad(rel_table, ((0, 0), (0, pair - own_heads)))

    def mine(values):
        return lax.dynamic_slice_in_dim(values, me * count, count, 0)

    own_input = mine(dec_input)
    inputs = own_input.astype(wide)
    grad_out = mine(cotangent)
    dec_ids = mine(dec_segments)
    enc_ids = jnp.concatenate(relative(mine(enc_segments), 1, mem), axis=1)
    enc_len = enc_ids.shape[1]

    lane_count = -(-dec_len // pair) * pair
    turned = jnp.concatenate(
        [
            buckets[:1],
            jnp.full((lane_count - dec_len,), -1, buckets.dtype),
            jnp.flip(buckets[1:]),
        ]
    )
    spread = (jnp.arange(bucket_count)[:, None] == turned[None, :]).astype(low)

    normed_one, scale_one = rms(inputs, gain_values[0])
    (
        attn_weights_in, in_weight, out_weight, memory,
        qkv, self_mixed, self_weights, first, normed_two,
        cross_queries, cross_sides, cross_mixed, cross_weights,
    ) = gather_all(
        attn_shard, ffn_shard, enc_output, padded_table,
        own_input, normed_one, gain_values, dec_ids, enc_ids, spread,
    )
    cross_out_weight = attn_weights_in[7].reshape(width, model)
    in_weight = in_weight.reshape(-1, model)
    out_weight = out_weight.reshape(-1, model)
    memory = memory.reshape(count, -1, model)
    second = first + times(cross_mixed, cross_out_weight)
    normed_three, scale_three = rms(second, gain_values[2])

    hidden_width = mem * own_hidden
    gate_up = times_t(normed_three, in_weight)
    hidden_float, pull = jax.vjp(gated, gate_up[..., :hidden_width], gate_up[..., hidden_width:])
    hidden = hidden_float.astype(low)
    output = second + times(hidden, out_weight)
    grad_gate, grad_up = pull(times_t(grad_out, out_weight))
    grad_gate_up = jnp.concatenate([grad_gate.astype(low), grad_up.astype(low)], axis=-1)
    grad_three = times(grad_gate_up, in_weight)
    ffn_grads = [
        grad.reshape(-1, mem, own_hidden, model)
        for grad in (weight_grad(grad_gate_up, normed_three), weight_grad(hidden, grad_out))
    ]

    grad_wide = grad_out.astype(wide)
    back, gain_three = rms_back(second, scale_three, gain_values[2], grad_three)
    grad_second = grad_wide + back
    attn_sums, ffn_sums, output, grad_memory, grad_input, small = back_all(
        ffn_grads, attn_weights_in, cross_weights, self_weights, cross_sides, qkv,
        jnp.stack(relative(output.astype(low), 1, mem)),
        grad_second, first, own_input, normed_one, normed_two, self_mixed, cross_mixed,
        cross_queries, memory, gain_values, gain_three[None], lane_count,
    )
    attn_sums = sum_blocks(attn_sums).astype(wide)
    ffn_sums = sum_blocks(ffn_sums).astype(wide)
    small = sum_blocks(small[:, 0])
    heads = mem * own_heads
    gain_sums = lax.dynamic_slice_in_dim(
        small[heads:].reshape(3, model), me * own_width, own_width, 1
    )
    falling = jnp.concatenate(
        [jnp.flip(buckets), jnp.full((lane_count - dec_len,), -1, buckets.dtype)]
    )
    one_hot = (falling[:, None] == jnp.arange(bucket_count)[None, :]).astype(wide)
    own_sums = lax.dynamic_slice_in_dim(small, me * own_heads, own_heads, 0)
    grad_table = jnp.einsum("hl,lb->bh", own_sums, one_hot, precision=highest)

    def columns(values):
        return jnp.swapaxes(values, -1, -2)

    return (
        output.reshape(group, -1, model).astype(wide),
        grad_input.reshape(group, -1, model).astype(wide),
        grad_memory.reshape(group, -1, model).astype(wide),
        gain_sums,
        columns(attn_sums[0]),
        columns(attn_sums[1:3]),
        attn_sums[3],
        grad_table,
        columns(attn_sums[4]),
        columns(attn_sums[5:7]),
        attn_sums[7],
        columns(ffn_sums[:2]),
        ffn_sums[2],
    )


def solution(mesh):
    in_specs = (
        P("rows", None, None),
        P("rows", "mem", None),
        P("rows", None),
        P("rows", None),
        P(),
        P(),
        P(None, "mem"),
        P(None, None, "mem"),
        P("mem", None),
        P(None, "mem"),
        P(None, "mem"),
        P(None, None, "mem"),
        P("mem", None),
        P(None, None, "mem"),
        P("mem", None),
        P("rows", None, None),
    )
    out_specs = (
        P("rows", "mem", None),
        P("rows", "mem", None),
        P("rows", "mem", None),
        P(None, "mem"),
        P(None, "mem"),
        P(None, None, "mem"),
        P("mem", None),
        P(None, "mem"),
        P(None, "mem"),
        P(None, None, "mem"),
        P("mem", None),
        P(None, None, "mem"),
        P("mem", None),
    )
    return jax.shard_map(shards, mesh=mesh, in_specs=in_specs, out_specs=out_specs, check_vma=False)
```

```python
from functools import partial

import jax
import jax.numpy as jnp
from jax import lax
from jax.experimental import pallas as pl
from jax.experimental.pallas import tpu as pltpu
from jax.sharding import PartitionSpec as P

epsilon = 1e-06
negative = -1e30
highest = lax.Precision.HIGHEST
low = jnp.bfloat16
wide = jnp.float32
pair = 128
head_size = 64


def flip(values, bit):
    size = lax.axis_size("rows")
    return lax.ppermute(values, "rows", [(i, i ^ bit) for i in range(size)])


def relative(values, axis, count):
    me = lax.axis_index("mem")
    size = values.shape[axis] // count
    return [
        lax.dynamic_slice_in_dim(values, ((me + step) % count) * size, size, axis)
        for step in range(count)
    ]


block = 8
quarters = 4
MESH = pl.DeviceIdType.MESH


class Place:
    def __init__(self):
        rows = lax.axis_index("rows")
        self.base = (rows // block) * block
        inner = rows - self.base
        self.core = inner % 2
        self.quarter = inner // 2
        self.near = self.quarter % 2
        self.far = self.quarter // 2
        self.me = lax.axis_index("mem")
        self.mem = lax.axis_size("mem")

    def at(self, quarter, core):
        return (self.base + quarter * 2 + core, self.me)

    def other_core(self):
        return self.at(self.quarter, 1 - self.core)

    def other_quarter(self, step):
        return self.at(self.turn(step), self.core)

    def turn(self, step):
        near = (self.near + step % 2) % 2
        far = (self.far + step // 2) % 2
        return far * 2 + near

    def along(self, step):
        rows = self.base + self.quarter * 2 + self.core
        return (rows, (self.me + step) % self.mem)

    def greet(self):
        barrier = pltpu.get_barrier_semaphore()
        count = 0
        for step in range(1, self.mem):
            pl.semaphore_signal(barrier, inc=1, device_id=self.along(step), device_id_type=MESH)
            count += 1
        for quarter in range(quarters):
            for core in range(2):
                if quarter or core:
                    there = self.at(self.turn(quarter), (self.core + core) % 2)
                    pl.semaphore_signal(barrier, inc=1, device_id=there, device_id_type=MESH)
                    count += 1
        pl.semaphore_wait(barrier, count)


def send(source, target, sems, index, there, arrival=None):
    copy = pltpu.make_async_remote_copy(
        src_ref=source,
        dst_ref=target,
        send_sem=sems[0].at[index],
        recv_sem=sems[1].at[index if arrival is None else arrival],
        device_id=there,
        device_id_type=MESH,
    )
    copy.start()
    return copy


def expect(buffer, sems, index, place):
    pltpu.make_async_remote_copy(
        src_ref=buffer,
        dst_ref=buffer,
        send_sem=sems[0].at[index],
        recv_sem=sems[1].at[index],
        device_id=place.other_core(),
        device_id_type=MESH,
    ).wait_recv()


class Chunk:
    def __init__(self, index, own_width, own_hidden):
        self.index = index
        self.is_ffn = index >= 2
        self.part = index % 2
        if self.is_ffn:
            self.k = 3
            self.rows = own_hidden // 16
        else:
            self.k = 1
            self.rows = own_width // 2

    def spot(self, quarter, core):
        if self.is_ffn:
            start = ((quarter * 2 + self.part) * 2 + core) * self.rows
            return pl.ds(0, 3), pl.ds(pl.multiple_of(start, self.rows), self.rows)
        start = core * self.rows
        return (
            pl.ds(self.part * quarters + quarter, 1),
            pl.ds(pl.multiple_of(start, self.rows), self.rows),
        )

    def shard(self, refs, quarter, core):
        k, rows = self.spot(quarter, core)
        return refs[self.is_ffn].at[k, rows]

    def shards(self, refs, quarter, core):
        k, rows = self.spot(quarter, core)
        if self.is_ffn:
            return [refs[1].at[:, rows], refs[2].at[:, rows]]
        return [refs[0].at[k, rows]]

    def wholes(self, refs, steps, quarter, core, half=None):
        k, rows = self.spot(quarter, core)
        if half is not None:
            size = self.rows // 2
            rows = pl.ds(pl.multiple_of(rows.start + half * size, size), size)
        if self.is_ffn:
            return [refs[1].at[:, steps, rows], refs[2].at[:, steps, rows]]
        return [refs[0].at[k, steps, rows]]


def between_ends(step, me, mem):
    to = (me + step) % mem
    return jnp.logical_and(me - to < mem - 1, to - me < mem - 1)


def gather_body(
    attn_ref, up_ref, down_ref, enc_ref, table_ref,
    input_ref, normed_ref, gain_ref, dec_row_ref, dec_column_ref, enc_row_ref, spread_ref,
    attn_out, in_out, down_out, memory_out,
    qkv_out, self_mixed_out, self_weights_out, first_out, normed_out,
    queries_out, sides_out, cross_mixed_out, cross_weights_out,
    own_enc, tables_out, bias_ref, weights_ref, memory_ref, local_sems, load_sems, far_send, far_recv, enc_send, enc_recv, table_send, table_recv,
    flat_send, flat_recv, core_send, core_recv,
):
    place = Place()
    mem = place.mem
    shards = (attn_ref, up_ref, down_ref)
    wholes = (attn_out, in_out, down_out)
    count = own_enc.shape[0]
    chunks = [Chunk(i, attn_ref.shape[1], up_ref.shape[1]) for i in range(4)]
    locals_in = pltpu.make_async_copy(
        enc_ref.at[pl.ds(place.me * count, count)], own_enc, local_sems.at[0]
    )
    locals_in.start()
    locals_out = [
        pltpu.make_async_copy(attn_ref, attn_out.at[:, 0], local_sems.at[1]),
        pltpu.make_async_copy(up_ref, in_out.at[:, 0], local_sems.at[2]),
        pltpu.make_async_copy(down_ref, down_out.at[:, 0], local_sems.at[3]),
    ]
    for copy in locals_out:
        copy.start()
    tables_out[0] = table_ref[...]
    place.greet()
    sent = []
    waits = []

    def start_far(i):
        sources = chunks[i].shards(shards, place.quarter, place.core)
        for step in range(1, mem):
            back = mem - step
            targets = chunks[i].wholes(wholes, back, place.quarter, place.core)
            for j, (source, target) in enumerate(zip(sources, targets)):
                copy = pltpu.make_async_remote_copy(
                    src_ref=source, dst_ref=target,
                    send_sem=far_send.at[i, 2 * step + j], recv_sem=far_recv.at[i, 2 * back + j],
                    device_id=place.along(step), device_id_type=MESH,
                )
                direct = between_ends(step, place.me, mem)
                pl.when(direct)(copy.start)
                waits.append((direct, copy))

    def relay(i):
        for step, ahead in ((mem - 2, 1), (2, mem - 1)):
            there = (step - ahead) % mem
            at_turn = place.me == (mem - 2 if ahead == 1 else 1)
            sources = chunks[i].wholes(wholes, step, place.quarter, place.core)
            targets = chunks[i].wholes(wholes, there, place.quarter, place.core)
            for j, (source, target) in enumerate(zip(sources, targets)):
                copy = pltpu.make_async_remote_copy(
                    src_ref=source, dst_ref=target,
                    send_sem=far_send.at[i, 2 * mem + (ahead > 1) * 2 + j],
                    recv_sem=far_recv.at[i, 2 * there + j],
                    device_id=place.along(ahead), device_id_type=MESH,
                )
                pl.when(at_turn)(copy.start)
                waits.append((at_turn, copy))

    def start_enc():
        for step in range(1, mem):
            back = mem - step
            target = ((place.me + step) % mem) * count
            sent.append(
                send(
                    enc_ref.at[pl.ds(target, count)], memory_out.at[:, back],
                    (enc_send, enc_recv), step, place.along(step), back,
                )
            )

    def pieces(i, turn, core):
        return enumerate(chunks[i].wholes(wholes, pl.ds(1, mem - 1), place.turn(turn), core))

    def pass_on(i, turn):
        for j, piece in pieces(i, turn, place.core):
            sems = (core_send.at[i], core_recv.at[i])
            sent.append(send(piece, piece, sems, 2 * turn + j, place.other_core()))

    def halves(i, turn, half):
        steps = pl.ds(1, mem - 1)
        return enumerate(chunks[i].wholes(wholes, steps, place.turn(turn), place.core, half))

    def relay_flat(i):
        sems = (flat_send.at[i], flat_recv.at[i])
        for turn in range(1, 3):
            for j, piece in pieces(i, turn, place.core):
                expect(piece, sems, 2 * turn + j, place)
            for j, piece in halves(i, turn, turn - 1):
                index = 4 + 2 * turn + j
                sent.append(send(piece, piece, sems, index, place.other_quarter(3 - turn)))
            pass_on(i, turn)

    def finish_flat(i):
        for turn in range(1, 3):
            for j, piece in halves(i, 3, turn - 1):
                expect(piece, (flat_send.at[i], flat_recv.at[i]), 4 + 2 * turn + j, place)
        pass_on(i, 3)

    def pass_far(i):
        for step in (2, mem - 1, 1) if mem == 4 else range(1, mem):
            for j, piece in enumerate(chunks[i].wholes(wholes, step, place.quarter, place.core)):
                expect(piece, far_sems_of(i), 2 * step + j, place)
            if step == 2:
                relay(i)
        for j, piece in pieces(i, 0, place.core):
            sems = (flat_send.at[i], flat_recv.at[i])
            for turn in range(1, 3):
                sent.append(send(piece, piece, sems, 2 * turn + j, place.other_quarter(turn)))
        pass_on(i, 0)

    def far_sems_of(i):
        return far_send.at[i], far_recv.at[i]

    def finish_core(i):
        for turn in range(quarters):
            for j, piece in pieces(i, turn, 1 - place.core):
                expect(piece, (core_send.at[i], core_recv.at[i]), 2 * turn + j, place)

    def bring(source, target):
        copy = pltpu.make_async_copy(source, target, load_sems.at[0])
        copy.start()
        copy.wait()

    def weight(k):
        return weights_ref[k].reshape(-1, model)

    model = attn_ref.shape[2]
    rows, dec_len, _ = input_ref.shape
    enc_len = mem * memory_ref.shape[2]
    pairs = model // pair
    own_heads = model // head_size // mem

    start_far(0)
    for step in range(1, mem):
        back = mem - step
        sent.append(
            send(table_ref, tables_out.at[back], (table_send, table_recv), step, place.along(step), back)
        )
    for i in range(1, 4):
        start_far(i)
    pass_far(0)
    for step in range(1, mem):
        expect(tables_out.at[step], (table_send, table_recv), step, place)
    for step in range(mem):
        per_lane = dot(tables_out[step], spread_ref[...], 0, 0)
        for head in range(own_heads):
            bias_ref[step * own_heads + head] = per_lane[head : head + 1]
    relay_flat(0)
    pass_far(1)
    start_enc()
    finish_flat(0)
    pass_far(2)
    finish_core(0)
    for copy in locals_out:
        copy.wait()
    bring(attn_out.at[pl.ds(0, quarters)], weights_ref)

    def project_self(k, carry):
        values = dot(normed_ref[...].reshape(-1, model), weight(k), 1, 1)
        qkv_out[k] = values.astype(low).reshape(rows, dec_len, model)
        return carry

    lax.fori_loop(0, 3, project_self, 0)
    relay_flat(1)
    pass_far(3)

    def lanes_at(p):
        return pl.ds(pl.multiple_of(p * pair, pair), pair)

    def self_row(r):
        allowed = causal_mask(dec_column_ref[r] == dec_row_ref[r])

        def step(p, carry):
            weights, mixed = attend_pair(
                qkv_out[0, r, :, lanes_at(p)],
                qkv_out[1, r, :, lanes_at(p)],
                qkv_out[2, r, :, lanes_at(p)],
                allowed,
                [bias_ref[2 * p], bias_ref[2 * p + 1]],
            )
            for half in range(2):
                self_weights_out[r, 2 * p + half] = weights[half]
            self_mixed_out[r, :, lanes_at(p)] = mixed
            return carry

        lax.fori_loop(0, pairs, step, 0)

    def cross_row(r):
        allowed = dec_column_ref[r] == enc_row_ref[r]

        def step(p, carry):
            weights, mixed = attend_pair(
                queries_out[r, :, lanes_at(p)],
                sides_out[0, r, :, lanes_at(p)],
                sides_out[1, r, :, lanes_at(p)],
                allowed,
                None,
            )
            for half in range(2):
                cross_weights_out[r, 2 * p + half] = weights[half]
            cross_mixed_out[r, :, lanes_at(p)] = mixed
            return carry

        lax.fori_loop(0, pairs, step, 0)

    self_row(0)
    finish_flat(1)
    relay_flat(2)
    for r in range(1, rows):
        self_row(r)
    added = dot(self_mixed_out[...].reshape(-1, model), weight(3), 1, 0)
    first = input_ref[...].astype(wide) + added.reshape(rows, dec_len, model)
    first_out[...] = first
    normed_out[...] = rms(first, gain_ref[1:2, :])[0]
    finish_core(1)
    bring(attn_out.at[pl.ds(quarters, quarters)], weights_ref)
    values = dot(normed_out[...].reshape(-1, model), weight(0), 1, 1)
    queries_out[...] = values.astype(low).reshape(rows, dec_len, model)
    finish_flat(2)
    relay_flat(3)
    locals_in.wait()
    own_out = pltpu.make_async_copy(own_enc, memory_out.at[:, 0], local_sems.at[0])
    own_out.start()
    for step in range(1, mem):
        expect(memory_out.at[:, step], (enc_send, enc_recv), step, place)
    own_out.wait()
    bring(memory_out, memory_ref)
    for k in range(2):

        def project_side(r, carry):
            values = dot(memory_ref[r].reshape(-1, model), weight(1 + k), 1, 1)
            sides_out[k, r] = values.astype(low)
            return carry

        lax.fori_loop(0, rows, project_side, 0)
    cross_row(0)
    finish_flat(3)
    for r in range(1, rows):
        cross_row(r)
    finish_core(2)
    finish_core(3)
    for copy in sent:
        copy.wait_send()
    for started, copy in waits:
        pl.when(started)(copy.wait_send)


def gather_all(attn, up, down, enc, table, inputs, normed, gains, dec_ids, enc_ids, spread):
    mem = lax.axis_size("mem")
    count, dec_len, model = inputs.shape
    enc_len = enc_ids.shape[1]
    heads = model // head_size
    dma = pltpu.SemaphoreType.DMA
    in_place = pl.BlockSpec(memory_space=pl.ANY)
    held = pl.BlockSpec(memory_space=pltpu.VMEM)
    operands = (
        attn, up, down, enc, table, inputs, normed, gains,
        dec_ids[:, None, :], dec_ids[:, :, None], enc_ids[:, None, :], spread,
    )

    def values(*shape, dtype=low):
        return jax.ShapeDtypeStruct(shape, dtype)

    return pl.pallas_call(
        gather_body,
        in_specs=[held, held, held, in_place] + [held] * (len(operands) - 4),
        out_specs=[in_place] * 4 + [held] * 9,
        out_shape=[
            values(attn.shape[0], mem, *attn.shape[1:]),
            values(2, mem, *up.shape[1:]),
            values(1, mem, *down.shape[1:]),
            values(count, mem, *enc.shape[1:]),
            values(3, count, dec_len, model),
            values(count, dec_len, model),
            values(count, heads, dec_len, dec_len),
            values(count, dec_len, model, dtype=wide),
            values(count, dec_len, model),
            values(count, dec_len, model),
            values(2, count, enc_len, model),
            values(count, dec_len, model),
            values(count, heads, dec_len, enc_len),
        ],
        scratch_shapes=[
            pltpu.VMEM((count,) + enc.shape[1:], low),
            pltpu.VMEM((mem,) + table.shape, low),
            pltpu.VMEM((heads, 1, spread.shape[1]), wide),
            pltpu.VMEM((quarters, mem) + attn.shape[1:], low),
            pltpu.VMEM((count, mem) + enc.shape[1:], low),
            dma((4,)), dma((1,)),
            dma((4, 2 * mem + 4)), dma((4, 2 * mem)),
            dma((mem,)), dma((mem,)),
            dma((mem,)), dma((mem,)),
            dma((4, 2 * quarters + 2)), dma((4, 2 * quarters + 2)),
            dma((4, 2 * quarters)), dma((4, 2 * quarters)),
        ],
        compiler_params=pltpu.CompilerParams(
            collective_id=0, has_side_effects=True, vmem_limit_bytes=60000000
        ),
    )(*operands)


def add_planes(total_ref, total_at, more_ref, more_at, k, steps):
    first, size = steps

    def plane(index, carry):
        i, d = index // size, index % size
        added = more_ref[more_at + (i, d)].astype(wide)
        here = total_at + (i, first + d)
        total_ref[here] = (total_ref[here].astype(wide) + added).astype(low)
        return carry

    lax.fori_loop(0, k * size, plane, 0)


class Reduction:
    def __init__(self, place, chunk, held, index, scratch, out_ref, sent, parts_of):
        self.place, self.chunk, self.out_ref, self.sent = place, chunk, out_ref, sent
        self.held = held
        refs = [ref.at[index] for ref in scratch]
        self.core, self.near, self.last, self.far, self.local = refs[:5]
        pairs = [(refs[j], refs[j + 1]) for j in range(5, len(refs), 2)]
        self.core_sems, self.near_sems, self.last_sems = pairs[:3]
        self.far_sems, self.flat_sems, self.pass_sems = pairs[3:]
        self.parts_of = parts_of
        self.loads = []
        self.half = place.mem // 2

    def begin(self):
        for quarter in range(quarters):
            for j, (source, first, planes) in enumerate(self.parts_of(quarter, self.place.core)):
                copy = pltpu.make_async_copy(
                    source, self.held.at[quarter, pl.ds(first, planes)],
                    self.local.at[2 * quarter + j],
                )
                copy.start()
                self.loads.append(copy)

    def to_core(self):
        for quarter in range(quarters):
            parts = self.parts_of(quarter, 1 - self.place.core)
            for j, (source, first, planes) in enumerate(parts):
                self.sent.append(
                    send(
                        source, self.core.at[quarter, pl.ds(first, planes)],
                        self.core_sems, 2 * quarter + j, self.place.other_core(),
                    )
                )

    def from_core(self):
        place, held, near, half = self.place, self.held, self.near, self.half
        for copy in self.loads:
            copy.wait()
        for quarter in range(quarters):
            parts = self.parts_of(quarter, place.core)
            for j, (_, first, planes) in enumerate(parts):
                landed = self.core.at[quarter, pl.ds(first, planes)]
                expect(landed, self.core_sems, 2 * quarter + j, place)
            add_planes(held, (quarter,), self.core, (quarter,), self.chunk.k, (0, place.mem))
        for bit in range(2):
            quarter = bit * 2 + (1 - place.near)
            source = held.at[quarter, :, pl.ds(0, half)]
            self.sent.append(
                send(source, near.at[0, bit], self.near_sems, bit, place.other_quarter(1))
            )
            quarter = (1 - place.far) * 2 + bit
            source = held.at[quarter, :, pl.ds(half, half)]
            self.sent.append(
                send(source, near.at[1, bit], self.near_sems, 2 + bit, place.other_quarter(2))
            )

    def from_near(self):
        place, held, near, half = self.place, self.held, self.near, self.half
        k = self.chunk.k
        for bit in range(2):
            expect(near.at[0, bit], self.near_sems, bit, place)
            add_planes(held, (bit * 2 + place.near,), near, (0, bit), k, (0, half))
            expect(near.at[1, bit], self.near_sems, 2 + bit, place)
            add_planes(held, (place.far * 2 + bit,), near, (1, bit), k, (half, half))
        quarter = (1 - place.far) * 2 + place.near
        source = held.at[quarter, :, pl.ds(0, half)]
        self.sent.append(send(source, self.last.at[0], self.last_sems, 0, place.other_quarter(2)))
        quarter = place.far * 2 + (1 - place.near)
        source = held.at[quarter, :, pl.ds(half, half)]
        self.sent.append(send(source, self.last.at[1], self.last_sems, 1, place.other_quarter(1)))

    def from_last(self):
        place, half = self.place, self.half
        for part in range(2):
            expect(self.last.at[part], self.last_sems, part, place)
            steps = (part * half, half)
            add_planes(self.held, (place.quarter,), self.last, (part,), self.chunk.k, steps)
        for step in range(1, place.mem):
            back = place.mem - step
            source = self.held.at[place.quarter, :, step]
            self.sent.append(
                send(source, self.far.at[back], self.far_sems, step, place.along(step), back)
            )

    def from_far(self):
        place = self.place
        for step in range(1, place.mem):
            expect(self.far.at[step], self.far_sems, step, place)
        k_at, rows_at = self.chunk.spot(place.quarter, place.core)
        for k in range(self.chunk.k):
            total = self.held[place.quarter, k, 0].astype(wide)
            for step in range(1, place.mem):
                total = total + self.far[step, k].astype(wide)
            self.out_ref[k_at.start + k, rows_at, :] = total.astype(low)
        piece = self.piece(place.quarter, place.core)
        for turn in range(1, quarters):
            self.sent.append(send(piece, piece, self.flat_sems, turn, place.other_quarter(turn)))
        self.sent.append(send(piece, piece, self.pass_sems, 0, place.other_core()))

    def piece(self, quarter, core):
        k, rows = self.chunk.spot(quarter, core)
        return self.out_ref.at[k, rows]

    def from_flat(self):
        place = self.place
        for turn in range(1, quarters):
            piece = self.piece(place.turn(turn), place.core)
            expect(piece, self.flat_sems, turn, place)
            self.sent.append(send(piece, piece, self.pass_sems, turn, place.other_core()))

    def from_pass(self):
        place = self.place
        for turn in range(quarters):
            piece = self.piece(place.turn(turn), 1 - place.core)
            expect(piece, self.pass_sems, turn, place)


def reduction_scratch(chunk, mem, model):
    k, rows = chunk.k, chunk.rows

    def room(*shape):
        return pltpu.VMEM((2,) + shape + (rows, model), low)

    buffers = [
        room(quarters, k, mem),
        room(2, 2, k, mem // 2),
        room(2, k, mem // 2),
        room(mem, k),
    ]
    sems = [pltpu.SemaphoreType.DMA((2, 2 * quarters))]
    for count in (2 * quarters, quarters, 2, mem, quarters, quarters):
        sems += [pltpu.SemaphoreType.DMA((2, count)) for _ in range(2)]
    return buffers + sems


reduction_refs = 17


class Move:
    def __init__(self, place, index, source, target, sems):
        self.place, self.target = place, target
        self.sems = (sems[0].at[index], sems[1].at[index])
        self.stay = pltpu.make_async_copy(source(0), target(place.me), sems[2].at[index])
        self.stay.start()
        self.sent = [
            send(
                source(step), target(place.me), self.sems, step, place.along(step),
                place.mem - step,
            )
            for step in range(1, place.mem)
        ]

    def finish(self):
        place = self.place
        for step in range(1, place.mem):
            expect(self.target((place.me + step) % place.mem), self.sems, step, place)
        for copy in self.sent:
            copy.wait_send()
        self.stay.wait()


def back_body(
    in_ref, down_ref, attn_weights_ref, cross_weights_ref, self_weights_ref, sides_in, qkv_in,
    output_ref, grad_second_ref, first_ref, input_ref, normed_one_ref, normed_two_ref,
    self_mixed_ref, cross_mixed_ref, queries_ref, memory_ref, gain_ref, gain_three_ref,
    attn_out, ffn_out, output_out, memory_out, input_out, small_out,
    held_ffn, grads_ref, weights_ref, cross_probs, self_probs, sides_ref, qkv_ref,
    mixed_grad_ref, query_grad_ref, grad_first_ref, memory_blocks, input_blocks,
    small_ref, small_far, small_flat,
    load_sems, move_send, move_recv, stay_sems, small_send, small_recv, *scratch,
):
    place = Place()
    mem = place.mem
    sent = []
    rows, dec_len, model = input_ref.shape
    pairs = model // pair
    heads = 2 * pairs
    own_heads = heads // mem

    def ffn_reduction(part):
        chunk = Chunk(2 + part, 0, ffn_out.shape[1])

        def parts_of(quarter, core):
            at = chunk.spot(quarter, core)[1]
            return [(in_ref.at[:, :, at], 0, 2), (down_ref.at[:, :, at], 2, 1)]

        return Reduction(
            place, chunk, held_ffn.at[part], part, scratch[:reduction_refs], ffn_out, sent,
            parts_of,
        )

    def attn_reduction(part):
        chunk = Chunk(part, attn_out.shape[1], 0)

        def parts_of(quarter, core):
            return [(grads_ref.at[part * quarters + quarter, :, :, core], 0, 1)]

        held = grads_ref.at[pl.ds(part * quarters, quarters), :, :, place.core]
        return Reduction(
            place, chunk, held, part, scratch[reduction_refs:], attn_out, sent, parts_of
        )

    one, two = ffn_reduction(0), ffn_reduction(1)
    third, fourth = attn_reduction(1), attn_reduction(0)

    def load(index, source, target):
        copy = pltpu.make_async_copy(source, target, load_sems.at[index])
        copy.start()
        return copy

    def load_weight(index, k, slot):
        return load(index, attn_weights_ref.at[k], weights_ref.at[slot])

    got_out = load_weight(0, 7, 0)
    got_sides = load(1, sides_in, sides_ref)
    got_probs = load(2, cross_weights_ref.at[0], cross_probs)
    got_kv = [load_weight(3, 5, 1), load_weight(4, 6, 2)]
    one.begin()
    two.begin()
    got_qkv = load(5, qkv_in, qkv_ref)
    got_self_probs = load(6, self_weights_ref.at[0], self_probs)
    place.greet()
    one.to_core()
    two.to_core()
    moves = []

    def move(source, target):
        sems = (move_send, move_recv, stay_sems)
        moves.append(Move(place, len(moves), source, target, sems))

    move(lambda step: output_ref.at[step], lambda d: output_out.at[d])

    def weight(slot):
        return weights_ref[slot].reshape(-1, model)

    def flat(values):
        return values.reshape(-1, model)

    def lanes_at(p):
        return pl.ds(pl.multiple_of(p * pair, pair), pair)

    def keep(k, grad):
        grads_ref[k] = grad.astype(low).reshape(grads_ref.shape[1:])

    grad_low = flat(grad_second_ref[...]).astype(low)
    got_out.wait()
    mixed_grad = dot(grad_low, weight(0), 1, 1).astype(low)
    mixed_grad_ref[...] = mixed_grad.reshape(rows, dec_len, model)
    got_query = load_weight(7, 4, 0)
    one.from_core()
    keep(7, dot(flat(cross_mixed_ref[...]), grad_low, 0, 0))
    two.from_core()
    got_sides.wait()
    got_probs.wait()
    for copy in got_kv:
        copy.wait()

    def cross_row(r):
        def step(p, carry):
            at = lanes_at(p)
            dq, dk, dv, _ = attend_back_pair(
                [cross_probs[2 * p], cross_probs[2 * p + 1]],
                queries_ref[r, :, at], sides_ref[0, r, :, at], sides_ref[1, r, :, at],
                mixed_grad_ref[r, :, at], None,
            )
            query_grad_ref[r, :, at] = dq
            sides_ref[0, r, :, at] = dk
            sides_ref[1, r, :, at] = dv
            return carry

        lax.fori_loop(0, pairs, step, 0)
        if r + 1 < rows:
            following = load(8 + r, cross_weights_ref.at[r + 1], cross_probs)
        both = dot(sides_ref[0, r], weight(1), 1, 0) + dot(sides_ref[1, r], weight(2), 1, 0)
        memory_blocks[r] = both.astype(low).reshape(memory_blocks.shape[1:])
        if r + 1 < rows:
            following.wait()

    def move_memory(r):
        move(lambda step: memory_blocks.at[r, step], lambda d: memory_out.at[d, r])

    cross_row(0)
    move_memory(0)
    one.from_near()
    for r in range(1, rows):
        cross_row(r)
    got_self_out = load_weight(3, 3, 1)
    query_grad = flat(query_grad_ref[...])
    keep(4, dot(query_grad, flat(normed_two_ref[...]), 0, 0))
    two.from_near()
    for k in range(2):
        keep(5 + k, dot(flat(sides_ref[k]), flat(memory_ref[...]), 0, 0))
    third.to_core()
    one.from_last()

    got_query.wait()
    grad_two = dot(query_grad, weight(0), 1, 0)
    back, gain_two = rms_back_flat(flat(first_ref[...]), gain_ref[1:2, :], grad_two)
    grad_first = flat(grad_second_ref[...]) + back
    grad_first_ref[...] = grad_first
    grad_low = grad_first.astype(low)
    got_self_out.wait()
    mixed_grad = dot(grad_low, weight(1), 1, 1).astype(low)
    mixed_grad_ref[...] = mixed_grad.reshape(rows, dec_len, model)
    got_qkv_weights = [load_weight(7, 0, 0), load_weight(3, 1, 1), load_weight(4, 2, 2)]
    third.from_core()
    two.from_last()
    for r in range(1, rows):
        move_memory(r)
    keep(3, dot(flat(self_mixed_ref[...]), grad_low, 0, 0))
    got_qkv.wait()
    got_self_probs.wait()

    def self_row(r):
        def step(p, carry):
            at = lanes_at(p)
            dq, dk, dv, dist = attend_back_pair(
                [self_probs[2 * p], self_probs[2 * p + 1]],
                qkv_ref[0, r, :, at], qkv_ref[1, r, :, at], qkv_ref[2, r, :, at],
                mixed_grad_ref[r, :, at], small_ref.shape[-1],
            )
            qkv_ref[0, r, :, at] = dq
            qkv_ref[1, r, :, at] = dk
            qkv_ref[2, r, :, at] = dv
            for half in range(2):
                spot = 2 * p + half
                owner = (place.me + lax.div(spot, own_heads)) % mem
                head = owner * own_heads + lax.rem(spot, own_heads)
                small_ref[head] = dist[half] if r == 0 else small_ref[head] + dist[half]
            return carry

        lax.fori_loop(0, pairs, step, 0)
        if r + 1 < rows:
            following = load(8 + r, self_weights_ref.at[r + 1], self_probs)
            following.wait()

    self_row(0)
    third.from_near()
    one.from_far()
    for r in range(1, rows):
        self_row(r)
    third.from_last()
    two.from_far()
    one.from_flat()

    def project_back(k, carry):
        keep(k, dot(flat(qkv_ref[k]), flat(normed_one_ref[...]), 0, 0))
        return carry

    lax.fori_loop(0, 3, project_back, 0)
    fourth.to_core()
    for copy in got_qkv_weights:
        copy.wait()
    grad_one = dot(flat(qkv_ref[0]), weight(0), 1, 0)
    fourth.from_core()
    for k in range(1, 3):
        grad_one = grad_one + dot(flat(qkv_ref[k]), weight(k), 1, 0)
    back, gain_one = rms_back_flat(flat(input_ref[...]).astype(wide), gain_ref[0:1, :], grad_one)
    grad_input = (grad_first_ref[...] + back).astype(low).reshape(rows, dec_len, model)
    own_len = dec_len // mem
    for d in range(mem):
        input_blocks[d] = grad_input[:, d * own_len : (d + 1) * own_len, :]
    size = small_ref.shape[-1]
    for index, gain_grad in enumerate((gain_one, gain_two, gain_three_ref[...])):
        for j in range(model // size):
            spot = heads + index * (model // size) + j
            small_ref[spot] = gain_grad[:, j * size : (j + 1) * size]
    for step in range(1, mem):
        back_step = mem - step
        sent.append(
            send(
                small_ref, small_far.at[back_step], (small_send, small_recv), step,
                place.along(step), back_step,
            )
        )
    two.from_flat()
    one.from_pass()
    third.from_far()
    fourth.from_near()
    move(
        lambda step: input_blocks.at[(place.me + step) % mem], lambda d: input_out.at[d]
    )
    total = small_ref[...]
    for step in range(1, mem):
        expect(small_far.at[step], (small_send, small_recv), step, place)
        total = total + small_far[step]
    small_flat[0] = total
    for turn in range(1, block):
        there = place.at(place.turn(turn // 2), (place.core + turn % 2) % 2)
        sems = (small_send, small_recv)
        sent.append(send(small_flat.at[0], small_flat.at[turn], sems, mem + turn, there))
    two.from_pass()
    third.from_flat()
    fourth.from_last()
    third.from_pass()
    total = small_flat[0]
    for turn in range(1, block):
        expect(small_flat.at[turn], (small_send, small_recv), mem + turn, place)
        total = total + small_flat[turn]
    small_out[...] = total
    fourth.from_far()
    fourth.from_flat()
    fourth.from_pass()
    for moving in moves:
        moving.finish()
    for copy in sent:
        copy.wait_send()


def back_all(
    ffn, attn_weights, cross_weights, self_weights, sides, qkv, output,
    grad_second, first, inputs, normed_one, normed_two, self_mixed, cross_mixed, queries,
    memory, gains, gain_three, lane_count,
):
    mem = lax.axis_size("mem")
    own_hidden, model = ffn[0].shape[-2:]
    own_width = attn_weights.shape[2]
    count, heads, dec_len, _ = self_weights.shape
    enc_len = memory.shape[1]
    small_shape = (heads + 3 * (model // lane_count), 1, lane_count)
    dma = pltpu.SemaphoreType.DMA
    in_place = pl.BlockSpec(memory_space=pl.ANY)
    held = pl.BlockSpec(memory_space=pltpu.VMEM)
    attn_chunk, ffn_chunk = Chunk(0, own_width, 0), Chunk(2, 0, own_hidden)
    move_count = count + 2

    def values(*shape, dtype=low):
        return jax.ShapeDtypeStruct(shape, dtype)

    return pl.pallas_call(
        back_body,
        in_specs=[in_place] * 7 + [held] * 12,
        out_specs=[held, held, in_place, in_place, in_place, held],
        out_shape=[
            values(2 * quarters, own_width, model),
            values(3, own_hidden, model),
            values(*output.shape),
            values(mem, count, enc_len // mem, model),
            values(*output.shape),
            values(*small_shape, dtype=wide),
        ],
        scratch_shapes=[
            pltpu.VMEM((2, quarters, 3, mem, ffn_chunk.rows, model), low),
            pltpu.VMEM((2 * quarters, 1, mem, 2, attn_chunk.rows, model), low),
            pltpu.VMEM((3,) + attn_weights.shape[1:], low),
            pltpu.VMEM(cross_weights.shape[1:], low),
            pltpu.VMEM(self_weights.shape[1:], low),
            pltpu.VMEM(sides.shape, low),
            pltpu.VMEM(qkv.shape, low),
            pltpu.VMEM(inputs.shape, low),
            pltpu.VMEM(inputs.shape, low),
            pltpu.VMEM((count * dec_len, model), wide),
            pltpu.VMEM((count, mem, enc_len // mem, model), low),
            pltpu.VMEM(output.shape, low),
            pltpu.VMEM(small_shape, wide),
            pltpu.VMEM((mem,) + small_shape, wide),
            pltpu.VMEM((block,) + small_shape, wide),
            dma((8 + count,)),
            dma((move_count, mem)), dma((move_count, mem)), dma((move_count,)),
            dma((mem + block,)), dma((mem + block,)),
        ]
        + reduction_scratch(ffn_chunk, mem, model)
        + reduction_scratch(attn_chunk, mem, model),
        compiler_params=pltpu.CompilerParams(
            collective_id=1, has_side_effects=True, vmem_limit_bytes=66000000
        ),
    )(
        *ffn, attn_weights, cross_weights, self_weights, sides, qkv, output,
        grad_second, first, inputs, normed_one, normed_two, self_mixed, cross_mixed, queries,
        memory, gains, gain_three,
    )


def sum_blocks(values):
    bit = block
    while bit < lax.axis_size("rows"):
        values = values + flip(values, bit)
        bit *= 2
    return values


def dot(left, right, left_dim, right_dim):
    return lax.dot_general(
        left, right, (((left_dim,), (right_dim,)), ((), ())), preferred_element_type=wide
    )


def lanes_of(half):
    lane = lax.broadcasted_iota(jnp.int32, (1, pair), 1)
    return ((lane // head_size) == half).astype(wide)


def skewed(row, height):
    spread = jnp.broadcast_to(row, (height, row.shape[1]))
    return pltpu.roll(spread, 0, 1, stride=1, stride_axis=0)


def causal_mask(same):
    rows, keys = same.shape
    i = lax.broadcasted_iota(jnp.int32, (rows, keys), 0)
    j = lax.broadcasted_iota(jnp.int32, (rows, keys), 1)
    return same & (i >= j)


def attend_pair(queries, keys_in, values_in, allowed, bias):
    rows, keys = allowed.shape
    kept = []
    mixed = jnp.zeros((rows, pair), wide)
    for half in range(2):
        lanes = lanes_of(half)
        scores = dot(queries * lanes.astype(low), keys_in, 1, 1)
        if bias is not None:
            scores = scores + skewed(bias[half], rows)[:, :keys]
        scores = jnp.where(allowed, scores, negative)
        raised = jnp.exp(scores - jnp.max(scores, axis=-1, keepdims=True))
        scale = 1.0 / jnp.sum(raised, axis=-1, keepdims=True)
        weights = (raised * scale).astype(low)
        kept.append(weights)
        mixed = mixed + dot(weights, values_in, 1, 0) * lanes
    return kept, mixed.astype(low)


def attend_back_pair(weights_pair, queries, keys_in, values_in, grad, dist_width):
    rows, keys = weights_pair[0].shape
    dq = jnp.zeros((rows, pair), wide)
    dk = jnp.zeros((keys, pair), wide)
    dv = jnp.zeros((keys, pair), wide)
    dist = []
    for half in range(2):
        lanes = lanes_of(half)
        weights = weights_pair[half]
        weights_wide = weights.astype(wide)
        grad_weights = dot(grad * lanes.astype(low), values_in, 1, 1)
        inner = jnp.sum(grad_weights * weights_wide, axis=-1, keepdims=True)
        grad_scores = (weights_wide * (grad_weights - inner)).astype(low)
        dv = dv + dot(weights, grad, 0, 0) * lanes
        dq = dq + dot(grad_scores, keys_in, 1, 0) * lanes
        dk = dk + dot(grad_scores, queries, 0, 0) * lanes
        if dist_width is not None:
            i = lax.broadcasted_iota(jnp.int32, (rows, rows), 0)
            j = lax.broadcasted_iota(jnp.int32, (rows, rows), 1)
            upside_down = dot((i + j == rows - 1).astype(wide).astype(low), grad_scores, 1, 0)
            padded = jnp.concatenate(
                [upside_down, jnp.zeros((rows, dist_width - keys), wide)], axis=1
            )
            turned = pltpu.roll(padded, 0, 1, stride=1, stride_axis=0)
            dist.append(jnp.sum(turned, axis=0, keepdims=True))
    return dq.astype(low), dk.astype(low), dv.astype(low), dist


def rms_back_flat(values, gain, grad):
    scale = lax.rsqrt(jnp.mean(values * values, axis=-1, keepdims=True) + epsilon)
    grad_gain = jnp.sum(grad * values * scale, axis=0, keepdims=True)
    scaled = grad * gain
    inner = jnp.mean(scaled * values, axis=-1, keepdims=True)
    return scaled * scale - values * (scale * scale * scale * inner), grad_gain


def rms(values, gain):
    scale = lax.rsqrt(jnp.mean(values * values, axis=-1, keepdims=True) + epsilon)
    return (values * scale * gain).astype(low), scale


def rms_back(values, scale, gain, grad):
    grad_gain = jnp.sum(grad * values * scale, axis=(0, 1))
    scaled = grad * gain
    inner = jnp.mean(scaled * values, axis=-1, keepdims=True)
    return scaled * scale - values * (scale * scale * scale * inner), grad_gain


def times_t(values, weight):
    return jnp.einsum("rtd,cd->rtc", values, weight, preferred_element_type=wide)


def times(values, weight):
    return jnp.einsum("rtc,cd->rtd", values, weight, preferred_element_type=wide)


def weight_grad(grads, values):
    return jnp.einsum("rtc,rtd->cd", grads, values, preferred_element_type=wide).astype(low)


def gated(gate, upward):
    return jax.nn.gelu(gate, approximate=True) * upward


def shards(
    dec_input,
    enc_output,
    dec_segments,
    enc_segments,
    buckets,
    gains,
    self_query,
    self_kv,
    self_out,
    rel_table,
    cross_query,
    cross_kv,
    cross_out,
    ffn_in,
    ffn_out,
    cotangent,
):
    mem = lax.axis_size("mem")
    me = lax.axis_index("mem")
    group, dec_len, model = dec_input.shape
    count = group // mem
    own_heads = rel_table.shape[1]
    own_width = self_query.shape[1]
    width = own_width * mem
    pairs = width // pair
    own_hidden = ffn_out.shape[0]
    gain_values = gains.astype(wide)
    bucket_count = rel_table.shape[0]

    attn_shard = jnp.stack(
        [self_query.T, self_kv[0].T, self_kv[1].T, self_out]
        + [cross_query.T, cross_kv[0].T, cross_kv[1].T, cross_out]
    )
    in_shard = jnp.swapaxes(ffn_in, 1, 2)
    down_shard = ffn_out[None]
    padded_table = jnp.pad(rel_table, ((0, 0), (0, pair - own_heads)))

    def mine(values):
        return lax.dynamic_slice_in_dim(values, me * count, count, 0)

    own_input = mine(dec_input)
    inputs = own_input.astype(wide)
    grad_out = mine(cotangent)
    dec_ids = mine(dec_segments)
    enc_ids = jnp.concatenate(relative(mine(enc_segments), 1, mem), axis=1)
    enc_len = enc_ids.shape[1]

    lane_count = -(-dec_len // pair) * pair
    turned = jnp.concatenate(
        [
            buckets[:1],
            jnp.full((lane_count - dec_len,), -1, buckets.dtype),
            jnp.flip(buckets[1:]),
        ]
    )
    spread = (jnp.arange(bucket_count)[:, None] == turned[None, :]).astype(low)

    normed_one, scale_one = rms(inputs, gain_values[0])
    (
        attn_weights_in, in_weight, out_weight, memory,
        qkv, self_mixed, self_weights, first, normed_two,
        cross_queries, cross_sides, cross_mixed, cross_weights,
    ) = gather_all(
        attn_shard, in_shard, down_shard, enc_output, padded_table,
        own_input, normed_one, gain_values, dec_ids, enc_ids, spread,
    )
    cross_out_weight = attn_weights_in[7].reshape(width, model)
    in_weight = in_weight.reshape(-1, model)
    out_weight = out_weight.reshape(-1, model)
    memory = memory.reshape(count, -1, model)
    second = first + times(cross_mixed, cross_out_weight)
    normed_three, scale_three = rms(second, gain_values[2])

    hidden_width = mem * own_hidden
    gate_up = times_t(normed_three, in_weight)
    hidden_float, pull = jax.vjp(gated, gate_up[..., :hidden_width], gate_up[..., hidden_width:])
    hidden = hidden_float.astype(low)
    output = second + times(hidden, out_weight)
    grad_gate, grad_up = pull(times_t(grad_out, out_weight))
    grad_gate_up = jnp.concatenate([grad_gate.astype(low), grad_up.astype(low)], axis=-1)
    grad_three = times(grad_gate_up, in_weight)
    ffn_grads = [
        grad.reshape(-1, mem, own_hidden, model)
        for grad in (weight_grad(grad_gate_up, normed_three), weight_grad(hidden, grad_out))
    ]

    grad_wide = grad_out.astype(wide)
    back, gain_three = rms_back(second, scale_three, gain_values[2], grad_three)
    grad_second = grad_wide + back
    attn_sums, ffn_sums, output, grad_memory, grad_input, small = back_all(
        ffn_grads, attn_weights_in, cross_weights, self_weights, cross_sides, qkv,
        jnp.stack(relative(output.astype(low), 1, mem)),
        grad_second, first, own_input, normed_one, normed_two, self_mixed, cross_mixed,
        cross_queries, memory, gain_values, gain_three[None], lane_count,
    )
    attn_sums = sum_blocks(attn_sums)
    ffn_sums = sum_blocks(ffn_sums)
    small = sum_blocks(small[:, 0])
    heads = mem * own_heads
    gain_sums = lax.dynamic_slice_in_dim(
        small[heads:].reshape(3, model), me * own_width, own_width, 1
    )
    falling = jnp.concatenate(
        [jnp.flip(buckets), jnp.full((lane_count - dec_len,), -1, buckets.dtype)]
    )
    one_hot = (falling[:, None] == jnp.arange(bucket_count)[None, :]).astype(wide)
    own_sums = lax.dynamic_slice_in_dim(small, me * own_heads, own_heads, 0)
    grad_table = jnp.einsum("hl,lb->bh", own_sums, one_hot, precision=highest)

    def columns(values):
        return jnp.swapaxes(values, -1, -2).astype(wide)

    return (
        output.reshape(group, -1, model).astype(wide),
        grad_input.reshape(group, -1, model).astype(wide),
        grad_memory.reshape(group, -1, model).astype(wide),
        gain_sums,
        columns(attn_sums[0]),
        columns(attn_sums[1:3]),
        attn_sums[3].astype(wide),
        grad_table,
        columns(attn_sums[4]),
        columns(attn_sums[5:7]),
        attn_sums[7].astype(wide),
        columns(ffn_sums[:2]),
        ffn_sums[2].astype(wide),
    )


def solution(mesh):
    in_specs = (
        P("rows", None, None),
        P("rows", "mem", None),
        P("rows", None),
        P("rows", None),
        P(),
        P(),
        P(None, "mem"),
        P(None, None, "mem"),
        P("mem", None),
        P(None, "mem"),
        P(None, "mem"),
        P(None, None, "mem"),
        P("mem", None),
        P(None, None, "mem"),
        P("mem", None),
        P("rows", None, None),
    )
    out_specs = (
        P("rows", "mem", None),
        P("rows", "mem", None),
        P("rows", "mem", None),
        P(None, "mem"),
        P(None, "mem"),
        P(None, None, "mem"),
        P("mem", None),
        P(None, "mem"),
        P(None, "mem"),
        P(None, None, "mem"),
        P("mem", None),
        P(None, None, "mem"),
        P("mem", None),
    )
    return jax.shard_map(shards, mesh=mesh, in_specs=in_specs, out_specs=out_specs, check_vma=False)
```
